256 devices in a mesh: grp: 2 (over y), tm: 128 (over x, z, core).
Axes of the slice: x: 4, y: 2, z: 16, core: 2. Of those that a mesh axis runs over, the one named last changes fastest.
The devices are a block of a 4x16x16 slice.
Arguments:
- traces: float32 [2048, 16384], P('grp', 'tm'), parts along dimension 0, may hold values from -6 to 6
- templates: float32 [512, 8192], P('tm'), may hold values from -6 to 6
- moveouts: int32 [2048], P('grp'), parts along dimension 0, may hold values from 0 to 2047
- masks: int32 [512, 2048], P(None, 'grp'), parts along dimension 1, may hold values 0 or 1
Outputs:
- detection: float32 [512, 16384], P('tm', 'grp'), parts along dimension 1
The draws below stay inside these ranges and needn't reach their ends.
There are 2 independent parts, one for each index of `grp`. The reference program is written for one: setup_inputs(seed, part) draws one part's arguments, and reference() takes and returns one part's arrays. A program takes and returns all parts, laid end to end along the dimension named above; an argument that names none is the same for every part. Nothing has to cross between parts.
All inputs are finite; a program needn't handle non-finite values.
Results may differ from the reference program's by a relative error of at most 0.000073.
Values sent between devices are 32-bit elements; how exact they have to be, the bound alone decides.
A program may use at most 64 MiB of HBM per device.

```python
import math
import jax
import jax.numpy as jnp
from jax import lax

C = 1024
L = 8192
NF = 16384
K = 512


def with_ends(drawn, key, least, top_value):
    index_at = [jax.random.randint(jax.random.fold_in(key, axis), (), 0, length) for axis, length in enumerate(drawn.shape)]
    main_axis = drawn.shape.index(max(drawn.shape))
    beside = index_at[:main_axis] + [(index_at[main_axis] + 1) % drawn.shape[main_axis]] + index_at[main_axis + 1:]
    return drawn.at[tuple(index_at)].set(least).at[tuple(beside)].set(top_value)


def block_scale(stream_key, dims, shards, low, top_value):
    def one(position, blocks):
        steps = jax.random.uniform(jax.random.fold_in(jax.random.fold_in(stream_key, 6), position), (blocks,), jnp.float32, low / len(shards), top_value / len(shards))
        return jnp.repeat(jnp.exp(steps), dims[position] // blocks).reshape((-1,) + (1,) * (len(dims) - position - 1))

    factor_of = one(*shards[0])
    for cut in shards[1:]:
        factor_of = factor_of * one(*cut)
    return factor_of


def gaussian(rng, dims, deviation, limit, split=(), kind=jnp.bfloat16):
    array = deviation * jax.random.normal(rng, dims, jnp.float32)
    if split:
        array = array * block_scale(rng, dims, split, -0.22, 0.18)
    return jnp.clip(array, -limit, limit).astype(kind)


def setup_inputs(seed: int = 0, part: int = 0) -> dict:
    arg_keys = jax.random.split(jax.random.key(seed), 5)
    part_keys = jax.random.split(jax.random.fold_in(arg_keys[4], part), 5)
    return {
        "traces": gaussian(part_keys[0], (C, NF), 1.0, 6.0, ((1, 128),), jnp.float32),
        "templates": gaussian(arg_keys[1], (K, L), 1.0, 6.0, ((0, 128),), jnp.float32),
        "moveouts": with_ends(jax.random.randint(part_keys[2], (C,), 0, NF // 8), jax.random.fold_in(part_keys[2], 1), 0, (NF // 8) - 1).astype(jnp.int32),
        "masks": with_ends((jax.random.randint(part_keys[3], (K, C), 0, 4) < 3).astype(jnp.int32), jax.random.fold_in(part_keys[3], 1), 0, 1),
    }


def reference(traces, templates, moveouts, masks):
    length = traces.shape[1]
    spectra = jnp.fft.fft(traces, axis=1)
    freqs = jnp.arange(length).astype(jnp.int32)
    angle = 2.0 * math.pi / length * (moveouts.astype(jnp.int32)[:, None] * freqs[None, :] % length).astype(jnp.float32)
    moved = spectra * (jnp.cos(angle) + 1j * jnp.sin(angle))
    mask_float = masks.astype(jnp.float32)
    stacked_re = jnp.dot(mask_float, jnp.real(moved), precision=lax.Precision.HIGHEST, preferred_element_type=jnp.float32)
    stacked_im = jnp.dot(mask_float, jnp.imag(moved), precision=lax.Precision.HIGHEST, preferred_element_type=jnp.float32)
    template_spectra = jnp.fft.fft(templates, n=length, axis=1)
    product = (stacked_re + 1j * stacked_im) * jnp.conj(template_spectra)
    correlation = jnp.real(jnp.fft.ifft(product, axis=1))[:, :templates.shape[1]]
    energy = jnp.sqrt(lax.optimization_barrier(jnp.sum(templates * templates, axis=1)) + 1e-06)
    return correlation / (math.sqrt(traces.shape[0]) * energy[:, None])
```

```python
import functools
import math

import jax
import jax.numpy as jnp
import numpy as np
from jax import lax
from jax.experimental import pallas as pl
from jax.experimental.pallas import tpu as pltpu
from jax.sharding import Mesh
from jax.sharding import PartitionSpec as P

MESH = pl.DeviceIdType.MESH
LANES = 128
GROUP = 2


def split(value):
    high = value.astype(jnp.bfloat16)
    low = (value - high.astype(jnp.float32)).astype(jnp.bfloat16)
    return high, low


def split_constant(value):
    value = np.asarray(value, np.float64).astype(np.float32)
    high = value.astype(jnp.bfloat16)
    low = (value - high.astype(np.float32)).astype(jnp.bfloat16)
    return jnp.asarray(np.stack([high, low]))


def mm(a, b):
    return jnp.dot(a, b, preferred_element_type=jnp.float32)


def dot3(left, right):
    (left_hi, left_lo), (right_hi, right_lo) = left, right
    return mm(left_hi, right_hi) + (mm(left_hi, right_lo) + mm(left_lo, right_hi))


def stack_kernel(
    cfg, x_hbm, masks_hbm, mo_ref, out_ref,
    pair, mask_int, mask_rows, rolled, shift_at, parts, partial, up, down, ready, landed,
    load_sem, pair_sem, up_send, up_recv, down_send, down_recv, last_send, last_recv,
):
    rows, ring, hops, above, below = cfg
    channels = x_hbm.shape[0]
    blocks = rows * ring
    chip_samples = 2 * LANES
    x = lax.axis_index("tm_0")
    z = lax.axis_index("tm_1")
    core = lax.axis_index("tm_2")
    here = x * ring + z

    def far(dx, dz):
        return {"tm_0": lax.rem(x + dx + rows, rows), "tm_1": lax.rem(z + dz + ring, ring)}

    def chip(step):
        other = lax.rem(here + step + blocks, blocks)
        return {"tm_0": other // ring, "tm_1": lax.rem(other, ring)}

    barrier = pltpu.get_barrier_semaphore()
    pl.semaphore_signal(barrier, inc=1, device_id={"tm_2": 1 - core}, device_id_type=MESH)
    senders = 1
    for dz in range(-above, below + 1):
        for dx in range(rows):
            if dx or dz:
                pl.semaphore_signal(barrier, inc=1, device_id=far(dx, dz), device_id_type=MESH)
                senders += 1

    mask_copy = pltpu.make_async_copy(masks_hbm, mask_int, load_sem.at[0])
    mask_copy.start()
    own_copy = pltpu.make_async_copy(x_hbm, pair.at[core], load_sem.at[1])
    own_copy.start()
    mask_copy.wait()

    tile_rows = mask_int.shape[2]
    half_tile = tile_rows // 2
    tops = lax.broadcasted_iota(jnp.int32, (tile_rows, channels), 0) < half_tile

    def pick(first, second):
        moved = pltpu.roll(jnp.where(core == 0, second, first), half_tile, 0)
        kept = jnp.where(core == 0, first, second)
        return jnp.where(tops == (core == 0), kept, moved)

    @pl.loop(0, ring)
    def _(e):
        owner = lax.rem(z + e, ring)
        pieces = [
            pick(mask_int[a, owner], mask_int[a + 1, owner]).astype(jnp.float32) for a in range(0, rows, 2)
        ]
        mask_rows[e] = jnp.concatenate(pieces, axis=0).astype(jnp.bfloat16)

    own_copy.wait()
    pl.semaphore_wait(barrier, senders)
    swap = pltpu.make_async_remote_copy(
        src_ref=pair.at[core],
        dst_ref=pair.at[core],
        send_sem=pair_sem.at[0],
        recv_sem=pair_sem.at[1],
        device_id={"tm_2": 1 - core},
        device_id_type=MESH,
    )
    swap.start()
    swap.wait()

    lane = lax.broadcasted_iota(jnp.int32, (LANES, LANES), 1)

    @pl.loop(0, channels // LANES)
    def _(b):
        at = pl.ds(pl.multiple_of(b * LANES, LANES), LANES)
        spread = jnp.broadcast_to(mo_ref[pl.ds(b, 1), :].astype(jnp.float32), (LANES, LANES))
        move = jnp.transpose(spread).astype(jnp.int32)
        fine = lax.rem(move, chip_samples)
        coarse = move // chip_samples
        first, second = pair[0, at, :], pair[1, at, :]
        swapped = fine >= LANES
        first, second = jnp.where(swapped, second, first), jnp.where(swapped, first, second)
        k = 1
        while k < LANES:
            taken = (fine & k) != 0
            inside = lane < LANES - k
            a, d = pltpu.roll(first, LANES - k, 1), pltpu.roll(second, LANES - k, 1)
            first, second = (
                jnp.where(taken, jnp.where(inside, a, d), first),
                jnp.where(taken, jnp.where(inside, d, a), second),
            )
            k *= 2
        rolled[at, :LANES] = first
        rolled[at, LANES:] = second
        shift_at[at, :LANES] = coarse + (lane >= chip_samples - fine).astype(jnp.int32)
        shift_at[at, LANES:] = coarse + (lane + LANES >= chip_samples - fine).astype(jnp.int32)

    def contribution(j):
        @pl.loop(0, channels // LANES)
        def _(b):
            at = pl.ds(pl.multiple_of(b * LANES, LANES), LANES)
            high, low = split(jnp.where(shift_at[at, :] == j, rolled[at, :], 0.0))
            parts[0, at, :] = high
            parts[1, at, :] = low

        weights = mask_rows[...].reshape(-1, channels)
        total = mm(weights, parts[0]) + mm(weights, parts[1])
        partial[j] = total.reshape(partial.shape[1:])

    @pl.loop(0, 2)
    def _(t):
        contribution(t * hops)

    sends = []

    def send(src, dst, send_sem, recv_sem, where):
        copy = pltpu.make_async_remote_copy(
            src_ref=src, dst_ref=dst, send_sem=send_sem, recv_sem=recv_sem, device_id=where, device_id_type=MESH
        )
        copy.start()
        sends.append(copy)

    up_groups = [(max(top - GROUP + 1, 1), top) for top in range(above_top(cfg), 0, -GROUP)]
    down_groups = [
        (low, min(low + GROUP - 1, hops - 1)) for low in range(-below, hops, GROUP)
    ]
    upward, downward = chip(1), chip(-1)

    def up_range(j, g):
        low, top = up_groups[g]
        low = max(low, j + 1)
        return (low - j, top - low + 1) if low <= top else None

    def down_range(j, g):
        low, top = down_groups[g]
        top = min(top, j - 1)
        return (low - j, top - low + 1) if low <= top else None

    def send_up(j, g):
        found = up_range(j, g)
        if found is None or j == hops:
            return
        e, count = found
        src = partial.at[0, pl.ds(e, count)] if j == 0 else up.at[j - 1, pl.ds(e, count)]
        send(src, up.at[j, pl.ds(e - 1, count)], up_send.at[j, g], up_recv.at[j, g], upward)

    def send_down(j, g):
        found = down_range(j, g)
        if found is None or j == 0:
            return
        e, count = found
        if j == hops:
            src = partial.at[hops, pl.ds(e + ring, count)]
        else:
            src = down.at[j, pl.ds(e + ring, count)]
        send(src, down.at[j - 1, pl.ds(e + 1 + ring, count)], down_send.at[j - 1, g], down_recv.at[j - 1, g], downward)

    for g in range(max(len(up_groups), len(down_groups))):
        if g < len(up_groups):
            send_up(0, g)
        if g < len(down_groups):
            send_down(hops, g)

    @pl.loop(1, hops)
    def _(j):
        contribution(j)

    per_owner = partial.shape[2] // rows

    def deliver(total, o, j, e):
        for a in range(rows):
            piece = total[a * per_owner : (a + 1) * per_owner]
            ready[o + below, a] = jnp.concatenate([piece[:, :LANES], piece[:, LANES:]], axis=0)
        block = lax.rem(here - j + blocks, blocks)
        for d in range(rows):
            owner = lax.rem(x + d, rows)
            src, dst = ready.at[o + below, owner], landed.at[block]
            if d == 0 and e == 0:
                copy = pltpu.make_async_copy(src, dst, last_recv)
                copy.start()
            else:
                send(src, dst, last_send.at[o + below, d], last_recv, far(d, e))

    def wait_for(ref, sem):
        pltpu.make_async_copy(ref, ref, sem).wait()

    for step in range(1, hops + 1):
        j, i = step, hops - step
        for g in range(max(len(up_groups), len(down_groups))):
            if g < len(up_groups):
                arrived = up_range(j - 1, g)
                if arrived is not None:
                    e, count = arrived[0] - 1, arrived[1]
                    wait_for(up.at[j - 1, pl.ds(e, count)], up_recv.at[j - 1, g])
                    for c in range(e, e + count):
                        if c > 0:
                            up[j - 1, c] = up[j - 1, c] + partial[j, c]
                    send_up(j, g)
            if g < len(down_groups):
                arrived = down_range(i + 1, g)
                if arrived is not None:
                    e, count = arrived[0] + 1, arrived[1]
                    wait_for(down.at[i, pl.ds(e + ring, count)], down_recv.at[i, g])
                    for c in range(e, e + count):
                        if c < 0:
                            down[i, c + ring] = down[i, c + ring] + partial[i, c + ring]
                    send_down(i, g)
        if j == hops:
            for o in range(above_top(cfg), hops, -1):
                deliver(up[j - 1, o - j], o, j, o - j)
            for o in range(-below, 0):
                deliver(down[0, o + ring], o, 0, o)
        ends = [j, i] if j > i else [j] if j == i else []
        for at in ends:
            total = partial[at, 0]
            if at > 0:
                total = total + up[at - 1, 0]
            if at < hops:
                total = total + down[at, ring]
            deliver(total, at, at, 0)

    wait_for(landed, last_recv)
    out_ref[...] = landed[...]
    for copy in sends:
        copy.wait_send()


def above_top(cfg):
    return cfg[2] + cfg[3]


def forward(series, first, twiddle, second):
    half = twiddle.shape[1]
    turned = []
    for s in series:
        y = dot3((first[0], first[1]), split(s))
        re, im = y[:half], y[half:]
        turned.append(
            jnp.concatenate(
                [re * twiddle[0] - im * twiddle[1], re * twiddle[1] + im * twiddle[0]], axis=1
            )
        )
    return dot3(split(jnp.concatenate(turned, axis=0)), (second[0], second[1]))


def correlate_kernel(
    scale, stack_ref, templ_ref, first_ref, first_half_ref, twiddle_ref, second_ref, third_ref, fourth_ref, out_ref
):
    count = out_ref.shape[1]
    long, short = stack_ref.shape[0] // count, templ_ref.shape[0] // count
    half = twiddle_ref.shape[1]
    templates = [templ_ref[pl.ds(i, short, stride=count), :] for i in range(count)]
    series = [stack_ref[pl.ds(i, long, stride=count), :] for i in range(count)]
    twiddle = twiddle_ref[...]
    second = second_ref[...]
    templ = forward(templates, first_half_ref[...], twiddle, second)
    spec = forward(series, first_ref[...], twiddle, second)
    sr, si, hr, hi = spec[:, :LANES], spec[:, LANES:], templ[:, :LANES], templ[:, LANES:]
    product = jnp.concatenate([sr * hr + si * hi, si * hr - sr * hi], axis=1)
    third = third_ref[...]
    back = dot3(split(product), (third[0], third[1]))
    fourth = fourth_ref[...]
    for i in range(count):
        re, im = back[i * half : (i + 1) * half, :LANES], back[i * half : (i + 1) * half, LANES:]
        turned = jnp.concatenate(
            [re * twiddle[0] + im * twiddle[1], im * twiddle[0] - re * twiddle[1]], axis=0
        )
        lags = dot3((fourth[0], fourth[1]), split(turned))
        energy = jnp.sqrt(jnp.sum(templates[i] * templates[i], keepdims=True) + 1e-06)
        out_ref[:, i, :] = lags * (1.0 / (scale * energy))


def fourier_tables(length, lag_count):
    blocks = length // LANES
    kept = blocks // 2 + 1
    half = -(-kept // 8) * 8
    f1 = np.arange(half)
    n1 = np.arange(blocks)
    n2 = np.arange(LANES)
    live = (f1 < kept)[:, None]
    angle = 2.0 * np.pi * ((f1[:, None] * n1[None, :]) % blocks) / blocks
    first = np.concatenate([np.cos(angle) * live, -np.sin(angle) * live])
    turn = 2.0 * np.pi * ((f1[:, None] * n2[None, :]) % length) / length
    twiddle = np.stack([np.cos(turn) * live, -np.sin(turn) * live]).astype(np.float32)
    inner = 2.0 * np.pi * ((n2[:, None] * n2[None, :]) % LANES) / LANES
    c, s = np.cos(inner), np.sin(inner)
    second = np.block([[c, -s], [s, c]])
    third = np.block([[c, s], [-s, c]])
    weight = np.where((f1 == 0) | (f1 == kept - 1), 1.0, 2.0) * (f1 < kept) / length
    lag_rows = lag_count // LANES
    back = angle.T[:lag_rows]
    fourth = np.concatenate([np.cos(back) * weight, -np.sin(back) * weight], axis=1)
    return (
        split_constant(first),
        split_constant(first[:, :lag_rows]),
        jnp.asarray(twiddle),
        split_constant(second),
        split_constant(third),
        split_constant(fourth),
    )


def on_device(traces, templates, moveouts, masks):
    rows, ring = lax.axis_size("tm_0"), lax.axis_size("tm_1")
    channels, samples = traces.shape
    devices = rows * ring * 2
    length = samples * devices
    count, lag_count = templates.shape
    chip_samples = 2 * samples
    hops = (length // 8) // chip_samples
    outside = ring - 1 - hops
    below = outside // 2
    above = outside - below
    cfg = (rows, ring, hops, above, below)
    chunk = (rows * count, chip_samples)
    groups_up = -(-(hops + above) // GROUP)
    groups_down = -(-(hops + below) // GROUP)
    vmem = pl.BlockSpec(memory_space=pltpu.VMEM)
    anywhere = pl.BlockSpec(memory_space=pl.ANY)
    dma = pltpu.SemaphoreType.DMA
    stacked = pl.pallas_call(
        functools.partial(stack_kernel, cfg),
        out_shape=jax.ShapeDtypeStruct((rows * ring, 2 * count, LANES), jnp.float32),
        in_specs=[anywhere, anywhere, vmem],
        out_specs=vmem,
        scratch_shapes=[
            pltpu.VMEM((2, channels, samples), jnp.float32),
            pltpu.VMEM((rows, ring, 2 * count, channels), jnp.int32),
            pltpu.VMEM((ring, rows * count, channels), jnp.bfloat16),
            pltpu.VMEM((channels, chip_samples), jnp.float32),
            pltpu.VMEM((channels, chip_samples), jnp.int32),
            pltpu.VMEM((2, channels, chip_samples), jnp.bfloat16),
            pltpu.VMEM((hops + 1, ring, *chunk), jnp.float32),
            pltpu.VMEM((hops, hops + above, *chunk), jnp.float32),
            pltpu.VMEM((hops, ring + 1, *chunk), jnp.float32),
            pltpu.VMEM((ring, rows, 2 * count, LANES), jnp.float32),
            pltpu.VMEM((rows * ring, 2 * count, LANES), jnp.float32),
            dma((2,)),
            dma((2,)),
            dma((hops, groups_up)),
            dma((hops, groups_up)),
            dma((hops, groups_down)),
            dma((hops, groups_down)),
            dma((ring, rows)),
            dma,
        ],
        compiler_params=pltpu.CompilerParams(collective_id=0, has_side_effects=True),
    )(
        traces,
        masks.reshape(rows, ring, 2 * count, channels),
        moveouts.reshape(channels // LANES, LANES),
    )
    lag_rows = lag_count // LANES
    tiles = templates.reshape(count, lag_rows, LANES).transpose(1, 0, 2).reshape(lag_rows * count, LANES)
    scale = math.sqrt(channels)
    tables = fourier_tables(length, lag_count)
    found = pl.pallas_call(
        functools.partial(correlate_kernel, scale),
        out_shape=jax.ShapeDtypeStruct((lag_rows, count, LANES), jnp.float32),
        in_specs=[vmem] * (2 + len(tables)),
        out_specs=vmem,
    )(stacked.reshape(-1, LANES), tiles, *tables)
    return found.transpose(1, 0, 2).reshape(count, lag_count)


def solution(mesh):
    finer = Mesh(mesh.devices.reshape(mesh.shape["grp"], 4, -1, 2), ("grp", "tm_0", "tm_1", "tm_2"))
    axes = ("tm_0", "tm_1", "tm_2")
    return jax.shard_map(
        on_device,
        mesh=finer,
        in_specs=(P("grp", axes), P(axes, None), P("grp"), P(None, "grp")),
        out_specs=P(axes, "grp"),
        check_vma=False,
    )
```

```python
import functools
import math

import jax
import jax.numpy as jnp
import numpy as np
from jax import lax
from jax.experimental import pallas as pl
from jax.experimental.pallas import tpu as pltpu
from jax.sharding import Mesh
from jax.sharding import PartitionSpec as P

MESH = pl.DeviceIdType.MESH
LANES = 128
GROUP = 2
PIECES = 4


def split(value):
    high = value.astype(jnp.bfloat16)
    low = (value - high.astype(jnp.float32)).astype(jnp.bfloat16)
    return high, low


def split_constant(value):
    value = np.asarray(value, np.float64).astype(np.float32)
    high = value.astype(jnp.bfloat16)
    low = (value - high.astype(np.float32)).astype(jnp.bfloat16)
    return jnp.asarray(np.stack([high, low]))


def mm(a, b):
    return jnp.dot(a, b, preferred_element_type=jnp.float32)


def dot3(left, right):
    (left_hi, left_lo), (right_hi, right_lo) = left, right
    return mm(left_hi, right_hi) + (mm(left_hi, right_lo) + mm(left_lo, right_hi))


def forward(series, first, twiddle, second):
    half = twiddle.shape[1]
    turned = []
    for s in series:
        y = dot3((first[0], first[1]), split(s))
        re, im = y[:half], y[half:]
        turned.append(
            jnp.concatenate([re * twiddle[0] - im * twiddle[1], re * twiddle[1] + im * twiddle[0]], axis=1)
        )
    return dot3(split(jnp.concatenate(turned, axis=0)), (second[0], second[1]))


def matched_kernel(
    cfg, scale,
    x_hbm, masks_hbm, mo_hbm, templ_hbm, first_hbm, first_half_hbm, twiddle_hbm, second_hbm, third_hbm, fourth_hbm,
    out_ref,
    raw, mo_ref, pair, mask_int, mask_rows, halves, shift_at, parts, partial, up, down, ready, landed,
    templ_ref, first_ref, first_half_ref, twiddle_ref, second_ref, third_ref, fourth_ref, templ_spec, gain,
    load_sem, pair_send, pair_recv, up_send, up_recv, down_send, down_recv, last_send, last_recv,
):
    rows, ring, hops, above, below, shared = cfg
    channels = x_hbm.shape[0]
    blocks = rows * ring
    x = lax.axis_index("tm_0")
    z = lax.axis_index("tm_1")
    core = lax.axis_index("tm_2")
    here = x * ring + z
    partner = {"tm_2": 1 - core}

    def chip(step):
        other = lax.rem(here + step + blocks, blocks)
        return {"tm_0": other // ring, "tm_1": lax.rem(other, ring)}

    loads = []

    def load(src, dst):
        copy = pltpu.make_async_copy(src, dst, load_sem.at[len(loads)])
        copy.start()
        loads.append(copy)
        return copy

    per_piece = channels // PIECES
    mo_copy = load(mo_hbm, mo_ref)
    x_copies = [load(x_hbm.at[pl.ds(p * per_piece, per_piece)], raw.at[pl.ds(p * per_piece, per_piece)]) for p in range(PIECES)]

    barrier = pltpu.get_barrier_semaphore()
    pl.semaphore_signal(barrier, inc=1, device_id=partner, device_id_type=MESH)
    senders = 1
    reach = max(above, below) + shared
    for dz in range(-reach, reach + 1):
        for dx in range(rows):
            if dx or dz:
                where = {"tm_0": lax.rem(x + dx, rows), "tm_1": lax.rem(z + dz + ring, ring)}
                pl.semaphore_signal(barrier, inc=1, device_id=where, device_id_type=MESH)
                senders += 1

    mask_copy = load(masks_hbm, mask_int)
    templ_copy = load(templ_hbm, templ_ref)
    table_copies = [
        load(first_half_hbm, first_half_ref),
        load(twiddle_hbm, twiddle_ref),
        load(second_hbm, second_ref),
        load(first_hbm, first_ref),
        load(third_hbm, third_ref),
        load(fourth_hbm, fourth_ref),
    ]

    lane = lax.broadcasted_iota(jnp.int32, (LANES, LANES), 1)
    mo_copy.wait()
    swaps = []
    for p in range(PIECES):
        x_copies[p].wait()

        @pl.loop(p * per_piece // LANES, (p + 1) * per_piece // LANES)
        def _(b):
            at = pl.ds(pl.multiple_of(b * LANES, LANES), LANES)
            spread = jnp.broadcast_to(mo_ref[pl.ds(b, 1), :].astype(jnp.float32), (LANES, LANES))
            move = jnp.transpose(spread).astype(jnp.int32)
            index = lane + (move & (LANES - 1))
            value = jnp.take_along_axis(raw[at, :], index & (LANES - 1), axis=1)
            pair[core, at, :] = value
            passed = (index >= LANES).astype(jnp.int32)
            shift_at[at, :] = ((move >> (LANES.bit_length() - 1)) + passed).astype(jnp.float32).astype(jnp.bfloat16)
            high, low = split(value)
            halves[0, core, at, :] = high
            halves[1, core, at, :] = low

        if p == 0:
            pl.semaphore_wait(barrier, senders)
        half = pair.at[core, pl.ds(p * per_piece, per_piece)]
        swap = pltpu.make_async_remote_copy(
            src_ref=half, dst_ref=half, send_sem=pair_send.at[p], recv_sem=pair_recv.at[p],
            device_id=partner, device_id_type=MESH,
        )
        swap.start()
        swaps.append(swap)

    mask_copy.wait()
    tile_rows = mask_int.shape[2]
    half_tile = tile_rows // 2
    tops = lax.broadcasted_iota(jnp.int32, (tile_rows, channels), 0) < half_tile

    def pick(first, second):
        moved = pltpu.roll(jnp.where(core == 0, second, first), half_tile, 0)
        kept = jnp.where(core == 0, first, second)
        return jnp.where(tops == (core == 0), kept, moved)

    @pl.loop(0, ring)
    def _(e):
        owner = lax.rem(z + e, ring)
        pieces = [
            pick(mask_int[a, owner], mask_int[a + 1, owner]).astype(jnp.float32) for a in range(0, rows, 2)
        ]
        mask_rows[e] = jnp.concatenate(pieces, axis=0).astype(jnp.bfloat16)

    for p in range(PIECES):
        swaps[p].wait_recv()

        @pl.loop(p * per_piece // LANES, (p + 1) * per_piece // LANES)
        def _(b):
            at = pl.ds(pl.multiple_of(b * LANES, LANES), LANES)
            high, low = split(pair[1 - core, at, :])
            halves[0, 1 - core, at, :] = high
            halves[1, 1 - core, at, :] = low

    zero = jnp.zeros((LANES, LANES), jnp.bfloat16)

    def contribution(j):
        twice = jnp.broadcast_to((2 * j).astype(jnp.float32), (LANES, LANES))
        before, same, after = ((twice + d).astype(jnp.bfloat16) for d in (-1, 0, 1))

        @pl.loop(0, channels // LANES)
        def _(b):
            at = pl.ds(pl.multiple_of(b * LANES, LANES), LANES)
            shift = shift_at[at, :]
            is_before, is_same, is_after = shift == before, shift == same, shift == after
            for t in range(2):
                first, second = halves[t, 0, at, :], halves[t, 1, at, :]
                parts[t, at, :LANES] = jnp.where(is_same, first, jnp.where(is_after, second, zero))
                parts[t, at, LANES:] = jnp.where(is_before, first, jnp.where(is_same, second, zero))

        weights = mask_rows[...].reshape(-1, channels)
        total = mm(weights, parts[0]) + mm(weights, parts[1])
        partial[j] = total.reshape(partial.shape[1:])

    def contributions(s):
        if s == hops - s:
            contribution(jnp.int32(s))
        else:
            @pl.loop(0, 2)
            def _(t):
                contribution(s + t * (hops - 2 * s))

    contributions(0)

    sends = []

    def send(src, dst, send_sem, recv_sem, where):
        copy = pltpu.make_async_remote_copy(
            src_ref=src, dst_ref=dst, send_sem=send_sem, recv_sem=recv_sem, device_id=where, device_id_type=MESH
        )
        copy.start()
        sends.append(copy)

    chunk_rows = partial.shape[2]
    part = chunk_rows // 2
    everything = (0, chunk_rows)
    up_groups = [(hops + above + 1, hops + above + 1, (0, part))] if shared else []
    up_groups += [(max(top - GROUP + 1, 1), top, everything) for top in range(hops + above, 0, -GROUP)]
    down_groups = [(-below - 1, -below - 1, (part, part))] if shared else []
    down_groups += [(low, min(low + GROUP - 1, hops - 1), everything) for low in range(-below, hops, GROUP)]
    upward, downward = chip(1), chip(-1)

    def up_range(j, g):
        low, top, held = up_groups[g]
        low = max(low, j + 1)
        return (low - j, top - low + 1, held) if low <= top else None

    def down_range(j, g):
        low, top, held = down_groups[g]
        top = min(top, j - 1)
        return (low - j, top - low + 1, held) if low <= top else None

    def send_up(j, g):
        found = up_range(j, g)
        if found is None or j == hops:
            return
        e, count, held = found
        held = pl.ds(*held)
        src = partial.at[0, pl.ds(e, count), held] if j == 0 else up.at[j - 1, pl.ds(e, count), held]
        send(src, up.at[j, pl.ds(e - 1, count), held], up_send.at[j, g], up_recv.at[j, g], upward)

    def send_down(j, g):
        found = down_range(j, g)
        if found is None or j == 0:
            return
        e, count, held = found
        held = pl.ds(*held)
        src = (partial.at[hops] if j == hops else down.at[j]).at[pl.ds(e + ring, count), held]
        dst = down.at[j - 1, pl.ds(e + 1 + ring, count), held]
        send(src, dst, down_send.at[j - 1, g], down_recv.at[j - 1, g], downward)

    most = max(len(up_groups), len(down_groups))
    for g in range(most):
        if g < len(up_groups):
            send_up(0, g)
        if g < len(down_groups):
            send_down(hops, g)

    contributions(1)

    per_owner = chunk_rows // rows

    def deliver(total, slot, j, e, start=0):
        owners = range(start // per_owner, (start + total.shape[0]) // per_owner)
        for a in owners:
            piece = total[a * per_owner - start : (a + 1) * per_owner - start]
            ready[slot, a] = jnp.concatenate([piece[:, :LANES], piece[:, LANES:]], axis=0)
        dst = landed.at[lax.rem(here - j + blocks, blocks)]
        for d in owners:
            if e:
                where = {"tm_0": d, "tm_1": lax.rem(z + e + ring, ring)}
                send(ready.at[slot, d], dst, last_send.at[slot, d], last_recv, where)
                continue
            owner = lax.rem(x + d, rows)
            src = ready.at[slot, owner]
            if d == 0:
                pltpu.make_async_copy(src, dst, last_recv).start()
            else:
                send(src, dst, last_send.at[slot, d], last_recv, {"tm_0": owner})

    def wait_for(ref, sem):
        pltpu.make_async_copy(ref, ref, sem).wait()

    def arrive_up(j, g):
        arrived = up_range(j - 1, g)
        if arrived is None:
            return
        e, count, held = arrived
        e, span = e - 1, pl.ds(*held)
        wait_for(up.at[j - 1, pl.ds(e, count), span], up_recv.at[j - 1, g])
        for c in range(e, e + count):
            if c > 0:
                total = up[j - 1, c, span] + partial[j, c, span]
                if j < hops:
                    up[j - 1, c, span] = total
                else:
                    deliver(total, c + hops + below, j, c, held[0])
        send_up(j, g)

    def arrive_down(i, g):
        arrived = down_range(i + 1, g)
        if arrived is None:
            return
        e, count, held = arrived
        e, span = e + 1, pl.ds(*held)
        wait_for(down.at[i, pl.ds(e + ring, count), span], down_recv.at[i, g])
        for c in range(e, e + count):
            if c < 0:
                total = down[i, c + ring, span] + partial[i, c + ring, span]
                if i > 0:
                    down[i, c + ring, span] = total
                else:
                    deliver(total, (c + below + ring) % ring, 0, c, held[0])
        send_down(i, g)

    def template_spectra():
        templ_copy.wait()
        for copy in table_copies[:3]:
            copy.wait()
        count = out_ref.shape[1]
        short = templ_ref.shape[0] // count
        templates = [templ_ref[pl.ds(i, short, stride=count), :] for i in range(count)]
        templ_spec[...] = forward(templates, first_half_ref[...], twiddle_ref[...], second_ref[...])
        for i in range(count):
            energy = jnp.sqrt(jnp.sum(templates[i] * templates[i], keepdims=True) + 1e-06)
            gain[pl.ds(i, 1), :] = jnp.broadcast_to(1.0 / (scale * energy), (1, LANES))

    for step in range(1, hops + 1):
        j, i = step, hops - step
        for g in range(most):
            if g < len(up_groups):
                arrive_up(j, g)
            if g < len(down_groups):
                arrive_down(i, g)
            if g == min(2, most - 1):
                if step + 1 <= hops // 2:
                    contributions(step + 1)
                elif step == hops // 2:
                    template_spectra()
        for at in [j, i] if j > i else [j] if j == i else []:
            total = partial[at, 0]
            if at > 0:
                total = total + up[at - 1, 0]
            if at < hops:
                total = total + down[at, ring]
            deliver(total, at + below, at, 0)

    for swap in swaps:
        swap.wait_send()
    for copy in sends:
        copy.wait_send()
    for copy in table_copies[3:]:
        copy.wait()
    wait_for(landed, last_recv)

    count = out_ref.shape[1]
    long = blocks * 2
    flat = landed.reshape(long * count, LANES)
    half = twiddle_ref.shape[1]
    series = [flat[pl.ds(i, long, stride=count), :] for i in range(count)]
    twiddle = twiddle_ref[...]
    spec = forward(series, first_ref[...], twiddle, second_ref[...])
    sr, si, hr, hi = spec[:, :LANES], spec[:, LANES:], templ_spec[:, :LANES], templ_spec[:, LANES:]
    product = jnp.concatenate([sr * hr + si * hi, si * hr - sr * hi], axis=1)
    back = dot3(split(product), (third_ref[0], third_ref[1]))
    for i in range(count):
        re, im = back[i * half : (i + 1) * half, :LANES], back[i * half : (i + 1) * half, LANES:]
        turned = jnp.concatenate([re * twiddle[0] + im * twiddle[1], im * twiddle[0] - re * twiddle[1]], axis=0)
        lags = dot3((fourth_ref[0], fourth_ref[1]), split(turned))
        out_ref[:, i, :] = lags * gain[pl.ds(i, 1), :]


def fourier_tables(length, lag_count):
    blocks = length // LANES
    kept = blocks // 2 + 1
    half = -(-kept // 8) * 8
    f1 = np.arange(half)
    n1 = np.arange(blocks)
    n2 = np.arange(LANES)
    live = (f1 < kept)[:, None]
    angle = 2.0 * np.pi * ((f1[:, None] * n1[None, :]) % blocks) / blocks
    first = np.concatenate([np.cos(angle) * live, -np.sin(angle) * live])
    turn = 2.0 * np.pi * ((f1[:, None] * n2[None, :]) % length) / length
    twiddle = np.stack([np.cos(turn) * live, -np.sin(turn) * live]).astype(np.float32)
    inner = 2.0 * np.pi * ((n2[:, None] * n2[None, :]) % LANES) / LANES
    c, s = np.cos(inner), np.sin(inner)
    second = np.block([[c, -s], [s, c]])
    third = np.block([[c, s], [-s, c]])
    weight = np.where((f1 == 0) | (f1 == kept - 1), 1.0, 2.0) * (f1 < kept) / length
    lag_rows = lag_count // LANES
    back = angle.T[:lag_rows]
    fourth = np.concatenate([np.cos(back) * weight, -np.sin(back) * weight], axis=1)
    return (
        split_constant(first),
        split_constant(first[:, :lag_rows]),
        jnp.asarray(twiddle),
        split_constant(second),
        split_constant(third),
        split_constant(fourth),
    )


def on_device(traces, templates, moveouts, masks):
    rows, ring = lax.axis_size("tm_0"), lax.axis_size("tm_1")
    channels, samples = traces.shape
    length = samples * rows * ring * 2
    count, lag_count = templates.shape
    chip_samples = 2 * samples
    hops = (length // 8) // chip_samples
    outside = ring - 1 - hops
    above = below = outside // 2
    shared = outside % 2
    cfg = (rows, ring, hops, above, below, shared)
    chunk = (rows * count, chip_samples)
    lag_rows = lag_count // LANES
    tiles = templates.reshape(count, lag_rows, LANES).transpose(1, 0, 2).reshape(lag_rows * count, LANES)
    tables = fourier_tables(length, lag_count)
    groups = -(-(hops + above) // GROUP) + shared
    vmem = pl.BlockSpec(memory_space=pltpu.VMEM)
    anywhere = pl.BlockSpec(memory_space=pl.ANY)
    dma = pltpu.SemaphoreType.DMA
    half = tables[2].shape[1]
    found = pl.pallas_call(
        functools.partial(matched_kernel, cfg, math.sqrt(channels)),
        out_shape=jax.ShapeDtypeStruct((lag_rows, count, LANES), jnp.float32),
        in_specs=[anywhere] * (4 + len(tables)),
        out_specs=vmem,
        scratch_shapes=[
            pltpu.VMEM((channels, samples), jnp.float32),
            pltpu.VMEM((channels // LANES, LANES), jnp.int32),
            pltpu.VMEM((2, channels, samples), jnp.float32),
            pltpu.VMEM((rows, ring, 2 * count, channels), jnp.int32),
            pltpu.VMEM((ring, rows * count, channels), jnp.bfloat16),
            pltpu.VMEM((2, 2, channels, samples), jnp.bfloat16),
            pltpu.VMEM((channels, samples), jnp.bfloat16),
            pltpu.VMEM((2, channels, chip_samples), jnp.bfloat16),
            pltpu.VMEM((hops + 1, ring, *chunk), jnp.float32),
            pltpu.VMEM((hops, ring, *chunk), jnp.float32),
            pltpu.VMEM((hops, ring + 1, *chunk), jnp.float32),
            pltpu.VMEM((ring, rows, 2 * count, LANES), jnp.float32),
            pltpu.VMEM((rows * ring, 2 * count, LANES), jnp.float32),
            pltpu.VMEM(tiles.shape, jnp.float32),
            *[pltpu.VMEM(t.shape, t.dtype) for t in tables],
            pltpu.VMEM((count * half, 2 * LANES), jnp.float32),
            pltpu.VMEM((count, LANES), jnp.float32),
            dma((4 + PIECES + len(tables),)),
            dma((PIECES,)),
            dma((PIECES,)),
            dma((hops, groups)),
            dma((hops, groups)),
            dma((hops, groups)),
            dma((hops, groups)),
            dma((ring, rows)),
            dma,
        ],
        compiler_params=pltpu.CompilerParams(collective_id=0, has_side_effects=True),
    )(
        traces,
        masks.reshape(rows, ring, 2 * count, channels),
        moveouts.reshape(channels // LANES, LANES),
        tiles,
        *tables,
    )
    return found.transpose(1, 0, 2).reshape(count, lag_count)


def solution(mesh):
    finer = Mesh(mesh.devices.reshape(mesh.shape["grp"], 4, -1, 2), ("grp", "tm_0", "tm_1", "tm_2"))
    axes = ("tm_0", "tm_1", "tm_2")
    return jax.shard_map(
        on_device,
        mesh=finer,
        in_specs=(P("grp", axes), P(axes, None), P("grp"), P(None, "grp")),
        out_specs=P(axes, "grp"),
        check_vma=False,
    )
```

```python
import functools
import math

import jax
import jax.numpy as jnp
import numpy as np
from jax import lax
from jax.experimental import pallas as pl
from jax.experimental.pallas import tpu as pltpu
from jax.sharding import Mesh
from jax.sharding import PartitionSpec as P

MESH = pl.DeviceIdType.MESH
LANES = 128
GROUP = 1
PIECES = 4


def split(value):
    high = value.astype(jnp.bfloat16)
    low = (value - high.astype(jnp.float32)).astype(jnp.bfloat16)
    return high, low


def split_constant(value):
    value = np.asarray(value, np.float64).astype(np.float32)
    high = value.astype(jnp.bfloat16)
    low = (value - high.astype(np.float32)).astype(jnp.bfloat16)
    return jnp.asarray(np.stack([high, low]))


def mm(a, b):
    return jnp.dot(a, b, preferred_element_type=jnp.float32)


def dot3(left, right):
    (left_hi, left_lo), (right_hi, right_lo) = left, right
    return mm(left_hi, right_hi) + (mm(left_hi, right_lo) + mm(left_lo, right_hi))


def forward(series, first, twiddle, second):
    half = twiddle.shape[1]
    turned = []
    for s in series:
        y = dot3((first[0], first[1]), split(s))
        re, im = y[:half], y[half:]
        turned.append(
            jnp.concatenate([re * twiddle[0] - im * twiddle[1], re * twiddle[1] + im * twiddle[0]], axis=1)
        )
    return dot3(split(jnp.concatenate(turned, axis=0)), (second[0], second[1]))


def matched_kernel(
    cfg, scale,
    x_hbm, masks_hbm, mo_hbm, templ_hbm, first_hbm, first_half_hbm, twiddle_hbm, second_hbm, third_hbm, fourth_hbm,
    out_ref,
    raw, mo_ref, pair, mask_int, mask_rows, halves, shift_at, parts, partial, up, down, ready, landed,
    templ_ref, first_ref, first_half_ref, twiddle_ref, second_ref, third_ref, fourth_ref, templ_spec, gain,
    load_sem, pair_send, pair_recv, up_send, up_recv, down_send, down_recv, last_send, last_recv,
):
    rows, ring, hops, above, below, shared = cfg
    channels = x_hbm.shape[0]
    blocks = rows * ring
    x = lax.axis_index("tm_0")
    z = lax.axis_index("tm_1")
    core = lax.axis_index("tm_2")
    here = x * ring + z
    partner = {"tm_2": 1 - core}

    def chip(step):
        other = lax.rem(here + step + blocks, blocks)
        return {"tm_0": other // ring, "tm_1": lax.rem(other, ring)}

    loads = []

    def load(src, dst):
        copy = pltpu.make_async_copy(src, dst, load_sem.at[len(loads)])
        copy.start()
        loads.append(copy)
        return copy

    per_piece = channels // PIECES
    mo_copy = load(mo_hbm, mo_ref)
    x_copies = [load(x_hbm.at[pl.ds(p * per_piece, per_piece)], raw.at[pl.ds(p * per_piece, per_piece)]) for p in range(PIECES)]

    barrier = pltpu.get_barrier_semaphore()
    pl.semaphore_signal(barrier, inc=1, device_id=partner, device_id_type=MESH)
    peers = [chip(1), chip(-1)] + [{"tm_0": lax.rem(x + d, rows)} for d in range(1, rows)]
    for where in peers:
        pl.semaphore_signal(barrier, inc=1, device_id=where, device_id_type=MESH)

    mask_copy = load(masks_hbm, mask_int)
    templ_copy = load(templ_hbm, templ_ref)
    table_copies = [
        load(first_half_hbm, first_half_ref),
        load(twiddle_hbm, twiddle_ref),
        load(second_hbm, second_ref),
        load(first_hbm, first_ref),
        load(third_hbm, third_ref),
        load(fourth_hbm, fourth_ref),
    ]

    lane = lax.broadcasted_iota(jnp.int32, (LANES, LANES), 1)
    mo_copy.wait()
    swaps = []
    for p in range(PIECES):
        x_copies[p].wait()

        @pl.loop(p * per_piece // LANES, (p + 1) * per_piece // LANES)
        def _(b):
            at = pl.ds(pl.multiple_of(b * LANES, LANES), LANES)
            spread = jnp.broadcast_to(mo_ref[pl.ds(b, 1), :].astype(jnp.float32), (LANES, LANES))
            move = jnp.transpose(spread).astype(jnp.int32)
            index = lane + (move & (LANES - 1))
            value = jnp.take_along_axis(raw[at, :], index & (LANES - 1), axis=1)
            pair[core, at, :] = value
            passed = (index >= LANES).astype(jnp.int32)
            shift_at[at, :] = ((move >> (LANES.bit_length() - 1)) + passed).astype(jnp.float32).astype(jnp.bfloat16)
            high, low = split(value)
            halves[0, core, at, :] = high
            halves[1, core, at, :] = low

        if p == 0:
            pl.semaphore_wait(barrier, 1 + len(peers))
        half = pair.at[core, pl.ds(p * per_piece, per_piece)]
        swap = pltpu.make_async_remote_copy(
            src_ref=half, dst_ref=half, send_sem=pair_send.at[p], recv_sem=pair_recv.at[p],
            device_id=partner, device_id_type=MESH,
        )
        swap.start()
        swaps.append(swap)

    mask_copy.wait()
    tile_rows = mask_int.shape[2]
    half_tile = tile_rows // 2
    tops = lax.broadcasted_iota(jnp.int32, (tile_rows, channels), 0) < half_tile

    def pick(first, second):
        moved = pltpu.roll(jnp.where(core == 0, second, first), half_tile, 0)
        kept = jnp.where(core == 0, first, second)
        return jnp.where(tops == (core == 0), kept, moved)

    @pl.loop(0, ring)
    def _(e):
        owner = lax.rem(z + e, ring)
        pieces = [
            pick(mask_int[a, owner], mask_int[a + 1, owner]).astype(jnp.float32) for a in range(0, rows, 2)
        ]
        mask_rows[e] = jnp.concatenate(pieces, axis=0).astype(jnp.bfloat16)

    for p in range(PIECES):
        swaps[p].wait_recv()

        @pl.loop(p * per_piece // LANES, (p + 1) * per_piece // LANES)
        def _(b):
            at = pl.ds(pl.multiple_of(b * LANES, LANES), LANES)
            high, low = split(pair[1 - core, at, :])
            halves[0, 1 - core, at, :] = high
            halves[1, 1 - core, at, :] = low

    zero = jnp.zeros((LANES, LANES), jnp.bfloat16)

    def contribution(j):
        twice = jnp.broadcast_to((2 * j).astype(jnp.float32), (LANES, LANES))
        before, same, after = ((twice + d).astype(jnp.bfloat16) for d in (-1, 0, 1))

        @pl.loop(0, channels // LANES)
        def _(b):
            at = pl.ds(pl.multiple_of(b * LANES, LANES), LANES)
            shift = shift_at[at, :]
            is_before, is_same, is_after = shift == before, shift == same, shift == after
            for t in range(2):
                first, second = halves[t, 0, at, :], halves[t, 1, at, :]
                parts[t, at, :LANES] = jnp.where(is_same, first, jnp.where(is_after, second, zero))
                parts[t, at, LANES:] = jnp.where(is_before, first, jnp.where(is_same, second, zero))

        weights = mask_rows[...].reshape(-1, channels)
        total = mm(weights, parts[0]) + mm(weights, parts[1])
        partial[j] = total.reshape(partial.shape[1:])

    def contributions(s):
        if s == hops - s:
            contribution(jnp.int32(s))
        else:
            @pl.loop(0, 2)
            def _(t):
                contribution(s + t * (hops - 2 * s))

    contributions(0)

    sent = {"up": 0, "down": 0, "last": 0}
    slots = {"up": {}, "down": {}}

    def slot_of(name, j, g):
        return slots[name].setdefault((j, g), len(slots[name]))

    def send(name, src, dst, send_sem, recv_sem, where):
        pltpu.make_async_remote_copy(
            src_ref=src, dst_ref=dst, send_sem=send_sem, recv_sem=recv_sem, device_id=where, device_id_type=MESH
        ).start()
        sent[name] += math.prod(src.shape)

    chunk_rows = partial.shape[2]
    part = chunk_rows // 2
    everything = (0, chunk_rows)
    up_groups = [(hops + above + 1, hops + above + 1, (0, part))] if shared else []
    up_groups += [(max(top - GROUP + 1, 1), top, everything) for top in range(hops + above, 0, -GROUP)]
    down_groups = [(-below - 1, -below - 1, (part, part))] if shared else []
    down_groups += [(low, min(low + GROUP - 1, hops - 1), everything) for low in range(-below, hops, GROUP)]
    upward, downward = chip(1), chip(-1)

    def up_range(j, g):
        low, top, held = up_groups[g]
        low = max(low, j + 1)
        return (low - j, top - low + 1, held) if low <= top else None

    def down_range(j, g):
        low, top, held = down_groups[g]
        top = min(top, j - 1)
        return (low - j, top - low + 1, held) if low <= top else None

    def send_up(j, g):
        found = up_range(j, g)
        if found is None or j == hops:
            return
        e, count, held = found
        held = pl.ds(*held)
        src = partial.at[0, pl.ds(e, count), held] if j == 0 else up.at[j - 1, pl.ds(e, count), held]
        send("up", src, up.at[j, pl.ds(e - 1, count), held], up_send, up_recv.at[slot_of("up", j, g)], upward)

    def send_down(j, g):
        found = down_range(j, g)
        if found is None or j == 0:
            return
        e, count, held = found
        held = pl.ds(*held)
        src = (partial.at[hops] if j == hops else down.at[j]).at[pl.ds(e + ring, count), held]
        dst = down.at[j - 1, pl.ds(e + 1 + ring, count), held]
        send("down", src, dst, down_send, down_recv.at[slot_of("down", j - 1, g)], downward)

    most = max(len(up_groups), len(down_groups))
    for g in range(most):
        if g < len(up_groups):
            send_up(0, g)
        if g < len(down_groups):
            send_down(hops, g)

    contributions(1)

    def template_spectra():
        templ_copy.wait()
        for copy in table_copies[:3]:
            copy.wait()
        count = out_ref.shape[1]
        short = templ_ref.shape[0] // count
        templates = [templ_ref[pl.ds(i, short, stride=count), :] for i in range(count)]
        templ_spec[...] = forward(templates, first_half_ref[...], twiddle_ref[...], second_ref[...])
        for i in range(count):
            energy = jnp.sqrt(jnp.sum(templates[i] * templates[i], keepdims=True) + 1e-06)
            gain[pl.ds(i, 1), :] = jnp.broadcast_to(1.0 / (scale * energy), (1, LANES))

    template_spectra()

    per_owner = chunk_rows // rows

    def deliver(total, slot, j, e, start=0):
        owners = range(start // per_owner, (start + total.shape[0]) // per_owner)
        for a in owners:
            piece = total[a * per_owner - start : (a + 1) * per_owner - start]
            ready[slot, a] = jnp.concatenate([piece[:, :LANES], piece[:, LANES:]], axis=0)
        dst = landed.at[lax.rem(here - j + blocks, blocks)]
        for d in owners:
            if e:
                where = {"tm_0": d, "tm_1": lax.rem(z + e + ring, ring)}
                send("last", ready.at[slot, d], dst, last_send, last_recv, where)
                continue
            owner = lax.rem(x + d, rows)
            src = ready.at[slot, owner]
            if d == 0:
                pltpu.make_async_copy(src, dst, last_recv).start()
            else:
                send("last", src, dst, last_send, last_recv, {"tm_0": owner})

    def wait_for(ref, sem):
        pltpu.make_async_copy(ref, ref, sem).wait()

    def arrive_up(j, g):
        arrived = up_range(j - 1, g)
        if arrived is None:
            return
        e, count, held = arrived
        e, span = e - 1, pl.ds(*held)
        wait_for(up.at[j - 1, pl.ds(e, count), span], up_recv.at[slot_of("up", j - 1, g)])
        for c in range(e, e + count):
            if c > 0:
                total = up[j - 1, c, span] + partial[j, c, span]
                if j < hops:
                    up[j - 1, c, span] = total
                else:
                    deliver(total, c + hops + below, j, c, held[0])
        send_up(j, g)

    def arrive_down(i, g):
        arrived = down_range(i + 1, g)
        if arrived is None:
            return
        e, count, held = arrived
        e, span = e + 1, pl.ds(*held)
        wait_for(down.at[i, pl.ds(e + ring, count), span], down_recv.at[slot_of("down", i, g)])
        for c in range(e, e + count):
            if c < 0:
                total = down[i, c + ring, span] + partial[i, c + ring, span]
                if i > 0:
                    down[i, c + ring, span] = total
                else:
                    deliver(total, (c + below + ring) % ring, 0, c, held[0])
        send_down(i, g)

    for step in range(1, hops + 1):
        j, i = step, hops - step
        for g in range(most):
            if g < len(up_groups):
                arrive_up(j, g)
            if g < len(down_groups):
                arrive_down(i, g)
            if g == min(2, most - 1):
                if step + 1 <= hops // 2:
                    contributions(step + 1)
        for at in [j, i] if j > i else [j] if j == i else []:
            total = partial[at, 0]
            if at > 0:
                total = total + up[at - 1, 0]
            if at < hops:
                total = total + down[at, ring]
            deliver(total, at + below, at, 0)

    for swap in swaps:
        swap.wait_send()
    chunk = math.prod(partial.shape[2:])
    stripes = (hops * ring, *partial.shape[2:])
    wait_for(up.reshape(stripes).at[pl.ds(0, sent["up"] // chunk)], up_send)
    wait_for(up.reshape(stripes).at[pl.ds(0, sent["down"] // chunk)], down_send)
    wait_for(landed.at[pl.ds(0, sent["last"] // math.prod(landed.shape[1:]))], last_send)
    for copy in table_copies[3:]:
        copy.wait()
    wait_for(landed, last_recv)

    count = out_ref.shape[1]
    long = blocks * 2
    flat = landed.reshape(long * count, LANES)
    half = twiddle_ref.shape[1]
    series = [flat[pl.ds(i, long, stride=count), :] for i in range(count)]
    twiddle = twiddle_ref[...]
    spec = forward(series, first_ref[...], twiddle, second_ref[...])
    sr, si, hr, hi = spec[:, :LANES], spec[:, LANES:], templ_spec[:, :LANES], templ_spec[:, LANES:]
    product = jnp.concatenate([sr * hr + si * hi, si * hr - sr * hi], axis=1)
    back = dot3(split(product), (third_ref[0], third_ref[1]))
    for i in range(count):
        re, im = back[i * half : (i + 1) * half, :LANES], back[i * half : (i + 1) * half, LANES:]
        turned = jnp.concatenate([re * twiddle[0] + im * twiddle[1], im * twiddle[0] - re * twiddle[1]], axis=0)
        lags = dot3((fourth_ref[0], fourth_ref[1]), split(turned))
        out_ref[:, i, :] = lags * gain[pl.ds(i, 1), :]


def fourier_tables(length, lag_count):
    blocks = length // LANES
    kept = blocks // 2 + 1
    half = -(-kept // 8) * 8
    f1 = np.arange(half)
    n1 = np.arange(blocks)
    n2 = np.arange(LANES)
    live = (f1 < kept)[:, None]
    angle = 2.0 * np.pi * ((f1[:, None] * n1[None, :]) % blocks) / blocks
    first = np.concatenate([np.cos(angle) * live, -np.sin(angle) * live])
    turn = 2.0 * np.pi * ((f1[:, None] * n2[None, :]) % length) / length
    twiddle = np.stack([np.cos(turn) * live, -np.sin(turn) * live]).astype(np.float32)
    inner = 2.0 * np.pi * ((n2[:, None] * n2[None, :]) % LANES) / LANES
    c, s = np.cos(inner), np.sin(inner)
    second = np.block([[c, -s], [s, c]])
    third = np.block([[c, s], [-s, c]])
    weight = np.where((f1 == 0) | (f1 == kept - 1), 1.0, 2.0) * (f1 < kept) / length
    lag_rows = lag_count // LANES
    back = angle.T[:lag_rows]
    fourth = np.concatenate([np.cos(back) * weight, -np.sin(back) * weight], axis=1)
    return (
        split_constant(first),
        split_constant(first[:, :lag_rows]),
        jnp.asarray(twiddle),
        split_constant(second),
        split_constant(third),
        split_constant(fourth),
    )


def on_device(traces, templates, moveouts, masks):
    rows, ring = lax.axis_size("tm_0"), lax.axis_size("tm_1")
    channels, samples = traces.shape
    length = samples * rows * ring * 2
    count, lag_count = templates.shape
    chip_samples = 2 * samples
    hops = (length // 8) // chip_samples
    outside = ring - 1 - hops
    above = below = outside // 2
    shared = outside % 2
    cfg = (rows, ring, hops, above, below, shared)
    chunk = (rows * count, chip_samples)
    lag_rows = lag_count // LANES
    tiles = templates.reshape(count, lag_rows, LANES).transpose(1, 0, 2).reshape(lag_rows * count, LANES)
    tables = fourier_tables(length, lag_count)
    messages = sum(min(top, hops) for top in range(hops + above, 0, -GROUP)) + shared * hops
    vmem = pl.BlockSpec(memory_space=pltpu.VMEM)
    anywhere = pl.BlockSpec(memory_space=pl.ANY)
    dma = pltpu.SemaphoreType.DMA
    half = tables[2].shape[1]
    found = pl.pallas_call(
        functools.partial(matched_kernel, cfg, math.sqrt(channels)),
        out_shape=jax.ShapeDtypeStruct((lag_rows, count, LANES), jnp.float32),
        in_specs=[anywhere] * (4 + len(tables)),
        out_specs=vmem,
        scratch_shapes=[
            pltpu.VMEM((channels, samples), jnp.float32),
            pltpu.VMEM((channels // LANES, LANES), jnp.int32),
            pltpu.VMEM((2, channels, samples), jnp.float32),
            pltpu.VMEM((rows, ring, 2 * count, channels), jnp.int32),
            pltpu.VMEM((ring, rows * count, channels), jnp.bfloat16),
            pltpu.VMEM((2, 2, channels, samples), jnp.bfloat16),
            pltpu.VMEM((channels, samples), jnp.bfloat16),
            pltpu.VMEM((2, channels, chip_samples), jnp.bfloat16),
            pltpu.VMEM((hops + 1, ring, *chunk), jnp.float32),
            pltpu.VMEM((hops, ring, *chunk), jnp.float32),
            pltpu.VMEM((hops, ring + 1, *chunk), jnp.float32),
            pltpu.VMEM((ring, rows, 2 * count, LANES), jnp.float32),
            pltpu.VMEM((rows * ring, 2 * count, LANES), jnp.float32),
            pltpu.VMEM(tiles.shape, jnp.float32),
            *[pltpu.VMEM(t.shape, t.dtype) for t in tables],
            pltpu.VMEM((count * half, 2 * LANES), jnp.float32),
            pltpu.VMEM((count, LANES), jnp.float32),
            dma((4 + PIECES + len(tables),)),
            dma((PIECES,)),
            dma((PIECES,)),
            dma,
            dma((messages,)),
            dma,
            dma((messages,)),
            dma,
            dma,
        ],
        compiler_params=pltpu.CompilerParams(collective_id=0, has_side_effects=True),
    )(
        traces,
        masks.reshape(rows, ring, 2 * count, channels),
        moveouts.reshape(channels // LANES, LANES),
        tiles,
        *tables,
    )
    return found.transpose(1, 0, 2).reshape(count, lag_count)


def solution(mesh):
    finer = Mesh(mesh.devices.reshape(mesh.shape["grp"], 4, -1, 2), ("grp", "tm_0", "tm_1", "tm_2"))
    axes = ("tm_0", "tm_1", "tm_2")
    return jax.shard_map(
        on_device,
        mesh=finer,
        in_specs=(P("grp", axes), P(axes, None), P("grp"), P(None, "grp")),
        out_specs=P(axes, "grp"),
        check_vma=False,
    )
```

```python
import functools
import math

import jax
import jax.numpy as jnp
import numpy as np
from jax import lax
from jax.experimental import pallas as pl
from jax.experimental.pallas import tpu as pltpu
from jax.sharding import Mesh
from jax.sharding import PartitionSpec as P

MESH = pl.DeviceIdType.MESH
LANES = 128
GROUP = 1
PIECES = 4


def split(value):
    high = value.astype(jnp.bfloat16)
    low = (value - high.astype(jnp.float32)).astype(jnp.bfloat16)
    return high, low


def split_constant(value):
    value = np.asarray(value, np.float64).astype(np.float32)
    high = value.astype(jnp.bfloat16)
    low = (value - high.astype(np.float32)).astype(jnp.bfloat16)
    return jnp.asarray(np.stack([high, low]))


def mm(a, b):
    return jnp.dot(a, b, preferred_element_type=jnp.float32)


def dot3(left, right):
    (left_hi, left_lo), (right_hi, right_lo) = left, right
    return mm(left_hi, right_hi) + (mm(left_hi, right_lo) + mm(left_lo, right_hi))


def forward(series, first, twiddle, second):
    half = twiddle.shape[1]
    turned = []
    for s in series:
        y = dot3((first[0], first[1]), split(s))
        re, im = y[:half], y[half:]
        turned.append(
            jnp.concatenate([re * twiddle[0] - im * twiddle[1], re * twiddle[1] + im * twiddle[0]], axis=1)
        )
    return dot3(split(jnp.concatenate(turned, axis=0)), (second[0], second[1]))


def matched_kernel(
    cfg, scale,
    x_hbm, masks_hbm, mo_hbm, templ_hbm, first_hbm, first_half_hbm, twiddle_hbm, second_hbm, third_hbm, fourth_hbm,
    out_ref,
    raw, mo_ref, pair, mask_int, mask_rows, halves, shift_at, parts, partial, flow, merge, ready, landed,
    templ_ref, first_ref, first_half_ref, twiddle_ref, second_ref, third_ref, fourth_ref, templ_spec, gain,
    load_sem, pair_send, pair_recv, flow_send, flow_recv, merge_send, merge_recv, last_send, last_recv,
):
    rows, ring, hops, outside, shared = cfg
    channels = x_hbm.shape[0]
    blocks = rows * ring
    x = lax.axis_index("tm_0")
    z = lax.axis_index("tm_1")
    core = lax.axis_index("tm_2")
    toward = 1 - 2 * core
    here = x * ring + z
    partner = {"tm_2": 1 - core}

    def chip(step):
        other = lax.rem(here + step + blocks, blocks)
        return {"tm_0": other // ring, "tm_1": lax.rem(other, ring)}

    def window_place(s):
        return core * hops + toward * s

    def wait_for(ref, sem):
        pltpu.make_async_copy(ref, ref, sem).wait()

    loads = []

    def load(src, dst):
        copy = pltpu.make_async_copy(src, dst, load_sem.at[len(loads)])
        copy.start()
        loads.append(copy)
        return copy

    per_piece = channels // PIECES
    mo_copy = load(mo_hbm, mo_ref)
    x_copies = [load(x_hbm.at[pl.ds(p * per_piece, per_piece)], raw.at[pl.ds(p * per_piece, per_piece)]) for p in range(PIECES)]

    barrier = pltpu.get_barrier_semaphore()
    peers = [partner, chip(1), chip(-1)]
    for d in range(1, rows):
        peers += [{"tm_0": lax.rem(x + d, rows), "tm_2": c} for c in (core, 1 - core)]
    for where in peers:
        pl.semaphore_signal(barrier, inc=1, device_id=where, device_id_type=MESH)

    mask_copy = load(masks_hbm, mask_int)
    templ_copy = load(templ_hbm, templ_ref)
    table_copies = [
        load(first_half_hbm, first_half_ref),
        load(twiddle_hbm, twiddle_ref),
        load(second_hbm, second_ref),
        load(first_hbm, first_ref),
        load(third_hbm, third_ref),
        load(fourth_hbm, fourth_ref),
    ]

    lane = lax.broadcasted_iota(jnp.int32, (LANES, LANES), 1)
    mo_copy.wait()
    swaps = []
    for p in range(PIECES):
        x_copies[p].wait()

        @pl.loop(p * per_piece // LANES, (p + 1) * per_piece // LANES)
        def _(b):
            at = pl.ds(pl.multiple_of(b * LANES, LANES), LANES)
            spread = jnp.broadcast_to(mo_ref[pl.ds(b, 1), :].astype(jnp.float32), (LANES, LANES))
            move = jnp.transpose(spread).astype(jnp.int32)
            index = lane + (move & (LANES - 1))
            value = jnp.take_along_axis(raw[at, :], index & (LANES - 1), axis=1)
            pair[core, at, :] = value
            passed = (index >= LANES).astype(jnp.int32)
            shift_at[at, :] = ((move >> (LANES.bit_length() - 1)) + passed).astype(jnp.float32).astype(jnp.bfloat16)
            high, low = split(value)
            halves[0, core, at, :] = high
            halves[1, core, at, :] = low

        if p == 0:
            pl.semaphore_wait(barrier, len(peers))
        half = pair.at[core, pl.ds(p * per_piece, per_piece)]
        swap = pltpu.make_async_remote_copy(
            src_ref=half, dst_ref=half, send_sem=pair_send.at[p], recv_sem=pair_recv.at[p],
            device_id=partner, device_id_type=MESH,
        )
        swap.start()
        swaps.append(swap)

    mask_copy.wait()
    tile_rows = mask_int.shape[2]
    per_owner = tile_rows // 2
    own_rows = rows * per_owner
    chunk_rows = 2 * own_rows
    tops = lax.broadcasted_iota(jnp.int32, (tile_rows, channels), 0) < per_owner

    def pick(first, second, side):
        moved = pltpu.roll(jnp.where(side == 0, second, first), per_owner, 0)
        kept = jnp.where(side == 0, first, second)
        return jnp.where(tops == (side == 0), kept, moved).astype(jnp.float32)

    @pl.loop(0, mask_rows.shape[0])
    def _(m):
        owner = lax.rem(z + toward * m + ring, ring)
        tiles = [mask_int[a, owner] for a in range(rows)]
        pieces = [pick(tiles[a], tiles[a + 1], side) for side in (core, 1 - core) for a in range(0, rows, 2)]
        mask_rows[m] = jnp.concatenate(pieces, axis=0).astype(jnp.bfloat16)

    for p in range(PIECES):
        swaps[p].wait_recv()

        @pl.loop(p * per_piece // LANES, (p + 1) * per_piece // LANES)
        def _(b):
            at = pl.ds(pl.multiple_of(b * LANES, LANES), LANES)
            high, low = split(pair[1 - core, at, :])
            halves[0, 1 - core, at, :] = high
            halves[1, 1 - core, at, :] = low

    zero = jnp.zeros((LANES, LANES), jnp.bfloat16)
    top = hops + outside

    def contribution(s):
        twice = jnp.broadcast_to((2 * window_place(s)).astype(jnp.float32), (LANES, LANES))
        before, same, after = ((twice + d).astype(jnp.bfloat16) for d in (-1, 0, 1))

        @pl.loop(0, channels // LANES)
        def _(b):
            at = pl.ds(pl.multiple_of(b * LANES, LANES), LANES)
            shift = shift_at[at, :]
            is_before, is_same, is_after = shift == before, shift == same, shift == after
            for t in range(2):
                first, second = halves[t, 0, at, :], halves[t, 1, at, :]
                parts[t, at, :LANES] = jnp.where(is_same, first, jnp.where(is_after, second, zero))
                parts[t, at, LANES:] = jnp.where(is_before, first, jnp.where(is_same, second, zero))

        full = top - s + 1
        weights = mask_rows[pl.ds(0, full)].reshape(full * chunk_rows, channels)
        if shared:
            weights = jnp.concatenate([weights, mask_rows[full, pl.ds(0, own_rows)]], axis=0)
        total = mm(weights, parts[0]) + mm(weights, parts[1])
        partial[s, pl.ds(0, full)] = total[: full * chunk_rows].reshape(full, chunk_rows, 2 * LANES)
        if shared:
            partial[s, full, pl.ds(0, own_rows)] = total[full * chunk_rows :]

    contribution(0)

    sent = {"flow": 0, "merge": 0, "last": 0}
    slots = {}

    def slot_of(s, g):
        return slots.setdefault((s, g), len(slots))

    def send(name, src, dst, send_sem, recv_sem, where):
        pltpu.make_async_remote_copy(
            src_ref=src, dst_ref=dst, send_sem=send_sem, recv_sem=recv_sem, device_id=where, device_id_type=MESH
        ).start()
        sent[name] += math.prod(src.shape)

    groups = [(top + 1, top + 1, own_rows)] if shared else []
    groups += [(max(high - GROUP + 1, 1), high, chunk_rows) for high in range(top, 0, -GROUP)]
    onward = chip(toward)

    def span(s, g):
        low, high, held = groups[g]
        low = max(low, s + 1)
        return (low - s, high - low + 1, pl.ds(0, held)) if low <= high and s < hops else None

    def send_on(s, g):
        found = span(s, g)
        if found is None:
            return
        m, count, held = found
        src = partial.at[0, pl.ds(m, count), held] if s == 0 else flow.at[s - 1, pl.ds(m, count), held]
        dst = flow.at[s, pl.ds(m - 1, count), held]
        send("flow", src, dst, flow_send, flow_recv.at[slot_of(s, g)], onward)

    for g in range(len(groups)):
        send_on(0, g)

    def template_spectra():
        templ_copy.wait()
        for copy in table_copies[:3]:
            copy.wait()
        count = out_ref.shape[1]
        short = templ_ref.shape[0] // count
        templates = [templ_ref[pl.ds(i, short, stride=count), :] for i in range(count)]
        templ_spec[...] = forward(templates, first_half_ref[...], twiddle_ref[...], second_ref[...])
        for i in range(count):
            energy = jnp.sqrt(jnp.sum(templates[i] * templates[i], keepdims=True) + 1e-06)
            gain[pl.ds(i, 1), :] = jnp.broadcast_to(1.0 / (scale * energy), (1, LANES))

    contribution(1)
    contribution(2)
    template_spectra()
    todo = list(range(3, hops + 1))

    def deliver(total, s, m, sides):
        slot = s + m
        for side in range(sides):
            for a in range(rows):
                start = side * own_rows + a * per_owner
                piece = total[start : start + per_owner]
                ready[slot, side, a] = jnp.concatenate([piece[:, :LANES], piece[:, LANES:]], axis=0)
        dst = landed.at[lax.rem(here - window_place(s) + blocks, blocks)]
        for side in range(sides):
            cores = core if side == 0 else 1 - core
            for d in range(rows):
                if m:
                    src, where = ready.at[slot, side, d], {"tm_0": d, "tm_1": lax.rem(z + toward * m + ring, ring)}
                else:
                    owner = lax.rem(x + d, rows)
                    src, where = ready.at[slot, side, owner], {"tm_0": owner}
                if m == 0 and side == 0 and d == 0:
                    pltpu.make_async_copy(src, dst, last_recv).start()
                else:
                    send("last", src, dst, last_send, last_recv, {**where, "tm_2": cores})

    def merge_and_deliver(s):
        wait_for(merge.at[s], merge_recv.at[s])
        own = pl.ds(0, own_rows)
        deliver(flow[s - 1, 0, own] + partial[s, 0, own] + merge[s], s, 0, 1)

    def arrive(s, g):
        arrived = span(s - 1, g)
        if arrived is None:
            return
        m, count, held = arrived
        m = m - 1
        wait_for(flow.at[s - 1, pl.ds(m, count), held], flow_recv.at[slot_of(s - 1, g)])
        for c in reversed(range(m, m + count)):
            if s == hops:
                deliver(flow[s - 1, c, held] + partial[s, c, held], s, c, held.size // own_rows)
            elif c > 0:
                flow[s - 1, c, held] = flow[s - 1, c, held] + partial[s, c, held]
            else:
                src = flow.at[s - 1, 0, pl.ds(own_rows, own_rows)]
                send("merge", src, merge.at[hops - s], merge_send, merge_recv.at[hops - s], partner)
        send_on(s, g)

    for s in range(1, hops + 1):
        if s == hops and hops % 2 == 0:
            merge_and_deliver(hops // 2)
        for g in range(len(groups)):
            arrive(s, g)
            if todo and g in (2, 6):
                contribution(todo.pop(0))
        if hops < 2 * s < 2 * hops:
            merge_and_deliver(s)
    for s in range((hops - 1) // 2, 0, -1):
        merge_and_deliver(s)

    for swap in swaps:
        swap.wait_send()
    wait_for(flow.reshape(-1, chunk_rows, 2 * LANES).at[pl.ds(0, sent["flow"] // math.prod(flow.shape[2:]))], flow_send)
    wait_for(merge.at[pl.ds(0, sent["merge"] // math.prod(merge.shape[1:]))], merge_send)
    wait_for(landed.at[pl.ds(0, sent["last"] // math.prod(landed.shape[1:]))], last_send)
    for copy in table_copies[3:]:
        copy.wait()
    wait_for(landed, last_recv)

    count = out_ref.shape[1]
    long = blocks * 2
    flat = landed.reshape(long * count, LANES)
    half = twiddle_ref.shape[1]
    series = [flat[pl.ds(i, long, stride=count), :] for i in range(count)]
    twiddle = twiddle_ref[...]
    spec = forward(series, first_ref[...], twiddle, second_ref[...])
    sr, si, hr, hi = spec[:, :LANES], spec[:, LANES:], templ_spec[:, :LANES], templ_spec[:, LANES:]
    product = jnp.concatenate([sr * hr + si * hi, si * hr - sr * hi], axis=1)
    back = dot3(split(product), (third_ref[0], third_ref[1]))
    for i in range(count):
        re, im = back[i * half : (i + 1) * half, :LANES], back[i * half : (i + 1) * half, LANES:]
        turned = jnp.concatenate([re * twiddle[0] + im * twiddle[1], im * twiddle[0] - re * twiddle[1]], axis=0)
        lags = dot3((fourth_ref[0], fourth_ref[1]), split(turned))
        out_ref[:, i, :] = lags * gain[pl.ds(i, 1), :]


def fourier_tables(length, lag_count):
    blocks = length // LANES
    kept = blocks // 2 + 1
    half = -(-kept // 8) * 8
    f1 = np.arange(half)
    n1 = np.arange(blocks)
    n2 = np.arange(LANES)
    live = (f1 < kept)[:, None]
    angle = 2.0 * np.pi * ((f1[:, None] * n1[None, :]) % blocks) / blocks
    first = np.concatenate([np.cos(angle) * live, -np.sin(angle) * live])
    turn = 2.0 * np.pi * ((f1[:, None] * n2[None, :]) % length) / length
    twiddle = np.stack([np.cos(turn) * live, -np.sin(turn) * live]).astype(np.float32)
    inner = 2.0 * np.pi * ((n2[:, None] * n2[None, :]) % LANES) / LANES
    c, s = np.cos(inner), np.sin(inner)
    second = np.block([[c, -s], [s, c]])
    third = np.block([[c, s], [-s, c]])
    weight = np.where((f1 == 0) | (f1 == kept - 1), 1.0, 2.0) * (f1 < kept) / length
    lag_rows = lag_count // LANES
    back = angle.T[:lag_rows]
    fourth = np.concatenate([np.cos(back) * weight, -np.sin(back) * weight], axis=1)
    return (
        split_constant(first),
        split_constant(first[:, :lag_rows]),
        jnp.asarray(twiddle),
        split_constant(second),
        split_constant(third),
        split_constant(fourth),
    )


def on_device(traces, templates, moveouts, masks):
    rows, ring = lax.axis_size("tm_0"), lax.axis_size("tm_1")
    channels, samples = traces.shape
    length = samples * rows * ring * 2
    count, lag_count = templates.shape
    chip_samples = 2 * samples
    hops = (length // 8) // chip_samples
    outside, shared = divmod(ring - 1 - hops, 2)
    top = hops + outside
    cfg = (rows, ring, hops, outside, shared)
    chunk = (2 * rows * count, chip_samples)
    lag_rows = lag_count // LANES
    tiles = templates.reshape(count, lag_rows, LANES).transpose(1, 0, 2).reshape(lag_rows * count, LANES)
    tables = fourier_tables(length, lag_count)
    messages = sum(min(high, hops) for high in range(top, 0, -GROUP)) + shared * hops
    vmem = pl.BlockSpec(memory_space=pltpu.VMEM)
    anywhere = pl.BlockSpec(memory_space=pl.ANY)
    dma = pltpu.SemaphoreType.DMA
    half = tables[2].shape[1]
    found = pl.pallas_call(
        functools.partial(matched_kernel, cfg, math.sqrt(channels)),
        out_shape=jax.ShapeDtypeStruct((lag_rows, count, LANES), jnp.float32),
        in_specs=[anywhere] * (4 + len(tables)),
        out_specs=vmem,
        scratch_shapes=[
            pltpu.VMEM((channels, samples), jnp.float32),
            pltpu.VMEM((channels // LANES, LANES), jnp.int32),
            pltpu.VMEM((2, channels, samples), jnp.float32),
            pltpu.VMEM((rows, ring, 2 * count, channels), jnp.int32),
            pltpu.VMEM((top + 1 + shared, 2 * rows * count, channels), jnp.bfloat16),
            pltpu.VMEM((2, 2, channels, samples), jnp.bfloat16),
            pltpu.VMEM((channels, samples), jnp.bfloat16),
            pltpu.VMEM((2, channels, chip_samples), jnp.bfloat16),
            pltpu.VMEM((hops + 1, top + 1 + shared, *chunk), jnp.float32),
            pltpu.VMEM((hops, top + shared, *chunk), jnp.float32),
            pltpu.VMEM((hops, rows * count, chip_samples), jnp.float32),
            pltpu.VMEM((top + 1 + shared, 2, rows, 2 * count, LANES), jnp.float32),
            pltpu.VMEM((rows * ring, 2 * count, LANES), jnp.float32),
            pltpu.VMEM(tiles.shape, jnp.float32),
            *[pltpu.VMEM(t.shape, t.dtype) for t in tables],
            pltpu.VMEM((count * half, 2 * LANES), jnp.float32),
            pltpu.VMEM((count, LANES), jnp.float32),
            dma((4 + PIECES + len(tables),)),
            dma((PIECES,)),
            dma((PIECES,)),
            dma,
            dma((messages,)),
            dma,
            dma((hops,)),
            dma,
            dma,
        ],
        compiler_params=pltpu.CompilerParams(collective_id=0, has_side_effects=True),
    )(
        traces,
        masks.reshape(rows, ring, 2 * count, channels),
        moveouts.reshape(channels // LANES, LANES),
        tiles,
        *tables,
    )
    return found.transpose(1, 0, 2).reshape(count, lag_count)


def solution(mesh):
    finer = Mesh(mesh.devices.reshape(mesh.shape["grp"], 4, -1, 2), ("grp", "tm_0", "tm_1", "tm_2"))
    axes = ("tm_0", "tm_1", "tm_2")
    return jax.shard_map(
        on_device,
        mesh=finer,
        in_specs=(P("grp", axes), P(axes, None), P("grp"), P(None, "grp")),
        out_specs=P(axes, "grp"),
        check_vma=False,
    )
```

```python
import functools
import math

import jax
import jax.numpy as jnp
import numpy as np
from jax import lax
from jax.experimental import pallas as pl
from jax.experimental.pallas import tpu as pltpu
from jax.sharding import Mesh
from jax.sharding import PartitionSpec as P

MESH = pl.DeviceIdType.MESH
LANES = 128
GROUP = 1
PIECES = 4


def split(value):
    high = value.astype(jnp.bfloat16)
    low = (value - high.astype(jnp.float32)).astype(jnp.bfloat16)
    return high, low


def split_constant(value):
    value = np.asarray(value, np.float64).astype(np.float32)
    high = value.astype(jnp.bfloat16)
    low = (value - high.astype(np.float32)).astype(jnp.bfloat16)
    return jnp.asarray(np.stack([high, low]))


def mm(a, b):
    return jnp.dot(a, b, preferred_element_type=jnp.float32)


def dot3(left, right):
    (left_hi, left_lo), (right_hi, right_lo) = left, right
    return mm(left_hi, right_hi) + (mm(left_hi, right_lo) + mm(left_lo, right_hi))


def forward(series, first, twiddle, second):
    half = twiddle.shape[1]
    turned = []
    for s in series:
        y = dot3((first[0], first[1]), split(s))
        re, im = y[:half], y[half:]
        turned.append(
            jnp.concatenate([re * twiddle[0] - im * twiddle[1], re * twiddle[1] + im * twiddle[0]], axis=1)
        )
    return dot3(split(jnp.concatenate(turned, axis=0)), (second[0], second[1]))


def matched_kernel(
    cfg, scale,
    x_hbm, masks_hbm, mo_hbm, templ_hbm, first_hbm, first_half_hbm, twiddle_hbm, second_hbm, third_hbm, fourth_hbm,
    out_ref,
    raw, mo_ref, pair, mask_int, mask_rows, halves, shift_at, parts, partial, flow, merge, ready, landed,
    templ_ref, first_ref, first_half_ref, twiddle_ref, second_ref, third_ref, fourth_ref, templ_spec, gain,
    load_sem, pair_send, pair_recv, flow_send, flow_recv, merge_send, merge_recv, last_send, last_recv,
):
    rows, ring, hops, outside, shared = cfg
    channels = x_hbm.shape[0]
    blocks = rows * ring
    x = lax.axis_index("tm_0")
    z = lax.axis_index("tm_1")
    core = lax.axis_index("tm_2")
    toward = 1 - 2 * core
    here = x * ring + z
    partner = {"tm_2": 1 - core}

    def chip(step):
        other = lax.rem(here + step + blocks, blocks)
        return {"tm_0": other // ring, "tm_1": lax.rem(other, ring)}

    def window_place(s):
        return core * hops + toward * s

    def wait_for(ref, sem):
        pltpu.make_async_copy(ref, ref, sem).wait()

    loads = []

    def load(src, dst):
        copy = pltpu.make_async_copy(src, dst, load_sem.at[len(loads)])
        copy.start()
        loads.append(copy)
        return copy

    per_piece = channels // PIECES
    mo_copy = load(mo_hbm, mo_ref)
    x_copies = [load(x_hbm.at[pl.ds(p * per_piece, per_piece)], raw.at[pl.ds(p * per_piece, per_piece)]) for p in range(PIECES)]

    barrier = pltpu.get_barrier_semaphore()
    peers = [partner, chip(1), chip(-1)]
    for d in range(1, rows):
        peers += [{"tm_0": lax.rem(x + d, rows), "tm_2": c} for c in (core, 1 - core)]
    for where in peers:
        pl.semaphore_signal(barrier, inc=1, device_id=where, device_id_type=MESH)

    mask_copy = load(masks_hbm, mask_int)
    templ_copy = load(templ_hbm, templ_ref)
    table_copies = [
        load(first_half_hbm, first_half_ref),
        load(twiddle_hbm, twiddle_ref),
        load(second_hbm, second_ref),
        load(first_hbm, first_ref),
        load(third_hbm, third_ref),
        load(fourth_hbm, fourth_ref),
    ]

    lane = lax.broadcasted_iota(jnp.int32, (LANES, LANES), 1)
    mo_copy.wait()
    swaps = []
    for p in range(PIECES):
        x_copies[p].wait()

        @pl.loop(p * per_piece // LANES, (p + 1) * per_piece // LANES)
        def _(b):
            at = pl.ds(pl.multiple_of(b * LANES, LANES), LANES)
            spread = jnp.broadcast_to(mo_ref[pl.ds(b, 1), :].astype(jnp.float32), (LANES, LANES))
            move = jnp.transpose(spread).astype(jnp.int32)
            index = lane + (move & (LANES - 1))
            value = jnp.take_along_axis(raw[at, :], index & (LANES - 1), axis=1)
            pair[core, at, :] = value
            passed = (index >= LANES).astype(jnp.int32)
            shift_at[at, :] = ((move >> (LANES.bit_length() - 1)) + passed).astype(jnp.float32).astype(jnp.bfloat16)
            high, low = split(value)
            halves[0, core, at, :] = high
            halves[1, core, at, :] = low

        if p == 0:
            pl.semaphore_wait(barrier, len(peers))
        half = pair.at[core, pl.ds(p * per_piece, per_piece)]
        swap = pltpu.make_async_remote_copy(
            src_ref=half, dst_ref=half, send_sem=pair_send.at[p], recv_sem=pair_recv.at[p],
            device_id=partner, device_id_type=MESH,
        )
        swap.start()
        swaps.append(swap)

    mask_copy.wait()
    tile_rows = mask_int.shape[2]
    per_owner = tile_rows // 2
    own_rows = rows * per_owner
    chunk_rows = 2 * own_rows
    tops = lax.broadcasted_iota(jnp.int32, (tile_rows, channels), 0) < per_owner

    def pick(first, second, side):
        moved = pltpu.roll(jnp.where(side == 0, second, first), per_owner, 0)
        kept = jnp.where(side == 0, first, second)
        return jnp.where(tops == (side == 0), kept, moved).astype(jnp.float32)

    @pl.loop(0, mask_rows.shape[0] // chunk_rows)
    def _(m):
        owner = lax.rem(z + toward * m + ring, ring)
        tiles = [mask_int[a, owner] for a in range(rows)]
        pieces = [pick(tiles[a], tiles[a + 1], side) for side in (core, 1 - core) for a in range(0, rows, 2)]
        kept = jnp.concatenate(pieces, axis=0).astype(jnp.bfloat16)
        at = pl.ds(pl.multiple_of(m * chunk_rows, chunk_rows), chunk_rows)
        mask_rows[at, :channels] = kept
        mask_rows[at, channels:] = kept

    for p in range(PIECES):
        swaps[p].wait_recv()

        @pl.loop(p * per_piece // LANES, (p + 1) * per_piece // LANES)
        def _(b):
            at = pl.ds(pl.multiple_of(b * LANES, LANES), LANES)
            high, low = split(pair[1 - core, at, :])
            halves[0, 1 - core, at, :] = high
            halves[1, 1 - core, at, :] = low

    zero = jnp.zeros((LANES, LANES), jnp.bfloat16)
    top = hops + outside

    def contribution(s):
        twice = jnp.broadcast_to((2 * window_place(s)).astype(jnp.float32), (LANES, LANES))
        before, same, after = ((twice + d).astype(jnp.bfloat16) for d in (-1, 0, 1))

        @pl.loop(0, channels // LANES)
        def _(b):
            at = pl.ds(pl.multiple_of(b * LANES, LANES), LANES)
            shift = shift_at[at, :]
            is_before, is_same, is_after = shift == before, shift == same, shift == after
            for t in range(2):
                first, second = halves[t, 0, at, :], halves[t, 1, at, :]
                to = pl.ds(pl.multiple_of(t * channels + b * LANES, LANES), LANES)
                parts[to, :LANES] = jnp.where(is_same, first, jnp.where(is_after, second, zero))
                parts[to, LANES:] = jnp.where(is_before, first, jnp.where(is_same, second, zero))

        live = pl.ds(0, (top - s + 1) * chunk_rows + shared * own_rows)
        partial[s, live] = mm(mask_rows[live], parts[...])

    contribution(0)

    sent = {"flow": 0, "merge": 0, "last": 0}
    slots = {}

    def slot_of(s, g):
        return slots.setdefault((s, g), len(slots))

    def send(name, src, dst, send_sem, recv_sem, where):
        pltpu.make_async_remote_copy(
            src_ref=src, dst_ref=dst, send_sem=send_sem, recv_sem=recv_sem, device_id=where, device_id_type=MESH
        ).start()
        sent[name] += math.prod(src.shape)

    groups = [(top + 1, top + 1, own_rows)] if shared else []
    groups += [(max(high - GROUP + 1, 1), high, chunk_rows) for high in range(top, 0, -GROUP)]
    onward = chip(toward)

    def chunks(m, count, held):
        return pl.ds(m * chunk_rows, (count - 1) * chunk_rows + held)

    def span(s, g):
        low, high, held = groups[g]
        low = max(low, s + 1)
        return (low - s, high - low + 1, held) if low <= high and s < hops else None

    def send_on(s, g):
        found = span(s, g)
        if found is None:
            return
        m, count, held = found
        src = (partial.at[0] if s == 0 else flow.at[s - 1]).at[chunks(m, count, held)]
        dst = flow.at[s, chunks(m - 1, count, held)]
        send("flow", src, dst, flow_send, flow_recv.at[slot_of(s, g)], onward)

    for g in range(len(groups)):
        send_on(0, g)

    def template_spectra():
        templ_copy.wait()
        for copy in table_copies[:3]:
            copy.wait()
        count = out_ref.shape[1]
        short = templ_ref.shape[0] // count
        templates = [templ_ref[pl.ds(i, short, stride=count), :] for i in range(count)]
        templ_spec[...] = forward(templates, first_half_ref[...], twiddle_ref[...], second_ref[...])
        for i in range(count):
            energy = jnp.sqrt(jnp.sum(templates[i] * templates[i], keepdims=True) + 1e-06)
            gain[pl.ds(i, 1), :] = jnp.broadcast_to(1.0 / (scale * energy), (1, LANES))

    contribution(1)
    contribution(2)
    template_spectra()
    todo = list(range(3, hops + 1))

    def deliver(total, s, m, sides):
        slot = s + m
        for side in range(sides):
            for a in range(rows):
                start = side * own_rows + a * per_owner
                piece = total[start : start + per_owner]
                ready[slot, side, a] = jnp.concatenate([piece[:, :LANES], piece[:, LANES:]], axis=0)
        dst = landed.at[lax.rem(here - window_place(s) + blocks, blocks)]
        for side in range(sides):
            cores = core if side == 0 else 1 - core
            for d in range(rows):
                if m:
                    src, where = ready.at[slot, side, d], {"tm_0": d, "tm_1": lax.rem(z + toward * m + ring, ring)}
                else:
                    owner = lax.rem(x + d, rows)
                    src, where = ready.at[slot, side, owner], {"tm_0": owner}
                if m == 0 and side == 0 and d == 0:
                    pltpu.make_async_copy(src, dst, last_recv).start()
                else:
                    send("last", src, dst, last_send, last_recv, {**where, "tm_2": cores})

    def merge_and_deliver(s):
        wait_for(merge.at[s], merge_recv.at[s])
        own = pl.ds(0, own_rows)
        deliver(flow[s - 1, own] + partial[s, own] + merge[s], s, 0, 1)

    def arrive(s, g):
        arrived = span(s - 1, g)
        if arrived is None:
            return
        m, count, held = arrived
        m = m - 1
        wait_for(flow.at[s - 1, chunks(m, count, held)], flow_recv.at[slot_of(s - 1, g)])
        for c in reversed(range(m, m + count)):
            at = chunks(c, 1, held)
            if s == hops:
                deliver(flow[s - 1, at] + partial[s, at], s, c, held // own_rows)
            elif c > 0:
                flow[s - 1, at] = flow[s - 1, at] + partial[s, at]
            else:
                src = flow.at[s - 1, pl.ds(own_rows, own_rows)]
                send("merge", src, merge.at[hops - s], merge_send, merge_recv.at[hops - s], partner)
        send_on(s, g)

    for s in range(1, hops + 1):
        if s == hops and hops % 2 == 0:
            merge_and_deliver(hops // 2)
        for g in range(len(groups)):
            arrive(s, g)
            if todo and g in (2, 6):
                contribution(todo.pop(0))
        if hops < 2 * s < 2 * hops:
            merge_and_deliver(s)
    for s in range((hops - 1) // 2, 0, -1):
        merge_and_deliver(s)

    for swap in swaps:
        swap.wait_send()
    flat = flow.reshape(-1, 2 * LANES)
    wait_for(flat.at[pl.ds(0, sent["flow"] // (2 * LANES))], flow_send)
    wait_for(merge.at[pl.ds(0, sent["merge"] // math.prod(merge.shape[1:]))], merge_send)
    wait_for(landed.at[pl.ds(0, sent["last"] // math.prod(landed.shape[1:]))], last_send)
    for copy in table_copies[3:]:
        copy.wait()
    wait_for(landed, last_recv)

    count = out_ref.shape[1]
    long = blocks * 2
    flat = landed.reshape(long * count, LANES)
    half = twiddle_ref.shape[1]
    series = [flat[pl.ds(i, long, stride=count), :] for i in range(count)]
    twiddle = twiddle_ref[...]
    spec = forward(series, first_ref[...], twiddle, second_ref[...])
    sr, si, hr, hi = spec[:, :LANES], spec[:, LANES:], templ_spec[:, :LANES], templ_spec[:, LANES:]
    product = jnp.concatenate([sr * hr + si * hi, si * hr - sr * hi], axis=1)
    back = dot3(split(product), (third_ref[0], third_ref[1]))
    for i in range(count):
        re, im = back[i * half : (i + 1) * half, :LANES], back[i * half : (i + 1) * half, LANES:]
        turned = jnp.concatenate([re * twiddle[0] + im * twiddle[1], im * twiddle[0] - re * twiddle[1]], axis=0)
        lags = dot3((fourth_ref[0], fourth_ref[1]), split(turned))
        out_ref[:, i, :] = lags * gain[pl.ds(i, 1), :]


def fourier_tables(length, lag_count):
    blocks = length // LANES
    kept = blocks // 2 + 1
    half = -(-kept // 8) * 8
    f1 = np.arange(half)
    n1 = np.arange(blocks)
    n2 = np.arange(LANES)
    live = (f1 < kept)[:, None]
    angle = 2.0 * np.pi * ((f1[:, None] * n1[None, :]) % blocks) / blocks
    first = np.concatenate([np.cos(angle) * live, -np.sin(angle) * live])
    turn = 2.0 * np.pi * ((f1[:, None] * n2[None, :]) % length) / length
    twiddle = np.stack([np.cos(turn) * live, -np.sin(turn) * live]).astype(np.float32)
    inner = 2.0 * np.pi * ((n2[:, None] * n2[None, :]) % LANES) / LANES
    c, s = np.cos(inner), np.sin(inner)
    second = np.block([[c, -s], [s, c]])
    third = np.block([[c, s], [-s, c]])
    weight = np.where((f1 == 0) | (f1 == kept - 1), 1.0, 2.0) * (f1 < kept) / length
    lag_rows = lag_count // LANES
    back = angle.T[:lag_rows]
    fourth = np.concatenate([np.cos(back) * weight, -np.sin(back) * weight], axis=1)
    return (
        split_constant(first),
        split_constant(first[:, :lag_rows]),
        jnp.asarray(twiddle),
        split_constant(second),
        split_constant(third),
        split_constant(fourth),
    )


def on_device(traces, templates, moveouts, masks):
    rows, ring = lax.axis_size("tm_0"), lax.axis_size("tm_1")
    channels, samples = traces.shape
    length = samples * rows * ring * 2
    count, lag_count = templates.shape
    chip_samples = 2 * samples
    hops = (length // 8) // chip_samples
    outside, shared = divmod(ring - 1 - hops, 2)
    top = hops + outside
    cfg = (rows, ring, hops, outside, shared)
    chunk = (2 * rows * count, chip_samples)
    lag_rows = lag_count // LANES
    tiles = templates.reshape(count, lag_rows, LANES).transpose(1, 0, 2).reshape(lag_rows * count, LANES)
    tables = fourier_tables(length, lag_count)
    messages = sum(min(high, hops) for high in range(top, 0, -GROUP)) + shared * hops
    vmem = pl.BlockSpec(memory_space=pltpu.VMEM)
    anywhere = pl.BlockSpec(memory_space=pl.ANY)
    dma = pltpu.SemaphoreType.DMA
    half = tables[2].shape[1]
    found = pl.pallas_call(
        functools.partial(matched_kernel, cfg, math.sqrt(channels)),
        out_shape=pltpu.VMEM((lag_rows, count, LANES), jnp.float32),
        in_specs=[anywhere] * (4 + len(tables)),
        out_specs=vmem,
        scratch_shapes=[
            pltpu.VMEM((channels, samples), jnp.float32),
            pltpu.VMEM((channels // LANES, LANES), jnp.int32),
            pltpu.VMEM((2, channels, samples), jnp.float32),
            pltpu.VMEM((rows, ring, 2 * count, channels), jnp.int32),
            pltpu.VMEM(((top + 1 + shared) * chunk[0], 2 * channels), jnp.bfloat16),
            pltpu.VMEM((2, 2, channels, samples), jnp.bfloat16),
            pltpu.VMEM((channels, samples), jnp.bfloat16),
            pltpu.VMEM((2 * channels, chip_samples), jnp.bfloat16),
            pltpu.VMEM((hops + 1, (top + 1 + shared) * chunk[0], chunk[1]), jnp.float32),
            pltpu.VMEM((hops, (top + shared) * chunk[0], chunk[1]), jnp.float32),
            pltpu.VMEM((hops, rows * count, chip_samples), jnp.float32),
            pltpu.VMEM((top + 1 + shared, 2, rows, 2 * count, LANES), jnp.float32),
            pltpu.VMEM((rows * ring, 2 * count, LANES), jnp.float32),
            pltpu.VMEM(tiles.shape, jnp.float32),
            *[pltpu.VMEM(t.shape, t.dtype) for t in tables],
            pltpu.VMEM((count * half, 2 * LANES), jnp.float32),
            pltpu.VMEM((count, LANES), jnp.float32),
            dma((4 + PIECES + len(tables),)),
            dma((PIECES,)),
            dma((PIECES,)),
            dma,
            dma((messages,)),
            dma,
            dma((hops,)),
            dma,
            dma,
        ],
        compiler_params=pltpu.CompilerParams(collective_id=0, has_side_effects=True),
    )(
        traces,
        masks.reshape(rows, ring, 2 * count, channels),
        moveouts.reshape(channels // LANES, LANES),
        tiles,
        *tables,
    )
    return found.transpose(1, 0, 2).reshape(count, lag_count)


def solution(mesh):
    finer = Mesh(mesh.devices.reshape(mesh.shape["grp"], 4, -1, 2), ("grp", "tm_0", "tm_1", "tm_2"))
    axes = ("tm_0", "tm_1", "tm_2")
    return jax.shard_map(
        on_device,
        mesh=finer,
        in_specs=(P("grp", axes), P(axes, None), P("grp"), P(None, "grp")),
        out_specs=P(axes, "grp"),
        check_vma=False,
    )
```

```python
import functools
import math

import jax
import jax.numpy as jnp
import numpy as np
from jax import lax
from jax.experimental import pallas as pl
from jax.experimental.pallas import tpu as pltpu
from jax.sharding import Mesh
from jax.sharding import PartitionSpec as P

MESH = pl.DeviceIdType.MESH
LANES = 128
GROUP = 1
PIECES = 4


def split(value):
    high = value.astype(jnp.bfloat16)
    low = (value - high.astype(jnp.float32)).astype(jnp.bfloat16)
    return high, low


def split_constant(value):
    value = np.asarray(value, np.float64).astype(np.float32)
    high = value.astype(jnp.bfloat16)
    low = (value - high.astype(np.float32)).astype(jnp.bfloat16)
    return jnp.asarray(np.stack([high, low]))


def mm(a, b):
    return jnp.dot(a, b, preferred_element_type=jnp.float32)


def dot3(left, right):
    (left_hi, left_lo), (right_hi, right_lo) = left, right
    lefts = jnp.concatenate([left_hi, left_hi, left_lo], axis=1)
    return mm(lefts, jnp.concatenate([right_hi, right_lo, right_hi], axis=0))


def forward(series, first, twiddle, second):
    half = twiddle.shape[1]
    turned = []
    for s in series:
        y = dot3((first[0], first[1]), split(s))
        re, im = y[:half], y[half:]
        turned.append(
            jnp.concatenate([re * twiddle[0] - im * twiddle[1], re * twiddle[1] + im * twiddle[0]], axis=1)
        )
    return dot3(split(jnp.concatenate(turned, axis=0)), (second[0], second[1]))


def matched_kernel(
    cfg, scale,
    x_hbm, masks_hbm, mo_hbm, templ_hbm, first_hbm, first_half_hbm, twiddle_hbm, second_hbm, third_hbm, fourth_hbm,
    out_ref,
    raw, mo_ref, pair, mask_int, mask_rows, halves, shift_at, parts, partial, flow, merge, ready, landed,
    templ_ref, first_ref, first_half_ref, twiddle_ref, second_ref, third_ref, fourth_ref, templ_spec, gain,
    load_sem, pair_send, pair_recv, flow_send, flow_recv, merge_send, merge_recv, last_send, last_recv,
):
    rows, ring, hops, outside, shared = cfg
    channels = x_hbm.shape[0]
    blocks = rows * ring
    x = lax.axis_index("tm_0")
    z = lax.axis_index("tm_1")
    core = lax.axis_index("tm_2")
    toward = 1 - 2 * core
    here = x * ring + z
    partner = {"tm_2": 1 - core}

    def chip(step):
        other = lax.rem(here + step + blocks, blocks)
        return {"tm_0": other // ring, "tm_1": lax.rem(other, ring)}

    def window_place(s):
        return core * hops + toward * s

    def wait_for(ref, sem):
        pltpu.make_async_copy(ref, ref, sem).wait()

    loads = []

    def load(src, dst):
        copy = pltpu.make_async_copy(src, dst, load_sem.at[len(loads)])
        copy.start()
        loads.append(copy)
        return copy

    per_piece = channels // PIECES
    mo_copy = load(mo_hbm, mo_ref)
    x_copies = [load(x_hbm.at[pl.ds(p * per_piece, per_piece)], raw.at[pl.ds(p * per_piece, per_piece)]) for p in range(PIECES)]

    barrier = pltpu.get_barrier_semaphore()
    peers = [partner, chip(1), chip(-1)]
    for d in range(1, rows):
        peers += [{"tm_0": lax.rem(x + d, rows), "tm_2": c} for c in (core, 1 - core)]
    for where in peers:
        pl.semaphore_signal(barrier, inc=1, device_id=where, device_id_type=MESH)

    mask_copy = load(masks_hbm, mask_int)
    templ_copy = load(templ_hbm, templ_ref)
    table_copies = [
        load(first_half_hbm, first_half_ref),
        load(twiddle_hbm, twiddle_ref),
        load(second_hbm, second_ref),
        load(first_hbm, first_ref),
        load(third_hbm, third_ref),
        load(fourth_hbm, fourth_ref),
    ]

    lane = lax.broadcasted_iota(jnp.int32, (LANES, LANES), 1)
    mo_copy.wait()
    for p in range(PIECES):
        x_copies[p].wait()

        @pl.loop(p * per_piece // LANES, (p + 1) * per_piece // LANES, unroll=True)
        def _(b):
            at = pl.ds(pl.multiple_of(b * LANES, LANES), LANES)
            spread = jnp.broadcast_to(mo_ref[pl.ds(b, 1), :].astype(jnp.float32), (LANES, LANES))
            move = jnp.transpose(spread).astype(jnp.int32)
            index = lane + (move & (LANES - 1))
            value = jnp.take_along_axis(raw[at, :], index & (LANES - 1), axis=1)
            pair[core, at, :] = value
            passed = (index >= LANES).astype(jnp.int32)
            shift_at[at, :] = ((move >> (LANES.bit_length() - 1)) + passed).astype(jnp.float32).astype(jnp.bfloat16)
            high, low = split(value)
            halves[0, core, at, :] = high
            halves[1, core, at, :] = low

    pl.semaphore_wait(barrier, len(peers))
    swaps = []
    for p in range(PIECES):
        half = pair.at[core, pl.ds(p * per_piece, per_piece)]
        swap = pltpu.make_async_remote_copy(
            src_ref=half, dst_ref=half, send_sem=pair_send.at[p], recv_sem=pair_recv.at[p],
            device_id=partner, device_id_type=MESH,
        )
        swap.start()
        swaps.append(swap)

    mask_copy.wait()
    tile_rows = mask_int.shape[2]
    per_owner = tile_rows // 2
    own_rows = rows * per_owner
    chunk_rows = 2 * own_rows
    tops = lax.broadcasted_iota(jnp.int32, (tile_rows, channels), 0) < per_owner

    def pick(first, second, side):
        moved = pltpu.roll(jnp.where(side == 0, second, first), per_owner, 0)
        kept = jnp.where(side == 0, first, second)
        return jnp.where(tops == (side == 0), kept, moved).astype(jnp.float32)

    @pl.loop(0, mask_rows.shape[0] // chunk_rows)
    def _(m):
        owner = lax.rem(z + toward * m + ring, ring)
        tiles = [mask_int[a, owner] for a in range(rows)]
        pieces = [pick(tiles[a], tiles[a + 1], side) for side in (core, 1 - core) for a in range(0, rows, 2)]
        kept = jnp.concatenate(pieces, axis=0).astype(jnp.bfloat16)
        at = pl.ds(pl.multiple_of(m * chunk_rows, chunk_rows), chunk_rows)
        mask_rows[at, :channels] = kept
        mask_rows[at, channels:] = kept

    for p in range(PIECES):
        swaps[p].wait_recv()

        @pl.loop(p * per_piece // LANES, (p + 1) * per_piece // LANES)
        def _(b):
            at = pl.ds(pl.multiple_of(b * LANES, LANES), LANES)
            high, low = split(pair[1 - core, at, :])
            halves[0, 1 - core, at, :] = high
            halves[1, 1 - core, at, :] = low

    zero = jnp.zeros((LANES, LANES), jnp.bfloat16)
    top = hops + outside

    def select(s):
        twice = jnp.broadcast_to((2 * window_place(s)).astype(jnp.float32), (LANES, LANES))
        before, same, after = ((twice + d).astype(jnp.bfloat16) for d in (-1, 0, 1))

        @pl.loop(0, channels // LANES)
        def _(b):
            at = pl.ds(pl.multiple_of(b * LANES, LANES), LANES)
            shift = shift_at[at, :]
            is_before, is_same, is_after = shift == before, shift == same, shift == after
            for t in range(2):
                first, second = halves[t, 0, at, :], halves[t, 1, at, :]
                to = pl.ds(pl.multiple_of(t * channels + b * LANES, LANES), LANES)
                parts[to, :LANES] = jnp.where(is_same, first, jnp.where(is_after, second, zero))
                parts[to, LANES:] = jnp.where(is_before, first, jnp.where(is_same, second, zero))

    def multiply(s, low=0, high=None):
        high = (top - s + 1) * chunk_rows + shared * own_rows if high is None else high
        live = pl.ds(low, high - low)
        partial[s, live] = mm(mask_rows[live], parts[...])

    def contribution(s):
        select(s)
        multiply(s)

    select(0)
    halfway = top // 2 + 1
    multiply(0, halfway * chunk_rows)

    sent = {"flow": 0, "merge": 0, "last": 0}
    slots = {}

    def slot_of(s, g):
        return slots.setdefault((s, g), len(slots))

    def send(name, src, dst, send_sem, recv_sem, where):
        pltpu.make_async_remote_copy(
            src_ref=src, dst_ref=dst, send_sem=send_sem, recv_sem=recv_sem, device_id=where, device_id_type=MESH
        ).start()
        sent[name] += math.prod(src.shape)

    groups = [(top + 1, top + 1, own_rows)] if shared else []
    groups += [(max(high - GROUP + 1, 1), high, chunk_rows) for high in range(top, 0, -GROUP)]
    onward = chip(toward)

    def chunks(m, count, held):
        return pl.ds(m * chunk_rows, (count - 1) * chunk_rows + held)

    def span(s, g):
        low, high, held = groups[g]
        low = max(low, s + 1)
        return (low - s, high - low + 1, held) if low <= high and s < hops else None

    def send_on(s, g):
        found = span(s, g)
        if found is None:
            return
        m, count, held = found
        src = (partial.at[0] if s == 0 else flow.at[s - 1]).at[chunks(m, count, held)]
        dst = flow.at[s, chunks(m - 1, count, held)]
        send("flow", src, dst, flow_send, flow_recv.at[slot_of(s, g)], onward)

    for g in range(len(groups)):
        if groups[g][0] < halfway:
            continue
        send_on(0, g)
    multiply(0, chunk_rows, halfway * chunk_rows)
    for g in range(len(groups)):
        if groups[g][0] < halfway:
            send_on(0, g)

    def template_spectra():
        templ_copy.wait()
        for copy in table_copies[:3]:
            copy.wait()
        count = out_ref.shape[1]
        short = templ_ref.shape[0] // count
        templates = [templ_ref[pl.ds(i, short, stride=count), :] for i in range(count)]
        templ_spec[...] = forward(templates, first_half_ref[...], twiddle_ref[...], second_ref[...])
        for i in range(count):
            energy = jnp.sqrt(jnp.sum(templates[i] * templates[i], keepdims=True) + 1e-06)
            gain[pl.ds(i, 1), :] = jnp.broadcast_to(1.0 / (scale * energy), (1, LANES))

    contribution(1)
    contribution(2)
    template_spectra()
    todo = list(range(3, hops + 1))

    def deliver(total, s, m, sides):
        slot = s + m
        for side in range(sides):
            for a in range(rows):
                start = side * own_rows + a * per_owner
                piece = total[start : start + per_owner]
                ready[slot, side, a] = jnp.concatenate([piece[:, :LANES], piece[:, LANES:]], axis=0)
        dst = landed.at[lax.rem(here - window_place(s) + blocks, blocks)]
        for side in range(sides):
            cores = core if side == 0 else 1 - core
            for d in range(rows):
                if m:
                    src, where = ready.at[slot, side, d], {"tm_0": d, "tm_1": lax.rem(z + toward * m + ring, ring)}
                else:
                    owner = lax.rem(x + d, rows)
                    src, where = ready.at[slot, side, owner], {"tm_0": owner}
                if m == 0 and side == 0 and d == 0:
                    pltpu.make_async_copy(src, dst, last_recv).start()
                else:
                    send("last", src, dst, last_send, last_recv, {**where, "tm_2": cores})

    def merge_and_deliver(s):
        wait_for(merge.at[s], merge_recv.at[s])
        own = pl.ds(0, own_rows)
        deliver(flow[s - 1, own] + partial[s, own] + merge[s], s, 0, 1)

    def arrive(s, g):
        arrived = span(s - 1, g)
        if arrived is None:
            return
        m, count, held = arrived
        m = m - 1
        wait_for(flow.at[s - 1, chunks(m, count, held)], flow_recv.at[slot_of(s - 1, g)])
        for c in reversed(range(m, m + count)):
            at = chunks(c, 1, held)
            if s == hops:
                deliver(flow[s - 1, at] + partial[s, at], s, c, held // own_rows)
            elif c > 0:
                flow[s - 1, at] = flow[s - 1, at] + partial[s, at]
            else:
                src = flow.at[s - 1, pl.ds(own_rows, own_rows)]
                send("merge", src, merge.at[hops - s], merge_send, merge_recv.at[hops - s], partner)
        send_on(s, g)

    for s in range(1, hops + 1):
        if s == hops and hops % 2 == 0:
            merge_and_deliver(hops // 2)
        for g in range(len(groups)):
            arrive(s, g)
            if todo and g in (2, 6):
                contribution(todo.pop(0))
        if hops < 2 * s < 2 * hops:
            merge_and_deliver(s)
    for s in range((hops - 1) // 2, 0, -1):
        merge_and_deliver(s)

    for swap in swaps:
        swap.wait_send()
    flat = flow.reshape(-1, 2 * LANES)
    wait_for(flat.at[pl.ds(0, sent["flow"] // (2 * LANES))], flow_send)
    wait_for(merge.at[pl.ds(0, sent["merge"] // math.prod(merge.shape[1:]))], merge_send)
    wait_for(landed.at[pl.ds(0, sent["last"] // math.prod(landed.shape[1:]))], last_send)
    for copy in table_copies[3:]:
        copy.wait()
    wait_for(landed, last_recv)

    count = out_ref.shape[1]
    long = blocks * 2
    flat = landed.reshape(long * count, LANES)
    half = twiddle_ref.shape[1]
    series = [flat[pl.ds(i, long, stride=count), :] for i in range(count)]
    twiddle = twiddle_ref[...]
    spec = forward(series, first_ref[...], twiddle, second_ref[...])
    sr, si, hr, hi = spec[:, :LANES], spec[:, LANES:], templ_spec[:, :LANES], templ_spec[:, LANES:]
    product = jnp.concatenate([sr * hr + si * hi, si * hr - sr * hi], axis=1)
    back = dot3(split(product), (third_ref[0], third_ref[1]))
    for i in range(count):
        re, im = back[i * half : (i + 1) * half, :LANES], back[i * half : (i + 1) * half, LANES:]
        turned = jnp.concatenate([re * twiddle[0] + im * twiddle[1], im * twiddle[0] - re * twiddle[1]], axis=0)
        lags = dot3((fourth_ref[0], fourth_ref[1]), split(turned))
        out_ref[:, i, :] = lags * gain[pl.ds(i, 1), :]


def fourier_tables(length, lag_count):
    blocks = length // LANES
    kept = blocks // 2 + 1
    half = -(-kept // 8) * 8
    f1 = np.arange(half)
    n1 = np.arange(blocks)
    n2 = np.arange(LANES)
    live = (f1 < kept)[:, None]
    angle = 2.0 * np.pi * ((f1[:, None] * n1[None, :]) % blocks) / blocks
    first = np.concatenate([np.cos(angle) * live, -np.sin(angle) * live])
    turn = 2.0 * np.pi * ((f1[:, None] * n2[None, :]) % length) / length
    twiddle = np.stack([np.cos(turn) * live, -np.sin(turn) * live]).astype(np.float32)
    inner = 2.0 * np.pi * ((n2[:, None] * n2[None, :]) % LANES) / LANES
    c, s = np.cos(inner), np.sin(inner)
    second = np.block([[c, -s], [s, c]])
    third = np.block([[c, s], [-s, c]])
    weight = np.where((f1 == 0) | (f1 == kept - 1), 1.0, 2.0) * (f1 < kept) / length
    lag_rows = lag_count // LANES
    back = angle.T[:lag_rows]
    fourth = np.concatenate([np.cos(back) * weight, -np.sin(back) * weight], axis=1)
    return (
        split_constant(first),
        split_constant(first[:, :lag_rows]),
        jnp.asarray(twiddle),
        split_constant(second),
        split_constant(third),
        split_constant(fourth),
    )


def on_device(traces, templates, moveouts, masks):
    rows, ring = lax.axis_size("tm_0"), lax.axis_size("tm_1")
    channels, samples = traces.shape
    length = samples * rows * ring * 2
    count, lag_count = templates.shape
    chip_samples = 2 * samples
    hops = (length // 8) // chip_samples
    outside, shared = divmod(ring - 1 - hops, 2)
    top = hops + outside
    cfg = (rows, ring, hops, outside, shared)
    chunk = (2 * rows * count, chip_samples)
    lag_rows = lag_count // LANES
    tiles = templates.reshape(count, lag_rows, LANES).transpose(1, 0, 2).reshape(lag_rows * count, LANES)
    tables = fourier_tables(length, lag_count)
    messages = sum(min(high, hops) for high in range(top, 0, -GROUP)) + shared * hops
    vmem = pl.BlockSpec(memory_space=pltpu.VMEM)
    anywhere = pl.BlockSpec(memory_space=pl.ANY)
    dma = pltpu.SemaphoreType.DMA
    half = tables[2].shape[1]
    found = pl.pallas_call(
        functools.partial(matched_kernel, cfg, math.sqrt(channels)),
        out_shape=pltpu.VMEM((lag_rows, count, LANES), jnp.float32),
        in_specs=[anywhere] * (4 + len(tables)),
        out_specs=vmem,
        scratch_shapes=[
            pltpu.VMEM((channels, samples), jnp.float32),
            pltpu.VMEM((channels // LANES, LANES), jnp.int32),
            pltpu.VMEM((2, channels, samples), jnp.float32),
            pltpu.VMEM((rows, ring, 2 * count, channels), jnp.int32),
            pltpu.VMEM(((top + 1 + shared) * chunk[0], 2 * channels), jnp.bfloat16),
            pltpu.VMEM((2, 2, channels, samples), jnp.bfloat16),
            pltpu.VMEM((channels, samples), jnp.bfloat16),
            pltpu.VMEM((2 * channels, chip_samples), jnp.bfloat16),
            pltpu.VMEM((hops + 1, (top + 1 + shared) * chunk[0], chunk[1]), jnp.float32),
            pltpu.VMEM((hops, (top + shared) * chunk[0], chunk[1]), jnp.float32),
            pltpu.VMEM((hops, rows * count, chip_samples), jnp.float32),
            pltpu.VMEM((top + 1 + shared, 2, rows, 2 * count, LANES), jnp.float32),
            pltpu.VMEM((rows * ring, 2 * count, LANES), jnp.float32),
            pltpu.VMEM(tiles.shape, jnp.float32),
            *[pltpu.VMEM(t.shape, t.dtype) for t in tables],
            pltpu.VMEM((count * half, 2 * LANES), jnp.float32),
            pltpu.VMEM((count, LANES), jnp.float32),
            dma((4 + PIECES + len(tables),)),
            dma((PIECES,)),
            dma((PIECES,)),
            dma,
            dma((messages,)),
            dma,
            dma((hops,)),
            dma,
            dma,
        ],
        compiler_params=pltpu.CompilerParams(collective_id=0, has_side_effects=True),
    )(
        traces,
        masks.reshape(rows, ring, 2 * count, channels),
        moveouts.reshape(channels // LANES, LANES),
        tiles,
        *tables,
    )
    return found.transpose(1, 0, 2).reshape(count, lag_count)


def solution(mesh):
    finer = Mesh(mesh.devices.reshape(mesh.shape["grp"], 4, -1, 2), ("grp", "tm_0", "tm_1", "tm_2"))
    axes = ("tm_0", "tm_1", "tm_2")
    return jax.shard_map(
        on_device,
        mesh=finer,
        in_specs=(P("grp", axes), P(axes, None), P("grp"), P(None, "grp")),
        out_specs=P(axes, "grp"),
        check_vma=False,
    )
```

```python
import functools
import math

import jax
import jax.numpy as jnp
import numpy as np
from jax import lax
from jax.experimental import pallas as pl
from jax.experimental.pallas import tpu as pltpu
from jax.sharding import Mesh
from jax.sharding import PartitionSpec as P

MESH = pl.DeviceIdType.MESH
LANES = 128
GROUP = 1
PIECES = 4


def split(value):
    high = value.astype(jnp.bfloat16)
    low = (value - high.astype(jnp.float32)).astype(jnp.bfloat16)
    return high, low


def split_constant(value):
    value = np.asarray(value, np.float64).astype(np.float32)
    high = value.astype(jnp.bfloat16)
    low = (value - high.astype(np.float32)).astype(jnp.bfloat16)
    return jnp.asarray(np.stack([high, low]))


def mm(a, b):
    return jnp.dot(a, b, preferred_element_type=jnp.float32)


def dot3(left, right):
    (left_hi, left_lo), (right_hi, right_lo) = left, right
    lefts = jnp.concatenate([left_hi, left_hi, left_lo], axis=1)
    return mm(lefts, jnp.concatenate([right_hi, right_lo, right_hi], axis=0))


def forward(series, first, twiddle, second):
    half = twiddle.shape[1]
    turned = []
    for s in series:
        y = dot3((first[0], first[1]), split(s))
        re, im = y[:half], y[half:]
        turned.append(
            jnp.concatenate([re * twiddle[0] - im * twiddle[1], re * twiddle[1] + im * twiddle[0]], axis=1)
        )
    return dot3(split(jnp.concatenate(turned, axis=0)), (second[0], second[1]))


def matched_kernel(
    cfg, scale,
    x_hbm, masks_hbm, mo_hbm, templ_hbm, first_hbm, first_half_hbm, twiddle_hbm, second_hbm, third_hbm, fourth_hbm,
    out_ref,
    raw, mo_ref, pair, mask_int, mask_rows, halves, shift_at, parts, partial, flow, merge, ready, landed,
    templ_ref, first_ref, first_half_ref, twiddle_ref, second_ref, third_ref, fourth_ref, templ_spec, gain,
    partner_sem, load_sem, pair_send, pair_recv, flow_send, flow_recv, merge_send, merge_recv, last_send, last_recv,
):
    rows, ring, hops, outside, shared = cfg
    channels = x_hbm.shape[0]
    blocks = rows * ring
    x = lax.axis_index("tm_0")
    z = lax.axis_index("tm_1")
    core = lax.axis_index("tm_2")
    toward = 1 - 2 * core
    here = x * ring + z
    partner = {"tm_2": 1 - core}

    def chip(step):
        other = lax.rem(here + step + blocks, blocks)
        return {"tm_0": other // ring, "tm_1": lax.rem(other, ring)}

    def window_place(s):
        return core * hops + toward * s

    def wait_for(ref, sem):
        pltpu.make_async_copy(ref, ref, sem).wait()

    loads = []

    def load(src, dst):
        copy = pltpu.make_async_copy(src, dst, load_sem.at[len(loads)])
        copy.start()
        loads.append(copy)
        return copy

    per_piece = channels // PIECES
    mo_copy = load(mo_hbm, mo_ref)
    x_copies = [load(x_hbm.at[pl.ds(p * per_piece, per_piece)], raw.at[pl.ds(p * per_piece, per_piece)]) for p in range(PIECES)]

    barrier = pltpu.get_barrier_semaphore()
    peers = [chip(-toward)]
    for d in range(1, rows):
        peers += [{"tm_0": lax.rem(x + d, rows), "tm_2": c} for c in (core, 1 - core)]
    for where in peers:
        pl.semaphore_signal(barrier, inc=1, device_id=where, device_id_type=MESH)

    @pl.when(core == 1)
    def _():
        pl.semaphore_signal(barrier, inc=1, device_id=partner, device_id_type=MESH)

    mask_copy = load(masks_hbm, mask_int)
    templ_copy = load(templ_hbm, templ_ref)
    table_copies = [
        load(first_half_hbm, first_half_ref),
        load(twiddle_hbm, twiddle_ref),
        load(second_hbm, second_ref),
        load(first_hbm, first_ref),
        load(third_hbm, third_ref),
        load(fourth_hbm, fourth_ref),
    ]

    lane = lax.broadcasted_iota(jnp.int32, (LANES, LANES), 1)
    mo_copy.wait()
    for p in range(PIECES):
        x_copies[p].wait()

        @pl.loop(p * per_piece // LANES, (p + 1) * per_piece // LANES, unroll=True)
        def _(b):
            at = pl.ds(pl.multiple_of(b * LANES, LANES), LANES)
            spread = jnp.broadcast_to(mo_ref[pl.ds(b, 1), :].astype(jnp.float32), (LANES, LANES))
            move = jnp.transpose(spread).astype(jnp.int32)
            index = lane + (move & (LANES - 1))
            value = jnp.take_along_axis(raw[at, :], index & (LANES - 1), axis=1)
            pair[core, at, :] = value
            passed = (index >= LANES).astype(jnp.int32)
            shift_at[at, :] = ((move >> (LANES.bit_length() - 1)) + passed).astype(jnp.float32).astype(jnp.bfloat16)
            high, low = split(value)
            halves[0, core, at, :] = high
            halves[1, core, at, :] = low

    @pl.when(core == 0)
    def _():
        pl.semaphore_wait(barrier, len(peers) + 1)
        pl.semaphore_signal(partner_sem, inc=1, device_id=partner, device_id_type=MESH)

    @pl.when(core == 1)
    def _():
        pl.semaphore_wait(partner_sem, 1)

    swaps = []
    for p in range(PIECES):
        half = pair.at[core, pl.ds(p * per_piece, per_piece)]
        swap = pltpu.make_async_remote_copy(
            src_ref=half, dst_ref=half, send_sem=pair_send.at[p], recv_sem=pair_recv.at[p],
            device_id=partner, device_id_type=MESH,
        )
        swap.start()
        swaps.append(swap)

    mask_copy.wait()
    tile_rows = mask_int.shape[2]
    per_owner = tile_rows // 2
    own_rows = rows * per_owner
    chunk_rows = 2 * own_rows
    tops = lax.broadcasted_iota(jnp.int32, (tile_rows, channels), 0) < per_owner

    def pick(first, second, side):
        moved = pltpu.roll(jnp.where(side == 0, second, first), per_owner, 0)
        kept = jnp.where(side == 0, first, second)
        return jnp.where(tops == (side == 0), kept, moved).astype(jnp.float32)

    @pl.loop(0, mask_rows.shape[0] // chunk_rows)
    def _(m):
        owner = lax.rem(z + toward * m + ring, ring)
        tiles = [mask_int[a, owner] for a in range(rows)]
        pieces = [pick(tiles[a], tiles[a + 1], side) for side in (core, 1 - core) for a in range(0, rows, 2)]
        kept = jnp.concatenate(pieces, axis=0).astype(jnp.bfloat16)
        at = pl.ds(pl.multiple_of(m * chunk_rows, chunk_rows), chunk_rows)
        mask_rows[at, :channels] = kept
        mask_rows[at, channels:] = kept

    for p in range(PIECES):
        swaps[p].wait_recv()

        @pl.loop(p * per_piece // LANES, (p + 1) * per_piece // LANES)
        def _(b):
            at = pl.ds(pl.multiple_of(b * LANES, LANES), LANES)
            high, low = split(pair[1 - core, at, :])
            halves[0, 1 - core, at, :] = high
            halves[1, 1 - core, at, :] = low

    zero = jnp.zeros((LANES, LANES), jnp.bfloat16)
    top = hops + outside

    def select(s):
        twice = jnp.broadcast_to((2 * window_place(s)).astype(jnp.float32), (LANES, LANES))
        before, same, after = ((twice + d).astype(jnp.bfloat16) for d in (-1, 0, 1))

        @pl.loop(0, channels // LANES)
        def _(b):
            at = pl.ds(pl.multiple_of(b * LANES, LANES), LANES)
            shift = shift_at[at, :]
            is_before, is_same, is_after = shift == before, shift == same, shift == after
            for t in range(2):
                first, second = halves[t, 0, at, :], halves[t, 1, at, :]
                to = pl.ds(pl.multiple_of(t * channels + b * LANES, LANES), LANES)
                parts[to, :LANES] = jnp.where(is_same, first, jnp.where(is_after, second, zero))
                parts[to, LANES:] = jnp.where(is_before, first, jnp.where(is_same, second, zero))

    def multiply(s, low=0, high=None):
        high = (top - s + 1) * chunk_rows + shared * own_rows if high is None else high
        live = pl.ds(low, high - low)
        partial[s, live] = mm(mask_rows[live], parts[...])

    def contribution(s):
        select(s)
        multiply(s)

    select(0)
    halfway = top // 2 + 1
    multiply(0, halfway * chunk_rows)

    sent = {"flow": 0, "merge": 0, "last": 0}
    slots = {}

    def slot_of(s, g):
        return slots.setdefault((s, g), len(slots))

    def send(name, src, dst, send_sem, recv_sem, where):
        pltpu.make_async_remote_copy(
            src_ref=src, dst_ref=dst, send_sem=send_sem, recv_sem=recv_sem, device_id=where, device_id_type=MESH
        ).start()
        sent[name] += math.prod(src.shape)

    groups = [(top + 1, top + 1, own_rows)] if shared else []
    groups += [(max(high - GROUP + 1, 1), high, chunk_rows) for high in range(top, 0, -GROUP)]
    onward = chip(toward)

    def chunks(m, count, held):
        return pl.ds(m * chunk_rows, (count - 1) * chunk_rows + held)

    def span(s, g):
        low, high, held = groups[g]
        low = max(low, s + 1)
        return (low - s, high - low + 1, held) if low <= high and s < hops else None

    def send_on(s, g):
        found = span(s, g)
        if found is None:
            return
        m, count, held = found
        src = (partial.at[0] if s == 0 else flow.at[s - 1]).at[chunks(m, count, held)]
        dst = flow.at[s, chunks(m - 1, count, held)]
        send("flow", src, dst, flow_send, flow_recv.at[slot_of(s, g)], onward)

    @pl.when(core == 1)
    def _():
        pl.semaphore_wait(barrier, len(peers))

    for g in range(len(groups)):
        if groups[g][0] < halfway:
            continue
        send_on(0, g)
    multiply(0, chunk_rows, halfway * chunk_rows)
    for g in range(len(groups)):
        if groups[g][0] < halfway:
            send_on(0, g)

    def template_spectra():
        templ_copy.wait()
        for copy in table_copies[:3]:
            copy.wait()
        count = out_ref.shape[1]
        short = templ_ref.shape[0] // count
        templates = [templ_ref[pl.ds(i, short, stride=count), :] for i in range(count)]
        templ_spec[...] = forward(templates, first_half_ref[...], twiddle_ref[...], second_ref[...])
        for i in range(count):
            energy = jnp.sqrt(jnp.sum(templates[i] * templates[i], keepdims=True) + 1e-06)
            gain[pl.ds(i, 1), :] = jnp.broadcast_to(1.0 / (scale * energy), (1, LANES))

    contribution(1)
    contribution(2)
    template_spectra()
    todo = list(range(3, hops + 1))

    def deliver(total, s, m, sides):
        slot = s + m
        for side in range(sides):
            for a in range(rows):
                start = side * own_rows + a * per_owner
                piece = total[start : start + per_owner]
                ready[slot, side, a] = jnp.concatenate([piece[:, :LANES], piece[:, LANES:]], axis=0)
        dst = landed.at[lax.rem(here - window_place(s) + blocks, blocks)]
        for side in range(sides):
            cores = core if side == 0 else 1 - core
            for d in range(rows):
                if m:
                    src, where = ready.at[slot, side, d], {"tm_0": d, "tm_1": lax.rem(z + toward * m + ring, ring)}
                else:
                    owner = lax.rem(x + d, rows)
                    src, where = ready.at[slot, side, owner], {"tm_0": owner}
                if m == 0 and side == 0 and d == 0:
                    pltpu.make_async_copy(src, dst, last_recv).start()
                else:
                    send("last", src, dst, last_send, last_recv, {**where, "tm_2": cores})

    def merge_and_deliver(s):
        wait_for(merge.at[s], merge_recv.at[s])
        own = pl.ds(0, own_rows)
        deliver(flow[s - 1, own] + partial[s, own] + merge[s], s, 0, 1)

    def arrive(s, g):
        arrived = span(s - 1, g)
        if arrived is None:
            return
        m, count, held = arrived
        m = m - 1
        wait_for(flow.at[s - 1, chunks(m, count, held)], flow_recv.at[slot_of(s - 1, g)])
        for c in reversed(range(m, m + count)):
            at = chunks(c, 1, held)
            if s == hops:
                deliver(flow[s - 1, at] + partial[s, at], s, c, held // own_rows)
            elif c > 0:
                flow[s - 1, at] = flow[s - 1, at] + partial[s, at]
            else:
                src = flow.at[s - 1, pl.ds(own_rows, own_rows)]
                send("merge", src, merge.at[hops - s], merge_send, merge_recv.at[hops - s], partner)
        send_on(s, g)

    for s in range(1, hops + 1):
        if s == hops and hops % 2 == 0:
            merge_and_deliver(hops // 2)
        for g in range(len(groups)):
            arrive(s, g)
            if todo and g in (2, 6):
                contribution(todo.pop(0))
        if hops < 2 * s < 2 * hops:
            merge_and_deliver(s)
    for s in range((hops - 1) // 2, 0, -1):
        merge_and_deliver(s)

    for swap in swaps:
        swap.wait_send()
    flat = flow.reshape(-1, 2 * LANES)
    wait_for(flat.at[pl.ds(0, sent["flow"] // (2 * LANES))], flow_send)
    wait_for(merge.at[pl.ds(0, sent["merge"] // math.prod(merge.shape[1:]))], merge_send)
    wait_for(landed.at[pl.ds(0, sent["last"] // math.prod(landed.shape[1:]))], last_send)
    for copy in table_copies[3:]:
        copy.wait()
    wait_for(landed, last_recv)

    count = out_ref.shape[1]
    long = blocks * 2
    flat = landed.reshape(long * count, LANES)
    half = twiddle_ref.shape[1]
    series = [flat[pl.ds(i, long, stride=count), :] for i in range(count)]
    twiddle = twiddle_ref[...]
    spec = forward(series, first_ref[...], twiddle, second_ref[...])
    sr, si, hr, hi = spec[:, :LANES], spec[:, LANES:], templ_spec[:, :LANES], templ_spec[:, LANES:]
    product = jnp.concatenate([sr * hr + si * hi, si * hr - sr * hi], axis=1)
    back = dot3(split(product), (third_ref[0], third_ref[1]))
    for i in range(count):
        re, im = back[i * half : (i + 1) * half, :LANES], back[i * half : (i + 1) * half, LANES:]
        turned = jnp.concatenate([re * twiddle[0] + im * twiddle[1], im * twiddle[0] - re * twiddle[1]], axis=0)
        lags = dot3((fourth_ref[0], fourth_ref[1]), split(turned))
        out_ref[:, i, :] = lags * gain[pl.ds(i, 1), :]


def fourier_tables(length, lag_count):
    blocks = length // LANES
    kept = blocks // 2 + 1
    half = -(-kept // 8) * 8
    f1 = np.arange(half)
    n1 = np.arange(blocks)
    n2 = np.arange(LANES)
    live = (f1 < kept)[:, None]
    angle = 2.0 * np.pi * ((f1[:, None] * n1[None, :]) % blocks) / blocks
    first = np.concatenate([np.cos(angle) * live, -np.sin(angle) * live])
    turn = 2.0 * np.pi * ((f1[:, None] * n2[None, :]) % length) / length
    twiddle = np.stack([np.cos(turn) * live, -np.sin(turn) * live]).astype(np.float32)
    inner = 2.0 * np.pi * ((n2[:, None] * n2[None, :]) % LANES) / LANES
    c, s = np.cos(inner), np.sin(inner)
    second = np.block([[c, -s], [s, c]])
    third = np.block([[c, s], [-s, c]])
    weight = np.where((f1 == 0) | (f1 == kept - 1), 1.0, 2.0) * (f1 < kept) / length
    lag_rows = lag_count // LANES
    back = angle.T[:lag_rows]
    fourth = np.concatenate([np.cos(back) * weight, -np.sin(back) * weight], axis=1)
    return (
        split_constant(first),
        split_constant(first[:, :lag_rows]),
        jnp.asarray(twiddle),
        split_constant(second),
        split_constant(third),
        split_constant(fourth),
    )


def on_device(traces, templates, moveouts, masks):
    rows, ring = lax.axis_size("tm_0"), lax.axis_size("tm_1")
    channels, samples = traces.shape
    length = samples * rows * ring * 2
    count, lag_count = templates.shape
    chip_samples = 2 * samples
    hops = (length // 8) // chip_samples
    outside, shared = divmod(ring - 1 - hops, 2)
    top = hops + outside
    cfg = (rows, ring, hops, outside, shared)
    chunk = (2 * rows * count, chip_samples)
    lag_rows = lag_count // LANES
    tiles = templates.reshape(count, lag_rows, LANES).transpose(1, 0, 2).reshape(lag_rows * count, LANES)
    tables = fourier_tables(length, lag_count)
    messages = sum(min(high, hops) for high in range(top, 0, -GROUP)) + shared * hops
    vmem = pl.BlockSpec(memory_space=pltpu.VMEM)
    anywhere = pl.BlockSpec(memory_space=pl.ANY)
    dma = pltpu.SemaphoreType.DMA
    half = tables[2].shape[1]
    found = pl.pallas_call(
        functools.partial(matched_kernel, cfg, math.sqrt(channels)),
        out_shape=pltpu.VMEM((lag_rows, count, LANES), jnp.float32),
        in_specs=[anywhere] * (4 + len(tables)),
        out_specs=vmem,
        scratch_shapes=[
            pltpu.VMEM((channels, samples), jnp.float32),
            pltpu.VMEM((channels // LANES, LANES), jnp.int32),
            pltpu.VMEM((2, channels, samples), jnp.float32),
            pltpu.VMEM((rows, ring, 2 * count, channels), jnp.int32),
            pltpu.VMEM(((top + 1 + shared) * chunk[0], 2 * channels), jnp.bfloat16),
            pltpu.VMEM((2, 2, channels, samples), jnp.bfloat16),
            pltpu.VMEM((channels, samples), jnp.bfloat16),
            pltpu.VMEM((2 * channels, chip_samples), jnp.bfloat16),
            pltpu.VMEM((hops + 1, (top + 1 + shared) * chunk[0], chunk[1]), jnp.float32),
            pltpu.VMEM((hops, (top + shared) * chunk[0], chunk[1]), jnp.float32),
            pltpu.VMEM((hops, rows * count, chip_samples), jnp.float32),
            pltpu.VMEM((top + 1 + shared, 2, rows, 2 * count, LANES), jnp.float32),
            pltpu.VMEM((rows * ring, 2 * count, LANES), jnp.float32),
            pltpu.VMEM(tiles.shape, jnp.float32),
            *[pltpu.VMEM(t.shape, t.dtype) for t in tables],
            pltpu.VMEM((count * half, 2 * LANES), jnp.float32),
            pltpu.VMEM((count, LANES), jnp.float32),
            pltpu.SemaphoreType.REGULAR,
            dma((4 + PIECES + len(tables),)),
            dma((PIECES,)),
            dma((PIECES,)),
            dma,
            dma((messages,)),
            dma,
            dma((hops,)),
            dma,
            dma,
        ],
        compiler_params=pltpu.CompilerParams(collective_id=0, has_side_effects=True),
    )(
        traces,
        masks.reshape(rows, ring, 2 * count, channels),
        moveouts.reshape(channels // LANES, LANES),
        tiles,
        *tables,
    )
    return found.transpose(1, 0, 2).reshape(count, lag_count)


def solution(mesh):
    finer = Mesh(mesh.devices.reshape(mesh.shape["grp"], 4, -1, 2), ("grp", "tm_0", "tm_1", "tm_2"))
    axes = ("tm_0", "tm_1", "tm_2")
    return jax.shard_map(
        on_device,
        mesh=finer,
        in_specs=(P("grp", axes), P(axes, None), P("grp"), P(None, "grp")),
        out_specs=P(axes, "grp"),
        check_vma=False,
    )
```

```python
import functools
import math

import jax
import jax.numpy as jnp
import numpy as np
from jax import lax
from jax.experimental import pallas as pl
from jax.experimental.pallas import tpu as pltpu
from jax.sharding import Mesh
from jax.sharding import PartitionSpec as P

MESH = pl.DeviceIdType.MESH
LANES = 128
GROUP = 1
PIECES = 4


def split(value):
    high = value.astype(jnp.bfloat16)
    low = (value - high.astype(jnp.float32)).astype(jnp.bfloat16)
    return high, low


def split_constant(value):
    value = np.asarray(value, np.float64).astype(np.float32)
    high = value.astype(jnp.bfloat16)
    low = (value - high.astype(np.float32)).astype(jnp.bfloat16)
    return jnp.asarray(np.stack([high, low]))


def mm(a, b):
    return jnp.dot(a, b, preferred_element_type=jnp.float32)


def dot3(left, right):
    (left_hi, left_lo), (right_hi, right_lo) = left, right
    lefts = jnp.concatenate([left_hi, left_hi, left_lo], axis=1)
    return mm(lefts, jnp.concatenate([right_hi, right_lo, right_hi], axis=0))


def forward(series, first, twiddle, second):
    half = twiddle.shape[1]
    turned = []
    for s in series:
        y = dot3((first[0], first[1]), split(s))
        re, im = y[:half], y[half:]
        turned.append(
            jnp.concatenate([re * twiddle[0] - im * twiddle[1], re * twiddle[1] + im * twiddle[0]], axis=1)
        )
    return dot3(split(jnp.concatenate(turned, axis=0)), (second[0], second[1]))


def matched_kernel(
    cfg, scale,
    x_hbm, masks_hbm, mo_hbm, templ_hbm, first_hbm, first_half_hbm, twiddle_hbm, second_hbm, third_hbm, fourth_hbm,
    out_ref,
    raw, mo_ref, pair, mask_int, mask_rows, halves, shift_at, parts, partial, flow, merge, ready, landed,
    templ_ref, first_ref, first_half_ref, twiddle_ref, second_ref, third_ref, fourth_ref, templ_spec, gain,
    partner_sem, load_sem, pair_send, pair_recv, flow_send, flow_recv, merge_send, merge_recv, last_send, last_recv,
):
    rows, ring, hops, outside, shared = cfg
    channels = x_hbm.shape[0]
    blocks = rows * ring
    x = lax.axis_index("tm_0")
    z = lax.axis_index("tm_1")
    core = lax.axis_index("tm_2")
    odd = lax.rem(z, 2)
    way = lax.rem(core + z, 2)
    toward = 1 - 2 * way
    here = x * ring + z
    partner = {"tm_2": 1 - core}

    def chip(step):
        other = lax.rem(here + step + blocks, blocks)
        return {"tm_0": other // ring, "tm_1": lax.rem(other, ring)}

    def window_place(s):
        return way * hops + toward * s

    def wait_for(ref, sem):
        pltpu.make_async_copy(ref, ref, sem).wait()

    loads = []

    def load(src, dst):
        copy = pltpu.make_async_copy(src, dst, load_sem.at[len(loads)])
        copy.start()
        loads.append(copy)
        return copy

    per_piece = channels // PIECES
    mo_copy = load(mo_hbm, mo_ref)
    x_copies = [load(x_hbm.at[pl.ds(p * per_piece, per_piece)], raw.at[pl.ds(p * per_piece, per_piece)]) for p in range(PIECES)]

    barrier = pltpu.get_barrier_semaphore()
    peers = [{**chip(-toward), "tm_2": 1 - core}]
    for d in range(1, rows):
        peers += [{"tm_0": lax.rem(x + d, rows), "tm_2": c} for c in (core, 1 - core)]
    for where in peers:
        pl.semaphore_signal(barrier, inc=1, device_id=where, device_id_type=MESH)

    @pl.when(way == 1)
    def _():
        pl.semaphore_signal(barrier, inc=1, device_id=partner, device_id_type=MESH)

    mask_copy = load(masks_hbm, mask_int)
    templ_copy = load(templ_hbm, templ_ref)
    table_copies = [
        load(first_half_hbm, first_half_ref),
        load(twiddle_hbm, twiddle_ref),
        load(second_hbm, second_ref),
        load(first_hbm, first_ref),
        load(third_hbm, third_ref),
        load(fourth_hbm, fourth_ref),
    ]

    lane = lax.broadcasted_iota(jnp.int32, (LANES, LANES), 1)
    mo_copy.wait()
    for p in range(PIECES):
        x_copies[p].wait()

        @pl.loop(p * per_piece // LANES, (p + 1) * per_piece // LANES, unroll=True)
        def _(b):
            at = pl.ds(pl.multiple_of(b * LANES, LANES), LANES)
            spread = jnp.broadcast_to(mo_ref[pl.ds(b, 1), :].astype(jnp.float32), (LANES, LANES))
            move = jnp.transpose(spread).astype(jnp.int32)
            index = lane + (move & (LANES - 1))
            value = jnp.take_along_axis(raw[at, :], index & (LANES - 1), axis=1)
            pair[core, at, :] = value
            passed = (index >= LANES).astype(jnp.int32)
            shift_at[at, :] = ((move >> (LANES.bit_length() - 1)) + passed).astype(jnp.float32).astype(jnp.bfloat16)
            high, low = split(value)
            halves[0, core, at, :] = high
            halves[1, core, at, :] = low

    @pl.when(way == 0)
    def _():
        pl.semaphore_wait(barrier, len(peers) + 1)
        pl.semaphore_signal(partner_sem, inc=1, device_id=partner, device_id_type=MESH)

    @pl.when(way == 1)
    def _():
        pl.semaphore_wait(partner_sem, 1)

    swaps = []
    for p in range(PIECES):
        half = pair.at[core, pl.ds(p * per_piece, per_piece)]
        swap = pltpu.make_async_remote_copy(
            src_ref=half, dst_ref=half, send_sem=pair_send.at[p], recv_sem=pair_recv.at[p],
            device_id=partner, device_id_type=MESH,
        )
        swap.start()
        swaps.append(swap)

    mask_copy.wait()
    tile_rows = mask_int.shape[2]
    per_owner = tile_rows // 2
    own_rows = rows * per_owner
    chunk_rows = 2 * own_rows
    tops = lax.broadcasted_iota(jnp.int32, (tile_rows, channels), 0) < per_owner

    def pick(first, second, side):
        moved = pltpu.roll(jnp.where(side == 0, second, first), per_owner, 0)
        kept = jnp.where(side == 0, first, second)
        return jnp.where(tops == (side == 0), kept, moved).astype(jnp.float32)

    @pl.loop(0, mask_rows.shape[0] // chunk_rows)
    def _(m):
        owner = lax.rem(z + toward * m + ring, ring)
        tiles = [mask_int[a, owner] for a in range(rows)]
        pieces = [pick(tiles[a], tiles[a + 1], side) for side in (way, 1 - way) for a in range(0, rows, 2)]
        kept = jnp.concatenate(pieces, axis=0).astype(jnp.bfloat16)
        at = pl.ds(pl.multiple_of(m * chunk_rows, chunk_rows), chunk_rows)
        mask_rows[at, :channels] = kept
        mask_rows[at, channels:] = kept

    for p in range(PIECES):
        swaps[p].wait_recv()

        @pl.loop(p * per_piece // LANES, (p + 1) * per_piece // LANES)
        def _(b):
            at = pl.ds(pl.multiple_of(b * LANES, LANES), LANES)
            high, low = split(pair[1 - core, at, :])
            halves[0, 1 - core, at, :] = high
            halves[1, 1 - core, at, :] = low

    zero = jnp.zeros((LANES, LANES), jnp.bfloat16)
    top = hops + outside

    def select(s):
        twice = jnp.broadcast_to((2 * window_place(s)).astype(jnp.float32), (LANES, LANES))
        before, same, after = ((twice + d).astype(jnp.bfloat16) for d in (-1, 0, 1))

        @pl.loop(0, channels // LANES)
        def _(b):
            at = pl.ds(pl.multiple_of(b * LANES, LANES), LANES)
            shift = shift_at[at, :]
            is_before, is_same, is_after = shift == before, shift == same, shift == after
            for t in range(2):
                first, second = halves[t, 0, at, :], halves[t, 1, at, :]
                to = pl.ds(pl.multiple_of(t * channels + b * LANES, LANES), LANES)
                parts[to, :LANES] = jnp.where(is_same, first, jnp.where(is_after, second, zero))
                parts[to, LANES:] = jnp.where(is_before, first, jnp.where(is_same, second, zero))

    def multiply(s, low=0, high=None):
        high = (top - s + 1) * chunk_rows + shared * own_rows if high is None else high
        live = pl.ds(low, high - low)
        partial[s, live] = mm(mask_rows[live], parts[...])

    def contribution(s):
        select(s)
        multiply(s)

    select(0)
    halfway = top // 2 + 1
    multiply(0, halfway * chunk_rows)

    sent = {"flow": 0, "merge": 0, "last": 0}
    slots = {}

    def slot_of(s, g):
        return slots.setdefault((s, g), len(slots))

    def send(name, src, dst, send_sem, recv_sem, where):
        pltpu.make_async_remote_copy(
            src_ref=src, dst_ref=dst, send_sem=send_sem, recv_sem=recv_sem, device_id=where, device_id_type=MESH
        ).start()
        sent[name] += math.prod(src.shape)

    groups = [(top + 1, top + 1, own_rows)] if shared else []
    groups += [(max(high - GROUP + 1, 1), high, chunk_rows) for high in range(top, 0, -GROUP)]
    onward = {**chip(toward), "tm_2": 1 - core}

    def chunks(m, count, held):
        return pl.ds(m * chunk_rows, (count - 1) * chunk_rows + held)

    def span(s, g):
        low, high, held = groups[g]
        low = max(low, s + 1)
        return (low - s, high - low + 1, held) if low <= high and s < hops else None

    def send_on(s, g):
        found = span(s, g)
        if found is None:
            return
        m, count, held = found
        src = (partial.at[0] if s == 0 else flow.at[s - 1]).at[chunks(m, count, held)]
        dst = flow.at[s, chunks(m - 1, count, held)]
        send("flow", src, dst, flow_send, flow_recv.at[slot_of(s, g)], onward)

    @pl.when(way == 1)
    def _():
        pl.semaphore_wait(barrier, len(peers))

    for g in range(len(groups)):
        if groups[g][0] < halfway:
            continue
        send_on(0, g)
    multiply(0, chunk_rows, halfway * chunk_rows)
    for g in range(len(groups)):
        if groups[g][0] < halfway:
            send_on(0, g)

    def template_spectra():
        templ_copy.wait()
        for copy in table_copies[:3]:
            copy.wait()
        count = out_ref.shape[1]
        short = templ_ref.shape[0] // count
        templates = [templ_ref[pl.ds(i, short, stride=count), :] for i in range(count)]
        templ_spec[...] = forward(templates, first_half_ref[...], twiddle_ref[...], second_ref[...])
        for i in range(count):
            energy = jnp.sqrt(jnp.sum(templates[i] * templates[i], keepdims=True) + 1e-06)
            gain[pl.ds(i, 1), :] = jnp.broadcast_to(1.0 / (scale * energy), (1, LANES))

    contribution(1)
    contribution(2)
    template_spectra()
    todo = list(range(3, hops + 1))

    def deliver(total, s, m, sides):
        slot = s + m
        for side in range(sides):
            for a in range(rows):
                start = side * own_rows + a * per_owner
                piece = total[start : start + per_owner]
                ready[slot, side, a] = jnp.concatenate([piece[:, :LANES], piece[:, LANES:]], axis=0)
        dst = landed.at[lax.rem(here - window_place(s) + blocks, blocks)]
        for side in range(sides):
            for d in range(rows):
                if m:
                    where = {"tm_0": d, "tm_1": lax.rem(z + toward * m + ring, ring), "tm_2": way if side == 0 else 1 - way}
                    send("last", ready.at[slot, side, d], dst, last_send, last_recv, where)
                    continue
                owner = lax.rem(x + d, rows)
                src = ready.at[slot, 0 if sides == 1 else odd if side == 0 else 1 - odd, owner]
                if side == 0 and d == 0:
                    pltpu.make_async_copy(src, dst, last_recv).start()
                else:
                    where = {"tm_0": owner, "tm_2": core if side == 0 else 1 - core}
                    send("last", src, dst, last_send, last_recv, where)

    own = pl.ds(pl.multiple_of(odd * own_rows, own_rows), own_rows)
    others = pl.ds(pl.multiple_of((1 - odd) * own_rows, own_rows), own_rows)

    def merge_and_deliver(s):
        wait_for(merge.at[s], merge_recv.at[s])
        deliver(flow[s - 1, own] + partial[s, own] + merge[s], s, 0, 1)

    def arrive(s, g):
        arrived = span(s - 1, g)
        if arrived is None:
            return
        m, count, held = arrived
        m = m - 1
        wait_for(flow.at[s - 1, chunks(m, count, held)], flow_recv.at[slot_of(s - 1, g)])
        for c in reversed(range(m, m + count)):
            at = chunks(c, 1, held)
            if s == hops:
                deliver(flow[s - 1, at] + partial[s, at], s, c, held // own_rows)
            elif c > 0:
                flow[s - 1, at] = flow[s - 1, at] + partial[s, at]
            else:
                src = flow.at[s - 1, others]
                send("merge", src, merge.at[hops - s], merge_send, merge_recv.at[hops - s], partner)
        send_on(s, g)

    for s in range(1, hops + 1):
        if s == hops and hops % 2 == 0:
            merge_and_deliver(hops // 2)
        for g in range(len(groups)):
            arrive(s, g)
            if todo and g in (2, 6):
                contribution(todo.pop(0))
        if hops < 2 * s < 2 * hops:
            merge_and_deliver(s)
    for s in range((hops - 1) // 2, 0, -1):
        merge_and_deliver(s)

    for swap in swaps:
        swap.wait_send()
    flat = flow.reshape(-1, 2 * LANES)
    wait_for(flat.at[pl.ds(0, sent["flow"] // (2 * LANES))], flow_send)
    wait_for(merge.at[pl.ds(0, sent["merge"] // math.prod(merge.shape[1:]))], merge_send)
    wait_for(landed.at[pl.ds(0, sent["last"] // math.prod(landed.shape[1:]))], last_send)
    for copy in table_copies[3:]:
        copy.wait()
    wait_for(landed, last_recv)

    count = out_ref.shape[1]
    long = blocks * 2
    flat = landed.reshape(long * count, LANES)
    half = twiddle_ref.shape[1]
    series = [flat[pl.ds(i, long, stride=count), :] for i in range(count)]
    twiddle = twiddle_ref[...]
    spec = forward(series, first_ref[...], twiddle, second_ref[...])
    sr, si, hr, hi = spec[:, :LANES], spec[:, LANES:], templ_spec[:, :LANES], templ_spec[:, LANES:]
    product = jnp.concatenate([sr * hr + si * hi, si * hr - sr * hi], axis=1)
    back = dot3(split(product), (third_ref[0], third_ref[1]))
    for i in range(count):
        re, im = back[i * half : (i + 1) * half, :LANES], back[i * half : (i + 1) * half, LANES:]
        turned = jnp.concatenate([re * twiddle[0] + im * twiddle[1], im * twiddle[0] - re * twiddle[1]], axis=0)
        lags = dot3((fourth_ref[0], fourth_ref[1]), split(turned))
        out_ref[:, i, :] = lags * gain[pl.ds(i, 1), :]


def fourier_tables(length, lag_count):
    blocks = length // LANES
    kept = blocks // 2 + 1
    half = -(-kept // 8) * 8
    f1 = np.arange(half)
    n1 = np.arange(blocks)
    n2 = np.arange(LANES)
    live = (f1 < kept)[:, None]
    angle = 2.0 * np.pi * ((f1[:, None] * n1[None, :]) % blocks) / blocks
    first = np.concatenate([np.cos(angle) * live, -np.sin(angle) * live])
    turn = 2.0 * np.pi * ((f1[:, None] * n2[None, :]) % length) / length
    twiddle = np.stack([np.cos(turn) * live, -np.sin(turn) * live]).astype(np.float32)
    inner = 2.0 * np.pi * ((n2[:, None] * n2[None, :]) % LANES) / LANES
    c, s = np.cos(inner), np.sin(inner)
    second = np.block([[c, -s], [s, c]])
    third = np.block([[c, s], [-s, c]])
    weight = np.where((f1 == 0) | (f1 == kept - 1), 1.0, 2.0) * (f1 < kept) / length
    lag_rows = lag_count // LANES
    back = angle.T[:lag_rows]
    fourth = np.concatenate([np.cos(back) * weight, -np.sin(back) * weight], axis=1)
    return (
        split_constant(first),
        split_constant(first[:, :lag_rows]),
        jnp.asarray(twiddle),
        split_constant(second),
        split_constant(third),
        split_constant(fourth),
    )


def on_device(traces, templates, moveouts, masks):
    rows, ring = lax.axis_size("tm_0"), lax.axis_size("tm_1")
    channels, samples = traces.shape
    length = samples * rows * ring * 2
    count, lag_count = templates.shape
    chip_samples = 2 * samples
    hops = (length // 8) // chip_samples
    outside, shared = divmod(ring - 1 - hops, 2)
    top = hops + outside
    cfg = (rows, ring, hops, outside, shared)
    chunk = (2 * rows * count, chip_samples)
    lag_rows = lag_count // LANES
    tiles = templates.reshape(count, lag_rows, LANES).transpose(1, 0, 2).reshape(lag_rows * count, LANES)
    tables = fourier_tables(length, lag_count)
    messages = sum(min(high, hops) for high in range(top, 0, -GROUP)) + shared * hops
    vmem = pl.BlockSpec(memory_space=pltpu.VMEM)
    anywhere = pl.BlockSpec(memory_space=pl.ANY)
    dma = pltpu.SemaphoreType.DMA
    half = tables[2].shape[1]
    found = pl.pallas_call(
        functools.partial(matched_kernel, cfg, math.sqrt(channels)),
        out_shape=pltpu.VMEM((lag_rows, count, LANES), jnp.float32),
        in_specs=[anywhere] * (4 + len(tables)),
        out_specs=vmem,
        scratch_shapes=[
            pltpu.VMEM((channels, samples), jnp.float32),
            pltpu.VMEM((channels // LANES, LANES), jnp.int32),
            pltpu.VMEM((2, channels, samples), jnp.float32),
            pltpu.VMEM((rows, ring, 2 * count, channels), jnp.int32),
            pltpu.VMEM(((top + 1 + shared) * chunk[0], 2 * channels), jnp.bfloat16),
            pltpu.VMEM((2, 2, channels, samples), jnp.bfloat16),
            pltpu.VMEM((channels, samples), jnp.bfloat16),
            pltpu.VMEM((2 * channels, chip_samples), jnp.bfloat16),
            pltpu.VMEM((hops + 1, (top + 1 + shared) * chunk[0], chunk[1]), jnp.float32),
            pltpu.VMEM((hops, (top + shared) * chunk[0], chunk[1]), jnp.float32),
            pltpu.VMEM((hops, rows * count, chip_samples), jnp.float32),
            pltpu.VMEM((top + 1 + shared, 2, rows, 2 * count, LANES), jnp.float32),
            pltpu.VMEM((rows * ring, 2 * count, LANES), jnp.float32),
            pltpu.VMEM(tiles.shape, jnp.float32),
            *[pltpu.VMEM(t.shape, t.dtype) for t in tables],
            pltpu.VMEM((count * half, 2 * LANES), jnp.float32),
            pltpu.VMEM((count, LANES), jnp.float32),
            pltpu.SemaphoreType.REGULAR,
            dma((4 + PIECES + len(tables),)),
            dma((PIECES,)),
            dma((PIECES,)),
            dma,
            dma((messages,)),
            dma,
            dma((hops,)),
            dma,
            dma,
        ],
        compiler_params=pltpu.CompilerParams(collective_id=0, has_side_effects=True),
    )(
        traces,
        masks.reshape(rows, ring, 2 * count, channels),
        moveouts.reshape(channels // LANES, LANES),
        tiles,
        *tables,
    )
    return found.transpose(1, 0, 2).reshape(count, lag_count)


def solution(mesh):
    finer = Mesh(mesh.devices.reshape(mesh.shape["grp"], 4, -1, 2), ("grp", "tm_0", "tm_1", "tm_2"))
    axes = ("tm_0", "tm_1", "tm_2")
    return jax.shard_map(
        on_device,
        mesh=finer,
        in_specs=(P("grp", axes), P(axes, None), P("grp"), P(None, "grp")),
        out_specs=P(axes, "grp"),
        check_vma=False,
    )
```

```python
import functools
import math

import jax
import jax.numpy as jnp
import numpy as np
from jax import lax
from jax.experimental import pallas as pl
from jax.experimental.pallas import tpu as pltpu
from jax.sharding import Mesh
from jax.sharding import PartitionSpec as P

MESH = pl.DeviceIdType.MESH
LANES = 128
HOP = 7.1
PIECES = 4


def split(value):
    high = value.astype(jnp.bfloat16)
    low = (value - high.astype(jnp.float32)).astype(jnp.bfloat16)
    return high, low


def split_constant(value):
    value = np.asarray(value, np.float64).astype(np.float32)
    high = value.astype(jnp.bfloat16)
    low = (value - high.astype(np.float32)).astype(jnp.bfloat16)
    return jnp.asarray(np.stack([high, low]))


def mm(a, b):
    return jnp.dot(a, b, preferred_element_type=jnp.float32)


def dot3(left, right):
    (left_hi, left_lo), (right_hi, right_lo) = left, right
    lefts = jnp.concatenate([left_hi, left_hi, left_lo], axis=1)
    return mm(lefts, jnp.concatenate([right_hi, right_lo, right_hi], axis=0))


def forward(series, first, twiddle, second):
    half = twiddle.shape[1]
    turned = []
    for s in series:
        y = dot3((first[0], first[1]), split(s))
        re, im = y[:half], y[half:]
        turned.append(
            jnp.concatenate([re * twiddle[0] - im * twiddle[1], re * twiddle[1] + im * twiddle[0]], axis=1)
        )
    return dot3(split(jnp.concatenate(turned, axis=0)), (second[0], second[1]))


def flow_plan(chunks, hops):
    waiting = [(0.0, 0, g) for g in range(len(chunks))]
    left = [min(o, hops) for o, _ in chunks]
    clock, found = 0.0, []
    while waiting:
        ready = [task for task in waiting if task[0] <= clock]
        if not ready:
            clock = min(waiting)[0]
            continue
        task = max(ready, key=lambda task: (left[task[2]] - task[1], -task[2]))
        waiting.remove(task)
        _, s, g = task
        found.append((clock, s, g))
        clock += chunks[g][1]
        there = max(clock + HOP, 8.2)
        if s + 1 < left[g]:
            waiting.append((there, s + 1, g))
        else:
            found.append((there + 1, s + 1, g))
    return [(s, g) for _, s, g in sorted(found, key=lambda task: task[0])]


def matched_kernel(
    cfg, scale,
    x_hbm, masks_hbm, mo_hbm, templ_hbm, first_hbm, first_half_hbm, twiddle_hbm, second_hbm, third_hbm, fourth_hbm,
    out_ref,
    raw, mo_ref, pair, mask_int, mask_rows, halves, shift_at, parts, partial, flow, merge, ready, landed,
    templ_ref, first_ref, first_half_ref, twiddle_ref, second_ref, third_ref, fourth_ref, templ_spec, gain,
    partner_sem, load_sem, pair_send, pair_recv, flow_send, flow_recv, merge_send, merge_recv, last_send, last_recv,
):
    rows, ring, hops, outside, shared = cfg
    channels = x_hbm.shape[0]
    blocks = rows * ring
    x = lax.axis_index("tm_0")
    z = lax.axis_index("tm_1")
    core = lax.axis_index("tm_2")
    odd = lax.rem(z, 2)
    way = lax.rem(core + z, 2)
    toward = 1 - 2 * way
    here = x * ring + z
    partner = {"tm_2": 1 - core}

    def chip(step):
        other = lax.rem(here + step + blocks, blocks)
        return {"tm_0": other // ring, "tm_1": lax.rem(other, ring)}

    def window_place(s):
        return way * hops + toward * s

    def wait_for(ref, sem):
        pltpu.make_async_copy(ref, ref, sem).wait()

    loads = []

    def load(src, dst):
        copy = pltpu.make_async_copy(src, dst, load_sem.at[len(loads)])
        copy.start()
        loads.append(copy)
        return copy

    per_piece = channels // PIECES
    mo_copy = load(mo_hbm, mo_ref)
    x_copies = [load(x_hbm.at[pl.ds(p * per_piece, per_piece)], raw.at[pl.ds(p * per_piece, per_piece)]) for p in range(PIECES)]

    barrier = pltpu.get_barrier_semaphore()
    peers = [{**chip(-toward), "tm_2": 1 - core}]
    for d in range(1, rows):
        peers += [{"tm_0": lax.rem(x + d, rows), "tm_2": c} for c in (core, 1 - core)]
    for where in peers:
        pl.semaphore_signal(barrier, inc=1, device_id=where, device_id_type=MESH)

    @pl.when(way == 1)
    def _():
        pl.semaphore_signal(barrier, inc=1, device_id=partner, device_id_type=MESH)

    mask_copy = load(masks_hbm, mask_int)
    templ_copy = load(templ_hbm, templ_ref)
    table_copies = [
        load(first_half_hbm, first_half_ref),
        load(twiddle_hbm, twiddle_ref),
        load(second_hbm, second_ref),
        load(first_hbm, first_ref),
        load(third_hbm, third_ref),
        load(fourth_hbm, fourth_ref),
    ]

    lane = lax.broadcasted_iota(jnp.int32, (LANES, LANES), 1)
    mo_copy.wait()
    for p in range(PIECES):
        x_copies[p].wait()

        @pl.loop(p * per_piece // LANES, (p + 1) * per_piece // LANES, unroll=True)
        def _(b):
            at = pl.ds(pl.multiple_of(b * LANES, LANES), LANES)
            spread = jnp.broadcast_to(mo_ref[pl.ds(b, 1), :].astype(jnp.float32), (LANES, LANES))
            move = jnp.transpose(spread).astype(jnp.int32)
            index = lane + (move & (LANES - 1))
            value = jnp.take_along_axis(raw[at, :], index & (LANES - 1), axis=1)
            pair[core, at, :] = value
            passed = (index >= LANES).astype(jnp.int32)
            shift_at[at, :] = ((move >> (LANES.bit_length() - 1)) + passed).astype(jnp.float32).astype(jnp.bfloat16)
            high, low = split(value)
            halves[0, core, at, :] = high
            halves[1, core, at, :] = low

    @pl.when(way == 0)
    def _():
        pl.semaphore_wait(barrier, len(peers) + 1)
        pl.semaphore_signal(partner_sem, inc=1, device_id=partner, device_id_type=MESH)

    @pl.when(way == 1)
    def _():
        pl.semaphore_wait(partner_sem, 1)

    swaps = []
    for p in range(PIECES):
        half = pair.at[core, pl.ds(p * per_piece, per_piece)]
        swap = pltpu.make_async_remote_copy(
            src_ref=half, dst_ref=half, send_sem=pair_send.at[p], recv_sem=pair_recv.at[p],
            device_id=partner, device_id_type=MESH,
        )
        swap.start()
        swaps.append(swap)

    mask_copy.wait()
    tile_rows = mask_int.shape[2]
    per_owner = tile_rows // 2
    own_rows = rows * per_owner
    chunk_rows = 2 * own_rows
    tops = lax.broadcasted_iota(jnp.int32, (tile_rows, channels), 0) < per_owner

    def pick(first, second, side):
        moved = pltpu.roll(jnp.where(side == 0, second, first), per_owner, 0)
        kept = jnp.where(side == 0, first, second)
        return jnp.where(tops == (side == 0), kept, moved).astype(jnp.float32)

    @pl.loop(0, mask_rows.shape[0] // chunk_rows)
    def _(m):
        owner = lax.rem(z + toward * m + ring, ring)
        tiles = [mask_int[a, owner] for a in range(rows)]
        pieces = [pick(tiles[a], tiles[a + 1], side) for side in (way, 1 - way) for a in range(0, rows, 2)]
        kept = jnp.concatenate(pieces, axis=0).astype(jnp.bfloat16)
        at = pl.ds(pl.multiple_of(m * chunk_rows, chunk_rows), chunk_rows)
        mask_rows[at, :channels] = kept
        mask_rows[at, channels:] = kept

    for p in range(PIECES):
        swaps[p].wait_recv()

        @pl.loop(p * per_piece // LANES, (p + 1) * per_piece // LANES)
        def _(b):
            at = pl.ds(pl.multiple_of(b * LANES, LANES), LANES)
            high, low = split(pair[1 - core, at, :])
            halves[0, 1 - core, at, :] = high
            halves[1, 1 - core, at, :] = low

    zero = jnp.zeros((LANES, LANES), jnp.bfloat16)
    top = hops + outside

    def select(s):
        twice = jnp.broadcast_to((2 * window_place(s)).astype(jnp.float32), (LANES, LANES))
        before, same, after = ((twice + d).astype(jnp.bfloat16) for d in (-1, 0, 1))

        @pl.loop(0, channels // LANES)
        def _(b):
            at = pl.ds(pl.multiple_of(b * LANES, LANES), LANES)
            shift = shift_at[at, :]
            is_before, is_same, is_after = shift == before, shift == same, shift == after
            for t in range(2):
                first, second = halves[t, 0, at, :], halves[t, 1, at, :]
                to = pl.ds(pl.multiple_of(t * channels + b * LANES, LANES), LANES)
                parts[to, :LANES] = jnp.where(is_same, first, jnp.where(is_after, second, zero))
                parts[to, LANES:] = jnp.where(is_before, first, jnp.where(is_same, second, zero))

    def multiply(s, low=0, high=None):
        high = (top - s + 1) * chunk_rows + shared * own_rows if high is None else high
        live = pl.ds(low, high - low)
        partial[s, live] = mm(mask_rows[live], parts[...])

    def contribution(s):
        select(s)
        multiply(s)

    select(0)
    halfway = top // 2 + 1
    multiply(0, halfway * chunk_rows)

    sent = {"flow": 0, "merge": 0, "last": 0}
    slots = {}

    def slot_of(s, g):
        return slots.setdefault((s, g), len(slots))

    def send(name, src, dst, send_sem, recv_sem, where):
        pltpu.make_async_remote_copy(
            src_ref=src, dst_ref=dst, send_sem=send_sem, recv_sem=recv_sem, device_id=where, device_id_type=MESH
        ).start()
        sent[name] += math.prod(src.shape)

    groups = [(top + 1, own_rows)] if shared else []
    groups += [(o, chunk_rows) for o in range(top, 0, -1)]
    onward = {**chip(toward), "tm_2": 1 - core}

    def chunk(m, held):
        return pl.ds(m * chunk_rows, held)

    def send_on(s, g):
        o, held = groups[g]
        if s == min(o, hops):
            return
        src = (partial.at[0] if s == 0 else flow.at[s - 1]).at[chunk(o - s, held)]
        dst = flow.at[s, chunk(o - s - 1, held)]
        send("flow", src, dst, flow_send, flow_recv.at[slot_of(s, g)], onward)

    @pl.when(way == 1)
    def _():
        pl.semaphore_wait(barrier, len(peers))

    plan = flow_plan([(o, held / chunk_rows) for o, held in groups], hops)
    begun = next(k for k, (s, _) in enumerate(plan) if s)
    for _, g in plan[:begun]:
        if groups[g][0] >= halfway:
            send_on(0, g)
    multiply(0, chunk_rows, halfway * chunk_rows)
    for _, g in plan[:begun]:
        if groups[g][0] < halfway:
            send_on(0, g)

    def template_spectra():
        templ_copy.wait()
        for copy in table_copies[:3]:
            copy.wait()
        count = out_ref.shape[1]
        short = templ_ref.shape[0] // count
        templates = [templ_ref[pl.ds(i, short, stride=count), :] for i in range(count)]
        templ_spec[...] = forward(templates, first_half_ref[...], twiddle_ref[...], second_ref[...])
        for i in range(count):
            energy = jnp.sqrt(jnp.sum(templates[i] * templates[i], keepdims=True) + 1e-06)
            gain[pl.ds(i, 1), :] = jnp.broadcast_to(1.0 / (scale * energy), (1, LANES))

    todo = list(range(1, hops + 1))
    for _ in range(min(3, hops)):
        contribution(todo.pop(0))

    def deliver(total, s, m, sides):
        slot = s + m
        for side in range(sides):
            for a in range(rows):
                start = side * own_rows + a * per_owner
                piece = total[start : start + per_owner]
                ready[slot, side, a] = jnp.concatenate([piece[:, :LANES], piece[:, LANES:]], axis=0)
        dst = landed.at[lax.rem(here - window_place(s) + blocks, blocks)]
        for side in range(sides):
            for d in range(rows):
                if m:
                    where = {"tm_0": d, "tm_1": lax.rem(z + toward * m + ring, ring), "tm_2": way if side == 0 else 1 - way}
                    send("last", ready.at[slot, side, d], dst, last_send, last_recv, where)
                    continue
                owner = lax.rem(x + d, rows)
                src = ready.at[slot, 0 if sides == 1 else odd if side == 0 else 1 - odd, owner]
                if side == 0 and d == 0:
                    pltpu.make_async_copy(src, dst, last_recv).start()
                else:
                    where = {"tm_0": owner, "tm_2": core if side == 0 else 1 - core}
                    send("last", src, dst, last_send, last_recv, where)

    own = pl.ds(pl.multiple_of(odd * own_rows, own_rows), own_rows)
    others = pl.ds(pl.multiple_of((1 - odd) * own_rows, own_rows), own_rows)

    def merge_and_deliver(s):
        wait_for(merge.at[s], merge_recv.at[s])
        deliver(flow[s - 1, own] + partial[s, own] + merge[s], s, 0, 1)

    def arrive(s, g):
        o, held = groups[g]
        m = o - s
        at = chunk(m, held)
        wait_for(flow.at[s - 1, at], flow_recv.at[slot_of(s - 1, g)])
        if s == hops:
            deliver(flow[s - 1, at] + partial[s, at], s, m, held // own_rows)
        elif m > 0:
            flow[s - 1, at] = flow[s - 1, at] + partial[s, at]
        else:
            send("merge", flow.at[s - 1, others], merge.at[hops - s], merge_send, merge_recv.at[hops - s], partner)
        send_on(s, g)

    merges = [hops // 2] + [s for s in range(hops - 1, 0, -1) if s != hops // 2]
    for s, g in plan[begun:]:
        if s == 0:
            send_on(0, g)
            continue
        while todo and todo[0] <= s:
            contribution(todo.pop(0))
        if s == hops and len(merges) == hops - 1:
            merge_and_deliver(merges.pop(0))
        arrive(s, g)
    for s in merges:
        merge_and_deliver(s)
    template_spectra()

    for swap in swaps:
        swap.wait_send()
    flat = flow.reshape(-1, 2 * LANES)
    wait_for(flat.at[pl.ds(0, sent["flow"] // (2 * LANES))], flow_send)
    wait_for(merge.at[pl.ds(0, sent["merge"] // math.prod(merge.shape[1:]))], merge_send)
    wait_for(landed.at[pl.ds(0, sent["last"] // math.prod(landed.shape[1:]))], last_send)
    for copy in table_copies[3:]:
        copy.wait()
    wait_for(landed, last_recv)

    count = out_ref.shape[1]
    long = blocks * 2
    flat = landed.reshape(long * count, LANES)
    half = twiddle_ref.shape[1]
    series = [flat[pl.ds(i, long, stride=count), :] for i in range(count)]
    twiddle = twiddle_ref[...]
    spec = forward(series, first_ref[...], twiddle, second_ref[...])
    sr, si, hr, hi = spec[:, :LANES], spec[:, LANES:], templ_spec[:, :LANES], templ_spec[:, LANES:]
    product = jnp.concatenate([sr * hr + si * hi, si * hr - sr * hi], axis=1)
    back = dot3(split(product), (third_ref[0], third_ref[1]))
    for i in range(count):
        re, im = back[i * half : (i + 1) * half, :LANES], back[i * half : (i + 1) * half, LANES:]
        turned = jnp.concatenate([re * twiddle[0] + im * twiddle[1], im * twiddle[0] - re * twiddle[1]], axis=0)
        lags = dot3((fourth_ref[0], fourth_ref[1]), split(turned))
        out_ref[:, i, :] = lags * gain[pl.ds(i, 1), :]


def fourier_tables(length, lag_count):
    blocks = length // LANES
    kept = blocks // 2 + 1
    half = -(-kept // 8) * 8
    f1 = np.arange(half)
    n1 = np.arange(blocks)
    n2 = np.arange(LANES)
    live = (f1 < kept)[:, None]
    angle = 2.0 * np.pi * ((f1[:, None] * n1[None, :]) % blocks) / blocks
    first = np.concatenate([np.cos(angle) * live, -np.sin(angle) * live])
    turn = 2.0 * np.pi * ((f1[:, None] * n2[None, :]) % length) / length
    twiddle = np.stack([np.cos(turn) * live, -np.sin(turn) * live]).astype(np.float32)
    inner = 2.0 * np.pi * ((n2[:, None] * n2[None, :]) % LANES) / LANES
    c, s = np.cos(inner), np.sin(inner)
    second = np.block([[c, -s], [s, c]])
    third = np.block([[c, s], [-s, c]])
    weight = np.where((f1 == 0) | (f1 == kept - 1), 1.0, 2.0) * (f1 < kept) / length
    lag_rows = lag_count // LANES
    back = angle.T[:lag_rows]
    fourth = np.concatenate([np.cos(back) * weight, -np.sin(back) * weight], axis=1)
    return (
        split_constant(first),
        split_constant(first[:, :lag_rows]),
        jnp.asarray(twiddle),
        split_constant(second),
        split_constant(third),
        split_constant(fourth),
    )


def on_device(traces, templates, moveouts, masks):
    rows, ring = lax.axis_size("tm_0"), lax.axis_size("tm_1")
    channels, samples = traces.shape
    length = samples * rows * ring * 2
    count, lag_count = templates.shape
    chip_samples = 2 * samples
    hops = (length // 8) // chip_samples
    outside, shared = divmod(ring - 1 - hops, 2)
    top = hops + outside
    cfg = (rows, ring, hops, outside, shared)
    chunk = (2 * rows * count, chip_samples)
    lag_rows = lag_count // LANES
    tiles = templates.reshape(count, lag_rows, LANES).transpose(1, 0, 2).reshape(lag_rows * count, LANES)
    tables = fourier_tables(length, lag_count)
    messages = sum(min(high, hops) for high in range(top, 0, -1)) + shared * hops
    vmem = pl.BlockSpec(memory_space=pltpu.VMEM)
    anywhere = pl.BlockSpec(memory_space=pl.ANY)
    dma = pltpu.SemaphoreType.DMA
    half = tables[2].shape[1]
    found = pl.pallas_call(
        functools.partial(matched_kernel, cfg, math.sqrt(channels)),
        out_shape=pltpu.VMEM((lag_rows, count, LANES), jnp.float32),
        in_specs=[anywhere] * (4 + len(tables)),
        out_specs=vmem,
        scratch_shapes=[
            pltpu.VMEM((channels, samples), jnp.float32),
            pltpu.VMEM((channels // LANES, LANES), jnp.int32),
            pltpu.VMEM((2, channels, samples), jnp.float32),
            pltpu.VMEM((rows, ring, 2 * count, channels), jnp.int32),
            pltpu.VMEM(((top + 1 + shared) * chunk[0], 2 * channels), jnp.bfloat16),
            pltpu.VMEM((2, 2, channels, samples), jnp.bfloat16),
            pltpu.VMEM((channels, samples), jnp.bfloat16),
            pltpu.VMEM((2 * channels, chip_samples), jnp.bfloat16),
            pltpu.VMEM((hops + 1, (top + 1 + shared) * chunk[0], chunk[1]), jnp.float32),
            pltpu.VMEM((hops, (top + shared) * chunk[0], chunk[1]), jnp.float32),
            pltpu.VMEM((hops, rows * count, chip_samples), jnp.float32),
            pltpu.VMEM((top + 1 + shared, 2, rows, 2 * count, LANES), jnp.float32),
            pltpu.VMEM((rows * ring, 2 * count, LANES), jnp.float32),
            pltpu.VMEM(tiles.shape, jnp.float32),
            *[pltpu.VMEM(t.shape, t.dtype) for t in tables],
            pltpu.VMEM((count * half, 2 * LANES), jnp.float32),
            pltpu.VMEM((count, LANES), jnp.float32),
            pltpu.SemaphoreType.REGULAR,
            dma((4 + PIECES + len(tables),)),
            dma((PIECES,)),
            dma((PIECES,)),
            dma,
            dma((messages,)),
            dma,
            dma((hops,)),
            dma,
            dma,
        ],
        compiler_params=pltpu.CompilerParams(collective_id=0, has_side_effects=True),
    )(
        traces,
        masks.reshape(rows, ring, 2 * count, channels),
        moveouts.reshape(channels // LANES, LANES),
        tiles,
        *tables,
    )
    return found.transpose(1, 0, 2).reshape(count, lag_count)


def solution(mesh):
    finer = Mesh(mesh.devices.reshape(mesh.shape["grp"], 4, -1, 2), ("grp", "tm_0", "tm_1", "tm_2"))
    axes = ("tm_0", "tm_1", "tm_2")
    return jax.shard_map(
        on_device,
        mesh=finer,
        in_specs=(P("grp", axes), P(axes, None), P("grp"), P(None, "grp")),
        out_specs=P(axes, "grp"),
        check_vma=False,
    )
```

```python
import functools
import math

import jax
import jax.numpy as jnp
import numpy as np
from jax import lax
from jax.experimental import pallas as pl
from jax.experimental.pallas import tpu as pltpu
from jax.sharding import Mesh
from jax.sharding import PartitionSpec as P

MESH = pl.DeviceIdType.MESH
LANES = 128
GROUP = 1
PIECES = 4


def split(value):
    high = value.astype(jnp.bfloat16)
    low = (value - high.astype(jnp.float32)).astype(jnp.bfloat16)
    return high, low


def split_constant(value):
    value = np.asarray(value, np.float64).astype(np.float32)
    high = value.astype(jnp.bfloat16)
    low = (value - high.astype(np.float32)).astype(jnp.bfloat16)
    return jnp.asarray(np.stack([high, low]))


def mm(a, b):
    return jnp.dot(a, b, preferred_element_type=jnp.float32)


def dot3(left, right):
    (left_hi, left_lo), (right_hi, right_lo) = left, right
    lefts = jnp.concatenate([left_hi, left_hi, left_lo], axis=1)
    return mm(lefts, jnp.concatenate([right_hi, right_lo, right_hi], axis=0))


def forward(series, first, twiddle, second):
    half = twiddle.shape[1]
    turned = []
    for s in series:
        y = dot3((first[0], first[1]), split(s))
        re, im = y[:half], y[half:]
        turned.append(
            jnp.concatenate([re * twiddle[0] - im * twiddle[1], re * twiddle[1] + im * twiddle[0]], axis=1)
        )
    return dot3(split(jnp.concatenate(turned, axis=0)), (second[0], second[1]))


def matched_kernel(
    cfg, scale,
    x_hbm, masks_hbm, mo_hbm, templ_hbm, first_hbm, first_half_hbm, twiddle_hbm, second_hbm, third_hbm, fourth_hbm,
    out_ref,
    raw, mo_ref, pair, mask_int, mask_rows, halves, shift_at, parts, partial, flow, merge, ready, landed,
    templ_ref, first_ref, first_half_ref, twiddle_ref, second_ref, third_ref, fourth_ref, templ_spec, gain,
    partner_sem, load_sem, pair_send, pair_recv, flow_send, flow_recv, merge_send, merge_recv, last_send, last_recv,
):
    rows, ring, hops, outside, shared = cfg
    channels = x_hbm.shape[0]
    blocks = rows * ring
    x = lax.axis_index("tm_0")
    z = lax.axis_index("tm_1")
    core = lax.axis_index("tm_2")
    odd = lax.rem(z, 2)
    way = lax.rem(core + z, 2)
    toward = 1 - 2 * way
    here = x * ring + z
    partner = {"tm_2": 1 - core}

    def chip(step):
        other = lax.rem(here + step + blocks, blocks)
        return {"tm_0": other // ring, "tm_1": lax.rem(other, ring)}

    def window_place(s):
        return way * hops + toward * s

    def wait_for(ref, sem):
        pltpu.make_async_copy(ref, ref, sem).wait()

    loads = []

    def load(src, dst):
        copy = pltpu.make_async_copy(src, dst, load_sem.at[len(loads)])
        copy.start()
        loads.append(copy)
        return copy

    per_piece = channels // PIECES
    mo_copy = load(mo_hbm, mo_ref)
    x_copies = [load(x_hbm.at[pl.ds(p * per_piece, per_piece)], raw.at[pl.ds(p * per_piece, per_piece)]) for p in range(PIECES)]

    barrier = pltpu.get_barrier_semaphore()
    peers = [{**chip(-toward), "tm_2": 1 - core}]
    for d in range(1, rows):
        peers += [{"tm_0": lax.rem(x + d, rows), "tm_2": c} for c in (core, 1 - core)]
    for where in peers:
        pl.semaphore_signal(barrier, inc=1, device_id=where, device_id_type=MESH)

    @pl.when(way == 1)
    def _():
        pl.semaphore_signal(barrier, inc=1, device_id=partner, device_id_type=MESH)

    mask_copy = load(masks_hbm, mask_int)
    templ_copy = load(templ_hbm, templ_ref)
    table_copies = [
        load(first_half_hbm, first_half_ref),
        load(twiddle_hbm, twiddle_ref),
        load(second_hbm, second_ref),
        load(first_hbm, first_ref),
        load(third_hbm, third_ref),
        load(fourth_hbm, fourth_ref),
    ]

    lane = lax.broadcasted_iota(jnp.int32, (LANES, LANES), 1)
    mo_copy.wait()
    def roll(p):
        x_copies[p].wait()

        @pl.loop(p * per_piece // LANES, (p + 1) * per_piece // LANES, unroll=True)
        def _(b):
            at = pl.ds(pl.multiple_of(b * LANES, LANES), LANES)
            spread = jnp.broadcast_to(mo_ref[pl.ds(b, 1), :].astype(jnp.float32), (LANES, LANES))
            move = jnp.transpose(spread).astype(jnp.int32)
            index = lane + (move & (LANES - 1))
            value = jnp.take_along_axis(raw[at, :], index & (LANES - 1), axis=1)
            pair[core, at, :] = value
            passed = (index >= LANES).astype(jnp.int32)
            shift_at[at, :] = ((move >> (LANES.bit_length() - 1)) + passed).astype(jnp.float32).astype(jnp.bfloat16)
            high, low = split(value)
            halves[0, core, at, :] = high
            halves[1, core, at, :] = low

    ahead = PIECES // 2
    for p in range(ahead):
        roll(p)

    @pl.when(way == 0)
    def _():
        pl.semaphore_wait(barrier, len(peers) + 1)
        pl.semaphore_signal(partner_sem, inc=1, device_id=partner, device_id_type=MESH)

    @pl.when(way == 1)
    def _():
        pl.semaphore_wait(partner_sem, 1)

    swaps = []
    for p in range(PIECES):
        if p >= ahead:
            roll(p)
        half = pair.at[core, pl.ds(p * per_piece, per_piece)]
        swap = pltpu.make_async_remote_copy(
            src_ref=half, dst_ref=half, send_sem=pair_send.at[p], recv_sem=pair_recv.at[p],
            device_id=partner, device_id_type=MESH,
        )
        swap.start()
        swaps.append(swap)

    mask_copy.wait()
    tile_rows = mask_int.shape[2]
    per_owner = tile_rows // 2
    own_rows = rows * per_owner
    chunk_rows = 2 * own_rows
    tops = lax.broadcasted_iota(jnp.int32, (tile_rows, channels), 0) < per_owner

    def pick(first, second, side):
        moved = pltpu.roll(jnp.where(side == 0, second, first), per_owner, 0)
        kept = jnp.where(side == 0, first, second)
        return jnp.where(tops == (side == 0), kept, moved).astype(jnp.float32)

    @pl.loop(0, mask_rows.shape[0] // chunk_rows)
    def _(m):
        owner = lax.rem(z + toward * m + ring, ring)
        tiles = [mask_int[a, owner] for a in range(rows)]
        pieces = [pick(tiles[a], tiles[a + 1], side) for side in (way, 1 - way) for a in range(0, rows, 2)]
        kept = jnp.concatenate(pieces, axis=0).astype(jnp.bfloat16)
        at = pl.ds(pl.multiple_of(m * chunk_rows, chunk_rows), chunk_rows)
        mask_rows[at, :channels] = kept
        mask_rows[at, channels:] = kept

    zero = jnp.zeros((LANES, LANES), jnp.bfloat16)
    top = hops + outside

    def select(s, start=0, end=channels // LANES):
        twice = jnp.broadcast_to((2 * window_place(s)).astype(jnp.float32), (LANES, LANES))
        before, same, after = ((twice + d).astype(jnp.bfloat16) for d in (-1, 0, 1))

        @pl.loop(start, end)
        def _(b):
            at = pl.ds(pl.multiple_of(b * LANES, LANES), LANES)
            shift = shift_at[at, :]
            is_before, is_same, is_after = shift == before, shift == same, shift == after
            for t in range(2):
                first, second = halves[t, 0, at, :], halves[t, 1, at, :]
                to = pl.ds(pl.multiple_of(t * channels + b * LANES, LANES), LANES)
                parts[to, :LANES] = jnp.where(is_same, first, jnp.where(is_after, second, zero))
                parts[to, LANES:] = jnp.where(is_before, first, jnp.where(is_same, second, zero))

    for p in range(PIECES):
        swaps[p].wait_recv()
        start, end = p * per_piece // LANES, (p + 1) * per_piece // LANES

        @pl.loop(start, end)
        def _(b):
            at = pl.ds(pl.multiple_of(b * LANES, LANES), LANES)
            high, low = split(pair[1 - core, at, :])
            halves[0, 1 - core, at, :] = high
            halves[1, 1 - core, at, :] = low

        select(0, start, end)

    def multiply(s, low=0, high=None):
        high = (top - s + 1) * chunk_rows + shared * own_rows if high is None else high
        live = pl.ds(low, high - low)
        partial[s, live] = mm(mask_rows[live], parts[...])

    def contribution(s):
        select(s)
        multiply(s)

    cuts = [top + 1 + shared, *range(top - 2, 1, -4), 1]
    multiply(0, cuts[1] * chunk_rows)

    sent = {"flow": 0, "merge": 0, "last": 0}
    slots = {}

    def slot_of(s, g):
        return slots.setdefault((s, g), len(slots))

    def send(name, src, dst, send_sem, recv_sem, where):
        pltpu.make_async_remote_copy(
            src_ref=src, dst_ref=dst, send_sem=send_sem, recv_sem=recv_sem, device_id=where, device_id_type=MESH
        ).start()
        sent[name] += math.prod(src.shape)

    groups = [(top + 1, top + 1, own_rows)] if shared else []
    groups += [(max(high - GROUP + 1, 1), high, chunk_rows) for high in range(top, 0, -GROUP)]
    onward = {**chip(toward), "tm_2": 1 - core}

    def chunks(m, count, held):
        return pl.ds(m * chunk_rows, (count - 1) * chunk_rows + held)

    def span(s, g):
        low, high, held = groups[g]
        low = max(low, s + 1)
        return (low - s, high - low + 1, held) if low <= high and s < hops else None

    def send_on(s, g):
        found = span(s, g)
        if found is None:
            return
        m, count, held = found
        src = (partial.at[0] if s == 0 else flow.at[s - 1]).at[chunks(m, count, held)]
        dst = flow.at[s, chunks(m - 1, count, held)]
        send("flow", src, dst, flow_send, flow_recv.at[slot_of(s, g)], onward)

    @pl.when(way == 1)
    def _():
        pl.semaphore_wait(barrier, len(peers))

    for k, (high, low) in enumerate(zip(cuts, cuts[1:])):
        if k:
            multiply(0, low * chunk_rows, high * chunk_rows)
        for g in range(len(groups)):
            if low <= groups[g][0] < high:
                send_on(0, g)

    def template_spectra():
        templ_copy.wait()
        for copy in table_copies[:3]:
            copy.wait()
        count = out_ref.shape[1]
        short = templ_ref.shape[0] // count
        templates = [templ_ref[pl.ds(i, short, stride=count), :] for i in range(count)]
        templ_spec[...] = forward(templates, first_half_ref[...], twiddle_ref[...], second_ref[...])
        for i in range(count):
            energy = jnp.sqrt(jnp.sum(templates[i] * templates[i], keepdims=True) + 1e-06)
            gain[pl.ds(i, 1), :] = jnp.broadcast_to(1.0 / (scale * energy), (1, LANES))

    contribution(1)
    contribution(2)
    template_spectra()
    todo = list(range(3, hops + 1))

    def deliver(total, s, m, sides):
        slot = s + m
        for side in range(sides):
            for a in range(rows):
                start = side * own_rows + a * per_owner
                piece = total[start : start + per_owner]
                ready[slot, side, a] = jnp.concatenate([piece[:, :LANES], piece[:, LANES:]], axis=0)
        dst = landed.at[lax.rem(here - window_place(s) + blocks, blocks)]
        for side in range(sides):
            for d in range(rows):
                if m:
                    where = {"tm_0": d, "tm_1": lax.rem(z + toward * m + ring, ring), "tm_2": way if side == 0 else 1 - way}
                    send("last", ready.at[slot, side, d], dst, last_send, last_recv, where)
                    continue
                owner = lax.rem(x + d, rows)
                src = ready.at[slot, 0 if sides == 1 else odd if side == 0 else 1 - odd, owner]
                if side == 0 and d == 0:
                    pltpu.make_async_copy(src, dst, last_recv).start()
                else:
                    where = {"tm_0": owner, "tm_2": core if side == 0 else 1 - core}
                    send("last", src, dst, last_send, last_recv, where)

    own = pl.ds(pl.multiple_of(odd * own_rows, own_rows), own_rows)
    others = pl.ds(pl.multiple_of((1 - odd) * own_rows, own_rows), own_rows)

    def merge_and_deliver(s):
        wait_for(merge.at[s], merge_recv.at[s])
        deliver(flow[s - 1, own] + partial[s, own] + merge[s], s, 0, 1)

    def arrive(s, g):
        arrived = span(s - 1, g)
        if arrived is None:
            return
        m, count, held = arrived
        m = m - 1
        wait_for(flow.at[s - 1, chunks(m, count, held)], flow_recv.at[slot_of(s - 1, g)])
        for c in reversed(range(m, m + count)):
            at = chunks(c, 1, held)
            if s == hops:
                deliver(flow[s - 1, at] + partial[s, at], s, c, held // own_rows)
            elif c > 0:
                flow[s - 1, at] = flow[s - 1, at] + partial[s, at]
            else:
                src = flow.at[s - 1, others]
                send("merge", src, merge.at[hops - s], merge_send, merge_recv.at[hops - s], partner)
        send_on(s, g)

    for s in range(1, hops + 1):
        if s == hops and hops % 2 == 0:
            merge_and_deliver(hops // 2)
        for g in range(len(groups)):
            arrive(s, g)
            if todo and g in (2, 6):
                contribution(todo.pop(0))
        if hops < 2 * s < 2 * hops:
            merge_and_deliver(s)
    for s in range((hops - 1) // 2, 0, -1):
        merge_and_deliver(s)

    for swap in swaps:
        swap.wait_send()
    flat = flow.reshape(-1, 2 * LANES)
    wait_for(flat.at[pl.ds(0, sent["flow"] // (2 * LANES))], flow_send)
    wait_for(merge.at[pl.ds(0, sent["merge"] // math.prod(merge.shape[1:]))], merge_send)
    wait_for(landed.at[pl.ds(0, sent["last"] // math.prod(landed.shape[1:]))], last_send)
    for copy in table_copies[3:]:
        copy.wait()
    wait_for(landed, last_recv)

    count = out_ref.shape[1]
    long = blocks * 2
    flat = landed.reshape(long * count, LANES)
    half = twiddle_ref.shape[1]
    series = [flat[pl.ds(i, long, stride=count), :] for i in range(count)]
    twiddle = twiddle_ref[...]
    spec = forward(series, first_ref[...], twiddle, second_ref[...])
    sr, si, hr, hi = spec[:, :LANES], spec[:, LANES:], templ_spec[:, :LANES], templ_spec[:, LANES:]
    product = jnp.concatenate([sr * hr + si * hi, si * hr - sr * hi], axis=1)
    back = dot3(split(product), (third_ref[0], third_ref[1]))
    for i in range(count):
        re, im = back[i * half : (i + 1) * half, :LANES], back[i * half : (i + 1) * half, LANES:]
        turned = jnp.concatenate([re * twiddle[0] + im * twiddle[1], im * twiddle[0] - re * twiddle[1]], axis=0)
        lags = dot3((fourth_ref[0], fourth_ref[1]), split(turned))
        out_ref[:, i, :] = lags * gain[pl.ds(i, 1), :]


def fourier_tables(length, lag_count):
    blocks = length // LANES
    kept = blocks // 2 + 1
    half = -(-kept // 8) * 8
    f1 = np.arange(half)
    n1 = np.arange(blocks)
    n2 = np.arange(LANES)
    live = (f1 < kept)[:, None]
    angle = 2.0 * np.pi * ((f1[:, None] * n1[None, :]) % blocks) / blocks
    first = np.concatenate([np.cos(angle) * live, -np.sin(angle) * live])
    turn = 2.0 * np.pi * ((f1[:, None] * n2[None, :]) % length) / length
    twiddle = np.stack([np.cos(turn) * live, -np.sin(turn) * live]).astype(np.float32)
    inner = 2.0 * np.pi * ((n2[:, None] * n2[None, :]) % LANES) / LANES
    c, s = np.cos(inner), np.sin(inner)
    second = np.block([[c, -s], [s, c]])
    third = np.block([[c, s], [-s, c]])
    weight = np.where((f1 == 0) | (f1 == kept - 1), 1.0, 2.0) * (f1 < kept) / length
    lag_rows = lag_count // LANES
    back = angle.T[:lag_rows]
    fourth = np.concatenate([np.cos(back) * weight, -np.sin(back) * weight], axis=1)
    return (
        split_constant(first),
        split_constant(first[:, :lag_rows]),
        jnp.asarray(twiddle),
        split_constant(second),
        split_constant(third),
        split_constant(fourth),
    )


def on_device(traces, templates, moveouts, masks):
    rows, ring = lax.axis_size("tm_0"), lax.axis_size("tm_1")
    channels, samples = traces.shape
    length = samples * rows * ring * 2
    count, lag_count = templates.shape
    chip_samples = 2 * samples
    hops = (length // 8) // chip_samples
    outside, shared = divmod(ring - 1 - hops, 2)
    top = hops + outside
    cfg = (rows, ring, hops, outside, shared)
    chunk = (2 * rows * count, chip_samples)
    lag_rows = lag_count // LANES
    tiles = templates.reshape(count, lag_rows, LANES).transpose(1, 0, 2).reshape(lag_rows * count, LANES)
    tables = fourier_tables(length, lag_count)
    messages = sum(min(high, hops) for high in range(top, 0, -GROUP)) + shared * hops
    vmem = pl.BlockSpec(memory_space=pltpu.VMEM)
    anywhere = pl.BlockSpec(memory_space=pl.ANY)
    dma = pltpu.SemaphoreType.DMA
    half = tables[2].shape[1]
    found = pl.pallas_call(
        functools.partial(matched_kernel, cfg, math.sqrt(channels)),
        out_shape=pltpu.VMEM((lag_rows, count, LANES), jnp.float32),
        in_specs=[anywhere] * (4 + len(tables)),
        out_specs=vmem,
        scratch_shapes=[
            pltpu.VMEM((channels, samples), jnp.float32),
            pltpu.VMEM((channels // LANES, LANES), jnp.int32),
            pltpu.VMEM((2, channels, samples), jnp.float32),
            pltpu.VMEM((rows, ring, 2 * count, channels), jnp.int32),
            pltpu.VMEM(((top + 1 + shared) * chunk[0], 2 * channels), jnp.bfloat16),
            pltpu.VMEM((2, 2, channels, samples), jnp.bfloat16),
            pltpu.VMEM((channels, samples), jnp.bfloat16),
            pltpu.VMEM((2 * channels, chip_samples), jnp.bfloat16),
            pltpu.VMEM((hops + 1, (top + 1 + shared) * chunk[0], chunk[1]), jnp.float32),
            pltpu.VMEM((hops, (top + shared) * chunk[0], chunk[1]), jnp.float32),
            pltpu.VMEM((hops, rows * count, chip_samples), jnp.float32),
            pltpu.VMEM((top + 1 + shared, 2, rows, 2 * count, LANES), jnp.float32),
            pltpu.VMEM((rows * ring, 2 * count, LANES), jnp.float32),
            pltpu.VMEM(tiles.shape, jnp.float32),
            *[pltpu.VMEM(t.shape, t.dtype) for t in tables],
            pltpu.VMEM((count * half, 2 * LANES), jnp.float32),
            pltpu.VMEM((count, LANES), jnp.float32),
            pltpu.SemaphoreType.REGULAR,
            dma((4 + PIECES + len(tables),)),
            dma((PIECES,)),
            dma((PIECES,)),
            dma,
            dma((messages,)),
            dma,
            dma((hops,)),
            dma,
            dma,
        ],
        compiler_params=pltpu.CompilerParams(collective_id=0, has_side_effects=True),
    )(
        traces,
        masks.reshape(rows, ring, 2 * count, channels),
        moveouts.reshape(channels // LANES, LANES),
        tiles,
        *tables,
    )
    return found.transpose(1, 0, 2).reshape(count, lag_count)


def solution(mesh):
    finer = Mesh(mesh.devices.reshape(mesh.shape["grp"], 4, -1, 2), ("grp", "tm_0", "tm_1", "tm_2"))
    axes = ("tm_0", "tm_1", "tm_2")
    return jax.shard_map(
        on_device,
        mesh=finer,
        in_specs=(P("grp", axes), P(axes, None), P("grp"), P(None, "grp")),
        out_specs=P(axes, "grp"),
        check_vma=False,
    )
```

```python
import functools
import math

import jax
import jax.numpy as jnp
import numpy as np
from jax import lax
from jax.experimental import pallas as pl
from jax.experimental.pallas import tpu as pltpu
from jax.sharding import Mesh
from jax.sharding import PartitionSpec as P

MESH = pl.DeviceIdType.MESH
LANES = 128
GROUP = 1
PIECES = 4


def split(value):
    high = value.astype(jnp.bfloat16)
    low = (value - high.astype(jnp.float32)).astype(jnp.bfloat16)
    return high, low


def split_constant(value):
    value = np.asarray(value, np.float64).astype(np.float32)
    high = value.astype(jnp.bfloat16)
    low = (value - high.astype(np.float32)).astype(jnp.bfloat16)
    return jnp.asarray(np.stack([high, low]))


def mm(a, b):
    return jnp.dot(a, b, preferred_element_type=jnp.float32)


def dot3(left, right):
    (left_hi, left_lo), (right_hi, right_lo) = left, right
    lefts = jnp.concatenate([left_hi, left_hi, left_lo], axis=1)
    return mm(lefts, jnp.concatenate([right_hi, right_lo, right_hi], axis=0))


def forward(series, first, twiddle, second):
    half = twiddle.shape[1]
    turned = []
    for s in series:
        y = dot3((first[0], first[1]), split(s))
        re, im = y[:half], y[half:]
        turned.append(
            jnp.concatenate([re * twiddle[0] - im * twiddle[1], re * twiddle[1] + im * twiddle[0]], axis=1)
        )
    return dot3(split(jnp.concatenate(turned, axis=0)), (second[0], second[1]))


def matched_kernel(
    cfg, scale,
    x_hbm, masks_hbm, mo_hbm, templ_hbm, first_hbm, first_half_hbm, twiddle_hbm, second_hbm, third_hbm, fourth_hbm,
    out_ref,
    raw, mo_ref, pair, mask_int, mask_rows, halves, shift_at, parts, partial, flow, merge, ready, landed,
    templ_ref, first_ref, first_half_ref, twiddle_ref, second_ref, third_ref, fourth_ref, templ_spec, gain,
    partner_sem, load_sem, pair_send, pair_recv, flow_send, flow_recv, merge_send, merge_recv, last_send, last_recv,
    far_send, far_last,
):
    rows, ring, hops, outside, shared = cfg
    channels = x_hbm.shape[0]
    blocks = rows * ring
    x = lax.axis_index("tm_0")
    z = lax.axis_index("tm_1")
    core = lax.axis_index("tm_2")
    odd = lax.rem(z, 2)
    way = lax.rem(core + z, 2)
    toward = 1 - 2 * way
    here = x * ring + z
    partner = {"tm_2": 1 - core}

    def chip(step):
        other = lax.rem(here + step + blocks, blocks)
        return {"tm_0": other // ring, "tm_1": lax.rem(other, ring)}

    def window_place(s):
        return way * hops + toward * s

    def wait_for(ref, sem):
        pltpu.make_async_copy(ref, ref, sem).wait()

    loads = []

    def load(src, dst):
        copy = pltpu.make_async_copy(src, dst, load_sem.at[len(loads)])
        copy.start()
        loads.append(copy)
        return copy

    per_piece = channels // PIECES
    mo_copy = load(mo_hbm, mo_ref)
    x_copies = [load(x_hbm.at[pl.ds(p * per_piece, per_piece)], raw.at[pl.ds(p * per_piece, per_piece)]) for p in range(PIECES)]

    barrier = pltpu.get_barrier_semaphore()
    peers = [{**chip(-toward), "tm_2": 1 - core}]
    for d in range(1, rows):
        peers += [{"tm_0": lax.rem(x + d, rows), "tm_2": c} for c in (core, 1 - core)]
    for where in peers:
        pl.semaphore_signal(barrier, inc=1, device_id=where, device_id_type=MESH)

    @pl.when(way == 1)
    def _():
        pl.semaphore_signal(barrier, inc=1, device_id=partner, device_id_type=MESH)

    mask_copy = load(masks_hbm, mask_int)
    templ_copy = load(templ_hbm, templ_ref)
    table_copies = [
        load(first_half_hbm, first_half_ref),
        load(twiddle_hbm, twiddle_ref),
        load(second_hbm, second_ref),
        load(first_hbm, first_ref),
        load(third_hbm, third_ref),
        load(fourth_hbm, fourth_ref),
    ]

    lane = lax.broadcasted_iota(jnp.int32, (LANES, LANES), 1)
    mo_copy.wait()
    def roll(p):
        x_copies[p].wait()

        @pl.loop(p * per_piece // LANES, (p + 1) * per_piece // LANES, unroll=True)
        def _(b):
            at = pl.ds(pl.multiple_of(b * LANES, LANES), LANES)
            spread = jnp.broadcast_to(mo_ref[pl.ds(b, 1), :].astype(jnp.float32), (LANES, LANES))
            move = jnp.transpose(spread).astype(jnp.int32)
            index = lane + (move & (LANES - 1))
            value = jnp.take_along_axis(raw[at, :], index & (LANES - 1), axis=1)
            pair[core, at, :] = value
            passed = (index >= LANES).astype(jnp.int32)
            shift_at[at, :] = ((move >> (LANES.bit_length() - 1)) + passed).astype(jnp.float32).astype(jnp.bfloat16)
            high, low = split(value)
            halves[0, core, at, :] = high
            halves[1, core, at, :] = low

    ahead = PIECES // 2
    for p in range(ahead):
        roll(p)

    @pl.when(way == 0)
    def _():
        pl.semaphore_wait(barrier, len(peers) + 1)
        pl.semaphore_signal(partner_sem, inc=1, device_id=partner, device_id_type=MESH)

    @pl.when(way == 1)
    def _():
        pl.semaphore_wait(partner_sem, 1)

    swaps = []
    for p in range(PIECES):
        if p >= ahead:
            roll(p)
        half = pair.at[core, pl.ds(p * per_piece, per_piece)]
        swap = pltpu.make_async_remote_copy(
            src_ref=half, dst_ref=half, send_sem=pair_send.at[p], recv_sem=pair_recv.at[p],
            device_id=partner, device_id_type=MESH,
        )
        swap.start()
        swaps.append(swap)

    mask_copy.wait()
    tile_rows = mask_int.shape[2]
    per_owner = tile_rows // 2
    own_rows = rows * per_owner
    chunk_rows = 2 * own_rows
    tops = lax.broadcasted_iota(jnp.int32, (tile_rows, channels), 0) < per_owner

    def pick(first, second, side):
        moved = pltpu.roll(jnp.where(side == 0, second, first), per_owner, 0)
        kept = jnp.where(side == 0, first, second)
        return jnp.where(tops == (side == 0), kept, moved).astype(jnp.float32)

    @pl.loop(0, mask_rows.shape[0] // chunk_rows)
    def _(m):
        owner = lax.rem(z + toward * m + ring, ring)
        tiles = [mask_int[a, owner] for a in range(rows)]
        pieces = [pick(tiles[a], tiles[a + 1], side) for side in (way, 1 - way) for a in range(0, rows, 2)]
        kept = jnp.concatenate(pieces, axis=0).astype(jnp.bfloat16)
        at = pl.ds(pl.multiple_of(m * chunk_rows, chunk_rows), chunk_rows)
        mask_rows[at, :channels] = kept
        mask_rows[at, channels:] = kept

    zero = jnp.zeros((LANES, LANES), jnp.bfloat16)
    top = hops + outside

    def select(s, start=0, end=channels // LANES):
        twice = jnp.broadcast_to((2 * window_place(s)).astype(jnp.float32), (LANES, LANES))
        before, same, after = ((twice + d).astype(jnp.bfloat16) for d in (-1, 0, 1))

        @pl.loop(start, end)
        def _(b):
            at = pl.ds(pl.multiple_of(b * LANES, LANES), LANES)
            shift = shift_at[at, :]
            is_before, is_same, is_after = shift == before, shift == same, shift == after
            for t in range(2):
                first, second = halves[t, 0, at, :], halves[t, 1, at, :]
                to = pl.ds(pl.multiple_of(t * channels + b * LANES, LANES), LANES)
                parts[to, :LANES] = jnp.where(is_same, first, jnp.where(is_after, second, zero))
                parts[to, LANES:] = jnp.where(is_before, first, jnp.where(is_same, second, zero))

    for p in range(PIECES):
        swaps[p].wait_recv()
        start, end = p * per_piece // LANES, (p + 1) * per_piece // LANES

        @pl.loop(start, end)
        def _(b):
            at = pl.ds(pl.multiple_of(b * LANES, LANES), LANES)
            high, low = split(pair[1 - core, at, :])
            halves[0, 1 - core, at, :] = high
            halves[1, 1 - core, at, :] = low

        select(0, start, end)

    def multiply(s, low=0, high=None):
        high = (top - s + 1 + shared) * chunk_rows if high is None else high
        live = pl.ds(low, high - low)
        partial[s, live] = mm(mask_rows[live], parts[...])

    def contribution(s):
        select(s)
        multiply(s)

    cuts = [top + 1 + shared, *range(top - 2, 1, -4), 1]
    multiply(0, cuts[1] * chunk_rows)

    sent = {"flow": 0, "merge": 0, "last": 0, "far": 0, "far last": 0}
    slots = {}

    def slot_of(s, g):
        return slots.setdefault((s, g), len(slots))

    def send(name, src, dst, send_sem, recv_sem, where):
        pltpu.make_async_remote_copy(
            src_ref=src, dst_ref=dst, send_sem=send_sem, recv_sem=recv_sem, device_id=where, device_id_type=MESH
        ).start()
        sent[name] += math.prod(src.shape)

    groups = [(top + 1, top + 1, chunk_rows)] if shared else []
    groups += [(max(high - GROUP + 1, 1), high, chunk_rows) for high in range(top, 0, -GROUP)]
    onward = {**chip(toward), "tm_2": 1 - core}

    def chunks(m, count, held):
        return pl.ds(m * chunk_rows, (count - 1) * chunk_rows + held)

    def span(s, g):
        low, high, held = groups[g]
        low = max(low, s + 1)
        return (low - s, high - low + 1, held) if low <= high and s < hops else None

    def alone(g):
        return bool(shared) and g == 0

    def send_on(s, g):
        found = span(s, g)
        if found is None:
            return
        m, count, held = found
        src = (partial.at[0] if s == 0 else flow.at[s - 1]).at[chunks(m, count, held)]
        dst = flow.at[s, chunks(m - 1, count, held)]
        if alone(g):
            send("far", src, dst, far_send, flow_recv.at[slot_of(s, g)], onward)
        else:
            send("flow", src, dst, flow_send, flow_recv.at[slot_of(s, g)], onward)

    def guarded(step, s, g):
        if alone(g):
            pl.when(way == 1)(lambda: step(s, g))
        else:
            step(s, g)

    @pl.when(way == 1)
    def _():
        pl.semaphore_wait(barrier, len(peers))

    for k, (high, low) in enumerate(zip(cuts, cuts[1:])):
        if k:
            multiply(0, low * chunk_rows, high * chunk_rows)
        for g in range(len(groups)):
            if low <= groups[g][0] < high:
                guarded(send_on, 0, g)

    def template_spectra():
        templ_copy.wait()
        for copy in table_copies[:3]:
            copy.wait()
        count = out_ref.shape[1]
        short = templ_ref.shape[0] // count
        templates = [templ_ref[pl.ds(i, short, stride=count), :] for i in range(count)]
        templ_spec[...] = forward(templates, first_half_ref[...], twiddle_ref[...], second_ref[...])
        for i in range(count):
            energy = jnp.sqrt(jnp.sum(templates[i] * templates[i], keepdims=True) + 1e-06)
            gain[pl.ds(i, 1), :] = jnp.broadcast_to(1.0 / (scale * energy), (1, LANES))

    contribution(1)
    contribution(2)
    template_spectra()
    todo = list(range(3, hops + 1))

    def deliver(total, s, m, sides, far=False):
        slot = s + m
        for side in range(sides):
            for a in range(rows):
                start = side * own_rows + a * per_owner
                piece = total[start : start + per_owner]
                ready[slot, side, a] = jnp.concatenate([piece[:, :LANES], piece[:, LANES:]], axis=0)
        dst = landed.at[lax.rem(here - window_place(s) + blocks, blocks)]
        for side in range(sides):
            for d in range(rows):
                if m:
                    where = {"tm_0": d, "tm_1": lax.rem(z + toward * m + ring, ring), "tm_2": way if side == 0 else 1 - way}
                    name, sem = ("far last", far_last) if far else ("last", last_send)
                    send(name, ready.at[slot, side, d], dst, sem, last_recv, where)
                    continue
                owner = lax.rem(x + d, rows)
                src = ready.at[slot, 0 if sides == 1 else odd if side == 0 else 1 - odd, owner]
                if side == 0 and d == 0:
                    pltpu.make_async_copy(src, dst, last_recv).start()
                else:
                    where = {"tm_0": owner, "tm_2": core if side == 0 else 1 - core}
                    send("last", src, dst, last_send, last_recv, where)

    own = pl.ds(pl.multiple_of(odd * own_rows, own_rows), own_rows)
    others = pl.ds(pl.multiple_of((1 - odd) * own_rows, own_rows), own_rows)

    def merge_and_deliver(s):
        wait_for(merge.at[s], merge_recv.at[s])
        deliver(flow[s - 1, own] + partial[s, own] + merge[s], s, 0, 1)

    def arrive(s, g):
        arrived = span(s - 1, g)
        if arrived is None:
            return
        m, count, held = arrived
        m = m - 1
        wait_for(flow.at[s - 1, chunks(m, count, held)], flow_recv.at[slot_of(s - 1, g)])
        for c in reversed(range(m, m + count)):
            at = chunks(c, 1, held)
            if s == hops:
                deliver(flow[s - 1, at] + partial[s, at], s, c, held // own_rows, alone(g))
            elif c > 0:
                flow[s - 1, at] = flow[s - 1, at] + partial[s, at]
            else:
                src = flow.at[s - 1, others]
                send("merge", src, merge.at[hops - s], merge_send, merge_recv.at[hops - s], partner)
        send_on(s, g)

    for s in range(1, hops + 1):
        if s == hops and hops % 2 == 0:
            merge_and_deliver(hops // 2)
        for g in range(len(groups)):
            guarded(arrive, s, g)
            if todo and g in (2, 6):
                contribution(todo.pop(0))
        if hops < 2 * s < 2 * hops:
            merge_and_deliver(s)
    for s in range((hops - 1) // 2, 0, -1):
        merge_and_deliver(s)

    for swap in swaps:
        swap.wait_send()
    flat = flow.reshape(-1, 2 * LANES)
    wait_for(flat.at[pl.ds(0, sent["flow"] // (2 * LANES))], flow_send)
    wait_for(merge.at[pl.ds(0, sent["merge"] // math.prod(merge.shape[1:]))], merge_send)
    wait_for(landed.at[pl.ds(0, sent["last"] // math.prod(landed.shape[1:]))], last_send)
    if shared:

        @pl.when(way == 1)
        def _():
            wait_for(flat.at[pl.ds(0, sent["far"] // (2 * LANES))], far_send)
            wait_for(landed.at[pl.ds(0, sent["far last"] // math.prod(landed.shape[1:]))], far_last)

    for copy in table_copies[3:]:
        copy.wait()
    wait_for(landed, last_recv)

    count = out_ref.shape[1]
    long = blocks * 2
    flat = landed.reshape(long * count, LANES)
    half = twiddle_ref.shape[1]
    series = [flat[pl.ds(i, long, stride=count), :] for i in range(count)]
    twiddle = twiddle_ref[...]
    spec = forward(series, first_ref[...], twiddle, second_ref[...])
    sr, si, hr, hi = spec[:, :LANES], spec[:, LANES:], templ_spec[:, :LANES], templ_spec[:, LANES:]
    product = jnp.concatenate([sr * hr + si * hi, si * hr - sr * hi], axis=1)
    back = dot3(split(product), (third_ref[0], third_ref[1]))
    for i in range(count):
        re, im = back[i * half : (i + 1) * half, :LANES], back[i * half : (i + 1) * half, LANES:]
        turned = jnp.concatenate([re * twiddle[0] + im * twiddle[1], im * twiddle[0] - re * twiddle[1]], axis=0)
        lags = dot3((fourth_ref[0], fourth_ref[1]), split(turned))
        out_ref[:, i, :] = lags * gain[pl.ds(i, 1), :]


def fourier_tables(length, lag_count):
    blocks = length // LANES
    kept = blocks // 2 + 1
    half = -(-kept // 8) * 8
    f1 = np.arange(half)
    n1 = np.arange(blocks)
    n2 = np.arange(LANES)
    live = (f1 < kept)[:, None]
    angle = 2.0 * np.pi * ((f1[:, None] * n1[None, :]) % blocks) / blocks
    first = np.concatenate([np.cos(angle) * live, -np.sin(angle) * live])
    turn = 2.0 * np.pi * ((f1[:, None] * n2[None, :]) % length) / length
    twiddle = np.stack([np.cos(turn) * live, -np.sin(turn) * live]).astype(np.float32)
    inner = 2.0 * np.pi * ((n2[:, None] * n2[None, :]) % LANES) / LANES
    c, s = np.cos(inner), np.sin(inner)
    second = np.block([[c, -s], [s, c]])
    third = np.block([[c, s], [-s, c]])
    weight = np.where((f1 == 0) | (f1 == kept - 1), 1.0, 2.0) * (f1 < kept) / length
    lag_rows = lag_count // LANES
    back = angle.T[:lag_rows]
    fourth = np.concatenate([np.cos(back) * weight, -np.sin(back) * weight], axis=1)
    return (
        split_constant(first),
        split_constant(first[:, :lag_rows]),
        jnp.asarray(twiddle),
        split_constant(second),
        split_constant(third),
        split_constant(fourth),
    )


def on_device(traces, templates, moveouts, masks):
    rows, ring = lax.axis_size("tm_0"), lax.axis_size("tm_1")
    channels, samples = traces.shape
    length = samples * rows * ring * 2
    count, lag_count = templates.shape
    chip_samples = 2 * samples
    hops = (length // 8) // chip_samples
    outside, shared = divmod(ring - 1 - hops, 2)
    top = hops + outside
    cfg = (rows, ring, hops, outside, shared)
    chunk = (2 * rows * count, chip_samples)
    lag_rows = lag_count // LANES
    tiles = templates.reshape(count, lag_rows, LANES).transpose(1, 0, 2).reshape(lag_rows * count, LANES)
    tables = fourier_tables(length, lag_count)
    messages = sum(min(high, hops) for high in range(top, 0, -GROUP)) + shared * hops
    vmem = pl.BlockSpec(memory_space=pltpu.VMEM)
    anywhere = pl.BlockSpec(memory_space=pl.ANY)
    dma = pltpu.SemaphoreType.DMA
    half = tables[2].shape[1]
    found = pl.pallas_call(
        functools.partial(matched_kernel, cfg, math.sqrt(channels)),
        out_shape=pltpu.VMEM((lag_rows, count, LANES), jnp.float32),
        in_specs=[anywhere] * (4 + len(tables)),
        out_specs=vmem,
        scratch_shapes=[
            pltpu.VMEM((channels, samples), jnp.float32),
            pltpu.VMEM((channels // LANES, LANES), jnp.int32),
            pltpu.VMEM((2, channels, samples), jnp.float32),
            pltpu.VMEM((rows, ring, 2 * count, channels), jnp.int32),
            pltpu.VMEM(((top + 1 + shared) * chunk[0], 2 * channels), jnp.bfloat16),
            pltpu.VMEM((2, 2, channels, samples), jnp.bfloat16),
            pltpu.VMEM((channels, samples), jnp.bfloat16),
            pltpu.VMEM((2 * channels, chip_samples), jnp.bfloat16),
            pltpu.VMEM((hops + 1, (top + 1 + shared) * chunk[0], chunk[1]), jnp.float32),
            pltpu.VMEM((hops, (top + shared) * chunk[0], chunk[1]), jnp.float32),
            pltpu.VMEM((hops, rows * count, chip_samples), jnp.float32),
            pltpu.VMEM((top + 1 + shared, 2, rows, 2 * count, LANES), jnp.float32),
            pltpu.VMEM((rows * ring, 2 * count, LANES), jnp.float32),
            pltpu.VMEM(tiles.shape, jnp.float32),
            *[pltpu.VMEM(t.shape, t.dtype) for t in tables],
            pltpu.VMEM((count * half, 2 * LANES), jnp.float32),
            pltpu.VMEM((count, LANES), jnp.float32),
            pltpu.SemaphoreType.REGULAR,
            dma((4 + PIECES + len(tables),)),
            dma((PIECES,)),
            dma((PIECES,)),
            dma,
            dma((messages,)),
            dma,
            dma((hops,)),
            dma,
            dma,
            dma,
            dma,
        ],
        compiler_params=pltpu.CompilerParams(collective_id=0, has_side_effects=True),
    )(
        traces,
        masks.reshape(rows, ring, 2 * count, channels),
        moveouts.reshape(channels // LANES, LANES),
        tiles,
        *tables,
    )
    return found.transpose(1, 0, 2).reshape(count, lag_count)


def solution(mesh):
    finer = Mesh(mesh.devices.reshape(mesh.shape["grp"], 4, -1, 2), ("grp", "tm_0", "tm_1", "tm_2"))
    axes = ("tm_0", "tm_1", "tm_2")
    return jax.shard_map(
        on_device,
        mesh=finer,
        in_specs=(P("grp", axes), P(axes, None), P("grp"), P(None, "grp")),
        out_specs=P(axes, "grp"),
        check_vma=False,
    )
```

```python
import functools
import math

import jax
import jax.numpy as jnp
import numpy as np
from jax import lax
from jax.experimental import pallas as pl
from jax.experimental.pallas import tpu as pltpu
from jax.sharding import Mesh
from jax.sharding import PartitionSpec as P

MESH = pl.DeviceIdType.MESH
LANES = 128
GROUP = 1
PIECES = 4


def split(value):
    high = value.astype(jnp.bfloat16)
    low = (value - high.astype(jnp.float32)).astype(jnp.bfloat16)
    return high, low


def split_constant(value):
    value = np.asarray(value, np.float64).astype(np.float32)
    high = value.astype(jnp.bfloat16)
    low = (value - high.astype(np.float32)).astype(jnp.bfloat16)
    return jnp.asarray(np.stack([high, low]))


def mm(a, b):
    return jnp.dot(a, b, preferred_element_type=jnp.float32)


def dot3(left, right):
    (left_hi, left_lo), (right_hi, right_lo) = left, right
    lefts = jnp.concatenate([left_hi, left_hi, left_lo], axis=1)
    return mm(lefts, jnp.concatenate([right_hi, right_lo, right_hi], axis=0))


def forward(series, first, twiddle, second):
    half = twiddle.shape[1]
    turned = []
    for s in series:
        y = dot3((first[0], first[1]), split(s))
        re, im = y[:half], y[half:]
        turned.append(
            jnp.concatenate([re * twiddle[0] - im * twiddle[1], re * twiddle[1] + im * twiddle[0]], axis=1)
        )
    return dot3(split(jnp.concatenate(turned, axis=0)), (second[0], second[1]))


def matched_kernel(
    cfg, scale,
    x_hbm, masks_hbm, mo_hbm, templ_hbm, first_hbm, first_half_hbm, twiddle_hbm, second_hbm, third_hbm, fourth_hbm,
    out_ref,
    raw, mo_ref, pair, mask_int, mask_rows, halves, shift_at, parts, partial, flow, merge, ready, landed,
    templ_ref, first_ref, first_half_ref, twiddle_ref, second_ref, third_ref, fourth_ref, templ_spec, gain,
    partner_sem, load_sem, pair_send, pair_recv, flow_send, flow_recv, merge_send, merge_recv, last_send, last_recv,
    far_send, far_last,
):
    rows, ring, hops, outside, shared = cfg
    channels = x_hbm.shape[0]
    blocks = rows * ring
    x = lax.axis_index("tm_0")
    z = lax.axis_index("tm_1")
    core = lax.axis_index("tm_2")
    odd = lax.rem(z, 2)
    way = lax.rem(core + z, 2)
    toward = 1 - 2 * way
    here = x * ring + z
    partner = {"tm_2": 1 - core}

    def chip(step):
        other = lax.rem(here + step + blocks, blocks)
        return {"tm_0": other // ring, "tm_1": lax.rem(other, ring)}

    def window_place(s):
        return way * hops + toward * s

    def wait_for(ref, sem):
        pltpu.make_async_copy(ref, ref, sem).wait()

    loads = []

    def load(src, dst):
        copy = pltpu.make_async_copy(src, dst, load_sem.at[len(loads)])
        copy.start()
        loads.append(copy)
        return copy

    per_piece = channels // PIECES
    mo_copy = load(mo_hbm, mo_ref)
    x_copies = [load(x_hbm.at[pl.ds(p * per_piece, per_piece)], raw.at[pl.ds(p * per_piece, per_piece)]) for p in range(PIECES)]

    barrier = pltpu.get_barrier_semaphore()
    peers = [{**chip(-toward), "tm_2": 1 - core}]
    for d in range(1, rows):
        peers += [{"tm_0": lax.rem(x + d, rows), "tm_2": c} for c in (core, 1 - core)]
    for where in peers:
        pl.semaphore_signal(barrier, inc=1, device_id=where, device_id_type=MESH)

    @pl.when(way == 1)
    def _():
        pl.semaphore_signal(barrier, inc=1, device_id=partner, device_id_type=MESH)

    mask_copy = load(masks_hbm, mask_int)
    templ_copy = load(templ_hbm, templ_ref)
    table_copies = [
        load(first_half_hbm, first_half_ref),
        load(twiddle_hbm, twiddle_ref),
        load(second_hbm, second_ref),
        load(first_hbm, first_ref),
        load(third_hbm, third_ref),
        load(fourth_hbm, fourth_ref),
    ]

    lane = lax.broadcasted_iota(jnp.int32, (LANES, LANES), 1)
    mo_copy.wait()
    def roll(p):
        x_copies[p].wait()

        @pl.loop(p * per_piece // LANES, (p + 1) * per_piece // LANES, unroll=True)
        def _(b):
            at = pl.ds(pl.multiple_of(b * LANES, LANES), LANES)
            spread = jnp.broadcast_to(mo_ref[pl.ds(b, 1), :].astype(jnp.float32), (LANES, LANES))
            move = jnp.transpose(spread).astype(jnp.int32)
            index = lane + (move & (LANES - 1))
            value = jnp.take_along_axis(raw[at, :], index & (LANES - 1), axis=1)
            pair[core, at, :] = value
            passed = (index >= LANES).astype(jnp.int32)
            shift_at[at, :] = ((move >> (LANES.bit_length() - 1)) + passed).astype(jnp.float32).astype(jnp.bfloat16)
            high, low = split(value)
            halves[0, core, at, :] = high
            halves[1, core, at, :] = low

    ahead = PIECES // 2
    for p in range(ahead):
        roll(p)

    @pl.when(way == 0)
    def _():
        pl.semaphore_wait(barrier, len(peers) + 1)
        pl.semaphore_signal(partner_sem, inc=1, device_id=partner, device_id_type=MESH)

    @pl.when(way == 1)
    def _():
        pl.semaphore_wait(partner_sem, 1)

    swaps = []
    for p in range(PIECES):
        if p >= ahead:
            roll(p)
        half = pair.at[core, pl.ds(p * per_piece, per_piece)]
        swap = pltpu.make_async_remote_copy(
            src_ref=half, dst_ref=half, send_sem=pair_send.at[p], recv_sem=pair_recv.at[p],
            device_id=partner, device_id_type=MESH,
        )
        swap.start()
        swaps.append(swap)

    mask_copy.wait()
    tile_rows = mask_int.shape[2]
    per_owner = tile_rows // 2
    own_rows = rows * per_owner
    chunk_rows = 2 * own_rows
    tops = lax.broadcasted_iota(jnp.int32, (tile_rows, channels), 0) < per_owner

    def pick(first, second, side):
        moved = pltpu.roll(jnp.where(side == 0, second, first), per_owner, 0)
        kept = jnp.where(side == 0, first, second)
        return jnp.where(tops == (side == 0), kept, moved).astype(jnp.float32)

    @pl.loop(0, mask_rows.shape[0] // chunk_rows)
    def _(m):
        owner = lax.rem(z + toward * m + ring, ring)
        tiles = [mask_int[a, owner] for a in range(rows)]
        pieces = [pick(tiles[a], tiles[a + 1], side) for side in (way, 1 - way) for a in range(0, rows, 2)]
        kept = jnp.concatenate(pieces, axis=0).astype(jnp.bfloat16)
        at = pl.ds(pl.multiple_of(m * chunk_rows, chunk_rows), chunk_rows)
        mask_rows[at, :channels] = kept
        mask_rows[at, channels:] = kept

    zero = jnp.zeros((LANES, LANES), jnp.bfloat16)
    top = hops + outside

    def select(s, start=0, end=channels // LANES):
        twice = jnp.broadcast_to((2 * window_place(s)).astype(jnp.float32), (LANES, LANES))
        before, same, after = ((twice + d).astype(jnp.bfloat16) for d in (-1, 0, 1))

        @pl.loop(start, end)
        def _(b):
            at = pl.ds(pl.multiple_of(b * LANES, LANES), LANES)
            shift = shift_at[at, :]
            is_before, is_same, is_after = shift == before, shift == same, shift == after
            for t in range(2):
                first, second = halves[t, 0, at, :], halves[t, 1, at, :]
                to = pl.ds(pl.multiple_of(t * channels + b * LANES, LANES), LANES)
                parts[to, :LANES] = jnp.where(is_same, first, jnp.where(is_after, second, zero))
                parts[to, LANES:] = jnp.where(is_before, first, jnp.where(is_same, second, zero))

    for p in range(PIECES):
        swaps[p].wait_recv()
        start, end = p * per_piece // LANES, (p + 1) * per_piece // LANES

        @pl.loop(start, end)
        def _(b):
            at = pl.ds(pl.multiple_of(b * LANES, LANES), LANES)
            high, low = split(pair[1 - core, at, :])
            halves[0, 1 - core, at, :] = high
            halves[1, 1 - core, at, :] = low

        select(0, start, end)

    def multiply(s, low=0, high=None):
        high = (top - s + 1 + shared) * chunk_rows if high is None else high
        live = pl.ds(low, high - low)
        partial[s, live] = mm(mask_rows[live], parts[...])

    def contribution(s):
        select(s)
        multiply(s)

    cuts = [top + 1 + shared, *range(top - 2, 1, -4), 1]
    multiply(0, cuts[1] * chunk_rows)

    sent = {"flow": 0, "merge": 0, "last": 0, "far": 0, "far last": 0}
    slots = {}

    def slot_of(s, g):
        return slots.setdefault((s, g), len(slots))

    def send(name, src, dst, send_sem, recv_sem, where):
        pltpu.make_async_remote_copy(
            src_ref=src, dst_ref=dst, send_sem=send_sem, recv_sem=recv_sem, device_id=where, device_id_type=MESH
        ).start()
        sent[name] += math.prod(src.shape)

    groups = [(top + 1, top + 1, chunk_rows)] if shared else []
    groups += [(max(high - GROUP + 1, 1), high, chunk_rows) for high in range(top, 0, -GROUP)]
    onward = {**chip(toward), "tm_2": 1 - core}

    def chunks(m, count, held):
        return pl.ds(m * chunk_rows, (count - 1) * chunk_rows + held)

    def span(s, g):
        low, high, held = groups[g]
        low = max(low, s + 1)
        return (low - s, high - low + 1, held) if low <= high and s < hops else None

    def alone(g):
        return bool(shared) and g == 0

    def send_on(s, g):
        found = span(s, g)
        if found is None:
            return
        m, count, held = found
        src = (partial.at[0] if s == 0 else flow.at[s - 1]).at[chunks(m, count, held)]
        dst = flow.at[s, chunks(m - 1, count, held)]
        if alone(g):
            send("far", src, dst, far_send, flow_recv.at[slot_of(s, g)], onward)
        else:
            send("flow", src, dst, flow_send, flow_recv.at[slot_of(s, g)], onward)

    def guarded(step, s, g):
        if alone(g):
            pl.when(way == 1)(lambda: step(s, g))
        else:
            step(s, g)

    @pl.when(way == 1)
    def _():
        pl.semaphore_wait(barrier, len(peers))

    for k, (high, low) in enumerate(zip(cuts, cuts[1:])):
        if k:
            multiply(0, low * chunk_rows, high * chunk_rows)
        for g in range(len(groups)):
            if low <= groups[g][0] < high:
                guarded(send_on, 0, g)

    def template_spectra():
        templ_copy.wait()
        for copy in table_copies[:3]:
            copy.wait()
        count = out_ref.shape[1]
        short = templ_ref.shape[0] // count
        templates = [templ_ref[pl.ds(i, short, stride=count), :] for i in range(count)]
        templ_spec[...] = forward(templates, first_half_ref[...], twiddle_ref[...], second_ref[...])
        for i in range(count):
            energy = jnp.sqrt(jnp.sum(templates[i] * templates[i], keepdims=True) + 1e-06)
            gain[pl.ds(i, 1), :] = jnp.broadcast_to(1.0 / (scale * energy), (1, LANES))

    contribution(1)
    contribution(2)
    todo = list(range(3, hops + 1))

    def deliver(total, s, m, sides, far=False):
        slot = s + m
        for side in range(sides):
            for a in range(rows):
                start = side * own_rows + a * per_owner
                piece = total[start : start + per_owner]
                ready[slot, side, a] = jnp.concatenate([piece[:, :LANES], piece[:, LANES:]], axis=0)
        dst = landed.at[lax.rem(here - window_place(s) + blocks, blocks)]
        for side in range(sides):
            for d in range(rows):
                if m:
                    where = {"tm_0": d, "tm_1": lax.rem(z + toward * m + ring, ring), "tm_2": way if side == 0 else 1 - way}
                    name, sem = ("far last", far_last) if far else ("last", last_send)
                    send(name, ready.at[slot, side, d], dst, sem, last_recv, where)
                    continue
                owner = lax.rem(x + d, rows)
                src = ready.at[slot, 0 if sides == 1 else odd if side == 0 else 1 - odd, owner]
                if side == 0 and d == 0:
                    pltpu.make_async_copy(src, dst, last_recv).start()
                else:
                    where = {"tm_0": owner, "tm_2": core if side == 0 else 1 - core}
                    send("last", src, dst, last_send, last_recv, where)

    own = pl.ds(pl.multiple_of(odd * own_rows, own_rows), own_rows)
    others = pl.ds(pl.multiple_of((1 - odd) * own_rows, own_rows), own_rows)

    def merge_and_deliver(s):
        wait_for(merge.at[s], merge_recv.at[s])
        deliver(flow[s - 1, own] + partial[s, own] + merge[s], s, 0, 1)

    def arrive(s, g):
        arrived = span(s - 1, g)
        if arrived is None:
            return
        m, count, held = arrived
        m = m - 1
        wait_for(flow.at[s - 1, chunks(m, count, held)], flow_recv.at[slot_of(s - 1, g)])
        for c in reversed(range(m, m + count)):
            at = chunks(c, 1, held)
            if s == hops:
                deliver(flow[s - 1, at] + partial[s, at], s, c, held // own_rows, alone(g))
            elif c > 0:
                flow[s - 1, at] = flow[s - 1, at] + partial[s, at]
            else:
                src = flow.at[s - 1, others]
                send("merge", src, merge.at[hops - s], merge_send, merge_recv.at[hops - s], partner)
        send_on(s, g)

    for s in range(1, hops + 1):
        if s == hops and hops % 2 == 0:
            merge_and_deliver(hops // 2)
        for g in range(len(groups)):
            guarded(arrive, s, g)
            if todo and g in (2, 6):
                contribution(todo.pop(0))
        if hops < 2 * s < 2 * hops:
            merge_and_deliver(s)
    for s in range((hops - 1) // 2, 0, -1):
        merge_and_deliver(s)

    template_spectra()

    for swap in swaps:
        swap.wait_send()
    flat = flow.reshape(-1, 2 * LANES)
    wait_for(flat.at[pl.ds(0, sent["flow"] // (2 * LANES))], flow_send)
    wait_for(merge.at[pl.ds(0, sent["merge"] // math.prod(merge.shape[1:]))], merge_send)
    wait_for(landed.at[pl.ds(0, sent["last"] // math.prod(landed.shape[1:]))], last_send)
    if shared:

        @pl.when(way == 1)
        def _():
            wait_for(flat.at[pl.ds(0, sent["far"] // (2 * LANES))], far_send)
            wait_for(landed.at[pl.ds(0, sent["far last"] // math.prod(landed.shape[1:]))], far_last)

    for copy in table_copies[3:]:
        copy.wait()
    wait_for(landed, last_recv)

    count = out_ref.shape[1]
    long = blocks * 2
    flat = landed.reshape(long * count, LANES)
    half = twiddle_ref.shape[1]
    series = [flat[pl.ds(i, long, stride=count), :] for i in range(count)]
    twiddle = twiddle_ref[...]
    spec = forward(series, first_ref[...], twiddle, second_ref[...])
    sr, si, hr, hi = spec[:, :LANES], spec[:, LANES:], templ_spec[:, :LANES], templ_spec[:, LANES:]
    product = jnp.concatenate([sr * hr + si * hi, si * hr - sr * hi], axis=1)
    back = dot3(split(product), (third_ref[0], third_ref[1]))
    for i in range(count):
        re, im = back[i * half : (i + 1) * half, :LANES], back[i * half : (i + 1) * half, LANES:]
        turned = jnp.concatenate([re * twiddle[0] + im * twiddle[1], im * twiddle[0] - re * twiddle[1]], axis=0)
        lags = dot3((fourth_ref[0], fourth_ref[1]), split(turned))
        out_ref[:, i, :] = lags * gain[pl.ds(i, 1), :]


def fourier_tables(length, lag_count):
    blocks = length // LANES
    kept = blocks // 2 + 1
    half = -(-kept // 8) * 8
    f1 = np.arange(half)
    n1 = np.arange(blocks)
    n2 = np.arange(LANES)
    live = (f1 < kept)[:, None]
    angle = 2.0 * np.pi * ((f1[:, None] * n1[None, :]) % blocks) / blocks
    first = np.concatenate([np.cos(angle) * live, -np.sin(angle) * live])
    turn = 2.0 * np.pi * ((f1[:, None] * n2[None, :]) % length) / length
    twiddle = np.stack([np.cos(turn) * live, -np.sin(turn) * live]).astype(np.float32)
    inner = 2.0 * np.pi * ((n2[:, None] * n2[None, :]) % LANES) / LANES
    c, s = np.cos(inner), np.sin(inner)
    second = np.block([[c, -s], [s, c]])
    third = np.block([[c, s], [-s, c]])
    weight = np.where((f1 == 0) | (f1 == kept - 1), 1.0, 2.0) * (f1 < kept) / length
    lag_rows = lag_count // LANES
    back = angle.T[:lag_rows]
    fourth = np.concatenate([np.cos(back) * weight, -np.sin(back) * weight], axis=1)
    return (
        split_constant(first),
        split_constant(first[:, :lag_rows]),
        jnp.asarray(twiddle),
        split_constant(second),
        split_constant(third),
        split_constant(fourth),
    )


def on_device(traces, templates, moveouts, masks):
    rows, ring = lax.axis_size("tm_0"), lax.axis_size("tm_1")
    channels, samples = traces.shape
    length = samples * rows * ring * 2
    count, lag_count = templates.shape
    chip_samples = 2 * samples
    hops = (length // 8) // chip_samples
    outside, shared = divmod(ring - 1 - hops, 2)
    top = hops + outside
    cfg = (rows, ring, hops, outside, shared)
    chunk = (2 * rows * count, chip_samples)
    lag_rows = lag_count // LANES
    tiles = templates.reshape(count, lag_rows, LANES).transpose(1, 0, 2).reshape(lag_rows * count, LANES)
    tables = fourier_tables(length, lag_count)
    messages = sum(min(high, hops) for high in range(top, 0, -GROUP)) + shared * hops
    vmem = pl.BlockSpec(memory_space=pltpu.VMEM)
    anywhere = pl.BlockSpec(memory_space=pl.ANY)
    dma = pltpu.SemaphoreType.DMA
    half = tables[2].shape[1]
    found = pl.pallas_call(
        functools.partial(matched_kernel, cfg, math.sqrt(channels)),
        out_shape=pltpu.VMEM((lag_rows, count, LANES), jnp.float32),
        in_specs=[anywhere] * (4 + len(tables)),
        out_specs=vmem,
        scratch_shapes=[
            pltpu.VMEM((channels, samples), jnp.float32),
            pltpu.VMEM((channels // LANES, LANES), jnp.int32),
            pltpu.VMEM((2, channels, samples), jnp.float32),
            pltpu.VMEM((rows, ring, 2 * count, channels), jnp.int32),
            pltpu.VMEM(((top + 1 + shared) * chunk[0], 2 * channels), jnp.bfloat16),
            pltpu.VMEM((2, 2, channels, samples), jnp.bfloat16),
            pltpu.VMEM((channels, samples), jnp.bfloat16),
            pltpu.VMEM((2 * channels, chip_samples), jnp.bfloat16),
            pltpu.VMEM((hops + 1, (top + 1 + shared) * chunk[0], chunk[1]), jnp.float32),
            pltpu.VMEM((hops, (top + shared) * chunk[0], chunk[1]), jnp.float32),
            pltpu.VMEM((hops, rows * count, chip_samples), jnp.float32),
            pltpu.VMEM((top + 1 + shared, 2, rows, 2 * count, LANES), jnp.float32),
            pltpu.VMEM((rows * ring, 2 * count, LANES), jnp.float32),
            pltpu.VMEM(tiles.shape, jnp.float32),
            *[pltpu.VMEM(t.shape, t.dtype) for t in tables],
            pltpu.VMEM((count * half, 2 * LANES), jnp.float32),
            pltpu.VMEM((count, LANES), jnp.float32),
            pltpu.SemaphoreType.REGULAR,
            dma((4 + PIECES + len(tables),)),
            dma((PIECES,)),
            dma((PIECES,)),
            dma,
            dma((messages,)),
            dma,
            dma((hops,)),
            dma,
            dma,
            dma,
            dma,
        ],
        compiler_params=pltpu.CompilerParams(collective_id=0, has_side_effects=True),
    )(
        traces,
        masks.reshape(rows, ring, 2 * count, channels),
        moveouts.reshape(channels // LANES, LANES),
        tiles,
        *tables,
    )
    return found.transpose(1, 0, 2).reshape(count, lag_count)


def solution(mesh):
    finer = Mesh(mesh.devices.reshape(mesh.shape["grp"], 4, -1, 2), ("grp", "tm_0", "tm_1", "tm_2"))
    axes = ("tm_0", "tm_1", "tm_2")
    return jax.shard_map(
        on_device,
        mesh=finer,
        in_specs=(P("grp", axes), P(axes, None), P("grp"), P(None, "grp")),
        out_specs=P(axes, "grp"),
        check_vma=False,
    )
```
